32 devices in a mesh: dp: 2 (over x), model: 4 (over z), ctx: 4 (over y, core).
Axes of the slice: x: 2, y: 2, z: 4, core: 2. Of those that a mesh axis runs over, the one named last changes fastest.
Arguments:
- x_tokens: bfloat16 [4096, 2560], P(('dp', 'ctx')), parts along dimension 0
- positions: int32 [4096], P(('dp', 'ctx')), parts along dimension 0
- w_dq: bfloat16 [2560, 768], replicated
- gain_q: float32 [768], replicated
- w_uq: bfloat16 [768, 2560], P(None, 'model')
- w_qr: bfloat16 [768, 1280], P(None, 'model')
- w_dkv: bfloat16 [2560, 256], replicated
- gain_kv: float32 [256], replicated
- w_kr: bfloat16 [2560, 32], replicated
- w_uk: bfloat16 [256, 2560], P(None, 'model')
- w_uv: bfloat16 [256, 2560], P(None, 'model')
- w_out: bfloat16 [2560, 2560], P('model')
Outputs:
- output: bfloat16 [4096, 2560], P(('dp', 'ctx', 'model')), parts along dimension 0
There are 2 independent parts. The reference program is written for one: setup_inputs(seed, part) draws one part's arguments, and reference() takes and returns one part's arrays. A program takes and returns all parts, laid end to end along the dimension named above; an argument that names none is the same for every part.
All inputs are finite; a program needn't handle non-finite values.
Results may differ from the reference program's by a relative error of at most 0.0080343.
Values are sent between devices in bfloat16 or wider.
A program may use at most 1 GiB of HBM per device.

```python
import jax
import jax.numpy as jnp
from jax import lax

HIDDEN = 2560
NUM_HEADS = 40
Q_RANK = 768
KV_RANK = 256
NOPE_DIM = 64
ROPE_DIM = 32
V_DIM = 64
TOKENS_DEV = 512
CTX_DEVS = 4
SEQ_LEN = 2048

SPAN_LEN = TOKENS_DEV // 2
QUERY_BLOCK = min(TOKENS_DEV, 256)
NORM_EPS = 1e-6
ROPE_BASE = 10000.0


def rms_norm(hidden, gain):
    mean_sq = jnp.mean(hidden * hidden, axis=-1, keepdims=True)
    return (hidden * lax.rsqrt(mean_sq + NORM_EPS) * gain).astype(jnp.bfloat16)


def apply_rope(vals, positions):
    half_dim = vals.shape[-1] // 2
    inv_freq = ROPE_BASE ** (-(jnp.arange(half_dim, dtype=jnp.float32) * 2.0 / vals.shape[-1]))
    angles = positions.astype(jnp.float32)[:, None] * inv_freq[None, :]
    angles = angles.reshape((vals.shape[0],) + (1,) * (vals.ndim - 2) + (half_dim,))
    cos_ang = jnp.cos(angles)
    sin_ang = jnp.sin(angles)
    lower_half = vals[..., :half_dim]
    upper_half = vals[..., half_dim:]
    return jnp.concatenate([lower_half * cos_ang - upper_half * sin_ang, upper_half * cos_ang + lower_half * sin_ang], axis=-1)


def draw_positions(rng_key):
    steps = jax.random.randint(rng_key, (SEQ_LEN,), 1, 3, dtype=jnp.int32)
    logical = (jnp.cumsum(steps) - steps[0]).astype(jnp.int32)
    device_idx = jnp.arange(CTX_DEVS)[:, None, None]
    half_idx = jnp.arange(2)[None, :, None]
    offset = jnp.arange(SPAN_LEN)[None, None, :]
    span_id = jnp.where(half_idx == 0, device_idx, 2 * CTX_DEVS - 1 - device_idx)
    storage_idx = (span_id * SPAN_LEN + offset).reshape(SEQ_LEN)
    return logical[storage_idx]


def setup_inputs(seed: int = 0, part: int = 0) -> dict:
    base_key = jax.random.key(seed)
    part_key = jax.random.fold_in(base_key, part)
    key_x, key_pos = jax.random.split(part_key)
    weight_keys = jax.random.split(jax.random.key(seed + 1), 10)

    def weight(rng_key, arr_shape, fan_in, scale_gain):
        return (jax.random.normal(rng_key, arr_shape, jnp.float32) * (scale_gain * fan_in ** -0.5)).astype(jnp.bfloat16)

    return {
        'x_tokens': jax.random.normal(key_x, (SEQ_LEN, HIDDEN), jnp.float32).astype(jnp.bfloat16),
        'positions': draw_positions(key_pos),
        'w_dq': weight(weight_keys[0], (HIDDEN, Q_RANK), HIDDEN, 1.0),
        'gain_q': 1.0 + 0.25 * jax.random.normal(weight_keys[1], (Q_RANK,), jnp.float32),
        'w_uq': weight(weight_keys[2], (Q_RANK, NUM_HEADS * NOPE_DIM), Q_RANK, 1.5),
        'w_qr': weight(weight_keys[3], (Q_RANK, NUM_HEADS * ROPE_DIM), Q_RANK, 1.5),
        'w_dkv': weight(weight_keys[4], (HIDDEN, KV_RANK), HIDDEN, 1.0),
        'gain_kv': 1.0 + 0.25 * jax.random.normal(weight_keys[5], (KV_RANK,), jnp.float32),
        'w_kr': weight(weight_keys[6], (HIDDEN, ROPE_DIM), HIDDEN, 1.0),
        'w_uk': weight(weight_keys[7], (KV_RANK, NUM_HEADS * NOPE_DIM), KV_RANK, 1.0),
        'w_uv': weight(weight_keys[8], (KV_RANK, NUM_HEADS * V_DIM), KV_RANK, 1.0),
        'w_out': weight(weight_keys[9], (NUM_HEADS * V_DIM, HIDDEN), NUM_HEADS * V_DIM, 1.0),
    }


def reference(x_tokens, positions, w_dq, gain_q, w_uq, w_qr, w_dkv, gain_kv, w_kr, w_uk, w_uv, w_out):
    c_q = rms_norm(jnp.dot(x_tokens, w_dq, preferred_element_type=jnp.float32), gain_q)
    c_kv = rms_norm(jnp.dot(x_tokens, w_dkv, preferred_element_type=jnp.float32), gain_kv)
    k_rope = apply_rope(jnp.dot(x_tokens, w_kr, preferred_element_type=jnp.float32), positions).astype(jnp.bfloat16)
    per_head = (
        w_uq.reshape(Q_RANK, NUM_HEADS, NOPE_DIM).transpose(1, 0, 2),
        w_qr.reshape(Q_RANK, NUM_HEADS, ROPE_DIM).transpose(1, 0, 2),
        w_uk.reshape(KV_RANK, NUM_HEADS, NOPE_DIM).transpose(1, 0, 2),
        w_uv.reshape(KV_RANK, NUM_HEADS, V_DIM).transpose(1, 0, 2),
        w_out.reshape(NUM_HEADS, V_DIM, HIDDEN),
    )
    score_scale = (NOPE_DIM + ROPE_DIM) ** -0.5
    num_blocks = SEQ_LEN // QUERY_BLOCK
    query_pos = positions.reshape(num_blocks, QUERY_BLOCK)

    def head_step(y_acc, head_w):
        w_uq_h, w_qr_h, w_uk_h, w_uv_h, w_out_h = head_w
        q_nope = jnp.dot(c_q, w_uq_h, preferred_element_type=jnp.float32).astype(jnp.bfloat16)
        q_rope = apply_rope(jnp.dot(c_q, w_qr_h, preferred_element_type=jnp.float32), positions).astype(jnp.bfloat16)
        k_nope = jnp.dot(c_kv, w_uk_h, preferred_element_type=jnp.float32).astype(jnp.bfloat16)
        v_full = jnp.dot(c_kv, w_uv_h, preferred_element_type=jnp.float32).astype(jnp.bfloat16).astype(jnp.float32)

        def query_block(blk_in):
            qn_blk, qr_blk, qpos_blk = blk_in
            scores = (jnp.dot(qn_blk, k_nope.T, preferred_element_type=jnp.float32) + jnp.dot(qr_blk, k_rope.T, preferred_element_type=jnp.float32)) * score_scale
            allowed = positions[None, :] <= qpos_blk[:, None]
            weights = jax.nn.softmax(jnp.where(allowed, scores, -jnp.inf), axis=-1)
            return jnp.dot(weights, v_full).astype(jnp.bfloat16)

        out_head = lax.map(query_block, (q_nope.reshape(num_blocks, QUERY_BLOCK, NOPE_DIM), q_rope.reshape(num_blocks, QUERY_BLOCK, ROPE_DIM), query_pos)).reshape(SEQ_LEN, V_DIM)
        return y_acc + jnp.dot(out_head, w_out_h, preferred_element_type=jnp.float32), None

    y_acc = lax.scan(head_step, jnp.zeros((SEQ_LEN, HIDDEN), jnp.float32), per_head)[0]
    return y_acc.astype(jnp.bfloat16)
```

```python
import functools

import jax
import jax.numpy as jnp
import numpy as np
from jax import lax
from jax.experimental import pallas as pl
from jax.experimental.pallas import tpu as pltpu
from jax.sharding import PartitionSpec as P

MESH = pl.DeviceIdType.MESH
F32 = jnp.float32
BF16 = jnp.bfloat16

HIDDEN = 2560
Q_RANK = 768
KV_RANK = 256
HEADS = 10
PAIRS = HEADS // 2
NOPE = 64
ROPE = 32
VDIM = 64
ROWS = 512
SPAN = 256
NSPAN = 8
CTX = 4
MODEL = 4
HV = HEADS * VDIM
NHALF = HIDDEN // 2
QROWS = HV // 4
KRP = SPAN // 8
EPS = 1e-6
ROPE_BASE = 10000.0
SM_SCALE = float((NOPE + ROPE) ** -0.5 * np.log2(np.e))
NEG = -1e30


def dot(a, b):
    return jnp.dot(a, b, preferred_element_type=F32)


def dot_nt(a, b):
    return lax.dot_general(a, b, (((1,), (1,)), ((), ())), preferred_element_type=F32)


def rms(h, gain):
    ms = jnp.mean(h * h, axis=-1, keepdims=True)
    return (h * lax.rsqrt(ms + EPS) * gain).astype(BF16)


def kernel(x_h, pos_r, freq_r, gq_r, gkv_r, wdq_h, wuq_h, wqr_h, wdkv_h, wkr_h, wuk_h, wuv_h, wout_h, out_h,
           x_v, wdq_v, wuq_v, wqr_v, wdkv_v, wkr_v, wkr4_v, wuk_v, wuv_v,
           cos_v, sin_v, tile_v, lat_v, cq_v, qm_v, k_v, v_v, kr_v, s_v, mx_v, mb_v, l_v, acc_v,
           os_v, oall_v, wall_v, yst_v,
           lsem, kv_ssem, kv_rsem, wz_own, wz_ssem, wz_rsem, wy_ssem, wy_rsem, wd_ssem, wd_rsem,
           oz_ssem, oz_rsem, ox_ssem, ox_rsem, yb_ssem, yb_rsem, yl_sem):
    dp = lax.axis_index('dp')
    z = lax.axis_index('model')
    ctx = lax.axis_index('ctx')
    partner = ctx + 1 - 2 * lax.rem(ctx, 2)
    ynbr = lax.rem(ctx + 2, CTX)
    diag = lax.rem(partner + 2, CTX)
    xn = 1 - dp

    def dev(d=None, m=None, c=None):
        return (dp if d is None else d, z if m is None else m, ctx if c is None else c)

    def remote(src, dst, ss, rs, where):
        return pltpu.make_async_remote_copy(src_ref=src, dst_ref=dst, send_sem=ss, recv_sem=rs,
                                            device_id=where, device_id_type=MESH)

    def local(src, dst, idx):
        return pltpu.make_async_copy(src, dst, lsem.at[idx])

    loads = [
        local(wkr_h, wkr_v, 0),
        local(x_h.at[pl.ds(0, SPAN)], x_v.at[pl.ds(0, SPAN)], 1),
        local(wdkv_h, wdkv_v, 2),
        local(x_h.at[pl.ds(SPAN, SPAN)], x_v.at[pl.ds(SPAN, SPAN)], 3),
        local(wdq_h, wdq_v, 4),
        local(wuq_h, wuq_v, 5),
        local(wqr_h, wqr_v, 6),
        local(wuk_h, wuk_v, 7),
        local(wuv_h, wuv_v, 8),
        local(wout_h.at[:, pl.ds(pl.multiple_of(dp * NHALF, 128), NHALF)], wall_v.at[z], 9),
    ]
    for c in loads:
        c.start()

    barrier = pltpu.get_barrier_semaphore()
    peers = [dev(m=lax.rem(z + d, MODEL)) for d in (1, 2, 3)] + [dev(d=xn), dev(c=partner), dev(c=ynbr)]
    for p in peers:
        pl.semaphore_signal(barrier, inc=1, device_id=p, device_id_type=MESH)
    pl.semaphore_wait(barrier, len(peers))

    def wpiece(s, c):
        return wall_v.at[s, pl.ds(pl.multiple_of(c * QROWS, 16), QROWS)]

    wout_src = wout_h.at[pl.ds(pl.multiple_of(ctx * QROWS, 16), QROWS), pl.ds(pl.multiple_of(dp * NHALF, 128), NHALF)]

    def w_own(up):
        return remote(wout_src, wpiece(z, ctx), wz_own.at[up], wz_rsem.at[z], dev(m=z + 2 * up - 1))

    def w_fwd_z(s, to):
        return remote(wpiece(s, ctx), wpiece(s, ctx), wz_ssem.at[s], wz_rsem.at[s], dev(m=to))

    def w_fwd_y(s):
        return remote(wpiece(s, ctx), wpiece(s, ctx), wy_ssem.at[s], wy_rsem.at[s], dev(c=ynbr))

    def w_fwd_d(s, which):
        c = ctx if which == 0 else ynbr
        return remote(wpiece(s, c), wpiece(s, c), wd_ssem.at[s, which], wd_rsem.at[s, which], dev(c=partner))

    def wait_wz(s):
        remote(wpiece(s, ctx), wpiece(s, ctx), wz_ssem.at[s], wz_rsem.at[s], dev()).wait_recv()

    def wait_wy(s):
        remote(wpiece(s, ynbr), wpiece(s, ynbr), wy_ssem.at[s], wy_rsem.at[s], dev()).wait_recv()

    def wait_wd(s, which):
        c = partner if which == 0 else diag
        remote(wpiece(s, c), wpiece(s, c), wd_ssem.at[s, which], wd_rsem.at[s, which], dev()).wait_recv()

    @pl.when(z < MODEL - 1)
    def _():
        w_own(1).start()

    @pl.when(z > 0)
    def _():
        w_own(0).start()

    def each_share(j, fn):
        for sign in (-1, 1):
            s = z + sign * j

            @pl.when((s >= 0) & (s < MODEL))
            def _(s=s, sign=sign):
                fn(s, sign)

    def w_hop(j):
        def step(s, sign):
            wait_wz(s)
            to = z - sign

            @pl.when((to >= 0) & (to < MODEL))
            def _():
                w_fwd_z(s, to).start()
            w_fwd_y(s).start()
            w_fwd_d(s, 0).start()
        each_share(j, step)

    def w_across(j):
        def step(s, sign):
            wait_wy(s)
            w_fwd_d(s, 1).start()
        each_share(j, step)

    lane = lax.broadcasted_iota(jnp.int32, (1, 128), 1)
    for g in range(ROWS // 128):
        row = pos_r[:, pl.ds(128 * g, 128)].astype(F32)
        col = jnp.transpose(jnp.broadcast_to(row, (128, 128)), (1, 0))
        ang = col * freq_r[...]
        cos_v[pl.ds(128 * g, 128), :] = jnp.cos(ang)
        sin_v[pl.ds(128 * g, 128), :] = jnp.sin(ang)
    rr = lax.broadcasted_iota(jnp.int32, (KV_RANK, 1024), 0)
    cc = lax.broadcasted_iota(jnp.int32, (KV_RANK, 1024), 1)
    tile_v[...] = jnp.where((rr // ROPE == cc // 128) & (rr % ROPE == cc % ROPE), 1.0, 0.0).astype(BF16)
    low = (lane % ROPE) < (ROPE // 2)

    def rope(v, r0):
        up = pltpu.roll(v, 128 - ROPE // 2, 1)
        dn = pltpu.roll(v, ROPE // 2, 1)
        rot = jnp.where(low, -up, dn)
        return v * cos_v[pl.ds(r0, SPAN), :] + rot * sin_v[pl.ds(r0, SPAN), :]

    loads[0].wait()
    t_r = lax.broadcasted_iota(jnp.int32, (ROPE, 128), 0)
    t_c = lax.broadcasted_iota(jnp.int32, (ROPE, 128), 1)
    rep = jnp.where(t_r == t_c % ROPE, 1.0, 0.0).astype(BF16)
    wkr4_v[...] = dot(wkr_v[...], rep).astype(BF16)
    for t in range(2):
        r0 = t * SPAN
        if t == 0:
            loads[1].wait()
            loads[2].wait()
        else:
            loads[3].wait()
        xs = x_v[pl.ds(r0, SPAN), :]
        lat_v[ctx, t, pl.ds(0, SPAN), :] = rms(dot(xs, wdkv_v[...]), gkv_r[...])
        kr = rope(dot(xs, wkr4_v[...]), r0)
        for half in range(2):
            packed = kr[128 * half:128 * half + KRP]
            for g in range(1, 4):
                a = 128 * half + KRP * g
                packed = jnp.where(lane // ROPE == g, kr[a:a + KRP], packed)
            lat_v[ctx, t, pl.ds(SPAN, KRP), pl.ds(128 * half, 128)] = packed.astype(BF16)

    def kv_copy(c, idx, to):
        return remote(lat_v.at[c], lat_v.at[c], kv_ssem.at[idx], kv_rsem.at[idx], dev(c=to))

    kv_copy(ctx, 0, ynbr).start()
    kv_copy(ctx, 1, partner).start()

    loads[4].wait()
    for t in range(2):
        cq_v[pl.ds(t * SPAN, SPAN), :] = rms(dot(x_v[pl.ds(t * SPAN, SPAN), :], wdq_v[...]), gq_r[...])
    loads[5].wait()
    loads[6].wait()
    for t in range(2):
        cq = cq_v[pl.ds(t * SPAN, SPAN), :]
        qn = dot(cq, wuq_v[...]).astype(BF16)
        zero = jnp.zeros((SPAN, 128), BF16)
        for p in range(PAIRS):
            blk = qn[:, 128 * p:128 * p + 128]
            qm_v[p, t, pl.ds(0, SPAN), pl.ds(0, 128)] = jnp.where(lane < NOPE, blk, zero)
            qm_v[p, t, pl.ds(SPAN, SPAN), pl.ds(0, 128)] = jnp.where(lane < NOPE, zero, blk)
        for b in range(3):
            w = wqr_v[:, pl.ds(128 * b, 128)] if b < 2 else jnp.concatenate([wqr_v[:, pl.ds(256, 64)]] * 2, axis=1)
            qr = rope(dot(cq, w), t * SPAN).astype(BF16)
            for h in range(4 * b, min(4 * b + 4, HEADS)):
                qm_v[h // 2, t, pl.ds(SPAN * (h % 2), SPAN), pl.ds(128, 128)] = jnp.where(lane // ROPE == h % 4, qr, zero)

    def up(c):
        for t in range(2):
            sp = c if t == 0 else NSPAN - 1 - c
            lat = lat_v[c, t, pl.ds(0, SPAN), :]
            k_v[sp] = dot(lat, wuk_v[...]).astype(BF16)
            v_v[sp] = dot(lat, wuv_v[...]).astype(BF16)
            big = dot(lat_v[c, t, pl.ds(SPAN, KRP), :], tile_v[...]).astype(BF16)
            for g in range(8):
                kr_v[sp, pl.ds(KRP * g, KRP), :] = big[:, 128 * g:128 * g + 128]

    loads[7].wait()
    loads[8].wait()
    up(ctx)
    kv_copy(partner, 1, ctx).wait_recv()
    up(partner)
    kv_copy(ynbr, 0, ctx).wait_recv()
    kv_copy(ynbr, 2, partner).start()
    up(ynbr)
    w_hop(1)
    kv_copy(diag, 2, ctx).wait_recv()
    up(diag)

    def block(b):
        if b < 5:
            return 1, NSPAN - 1 - ctx - b
        if b == 8:
            return 0, ctx
        hi = b < NSPAN - ctx
        return jnp.where(hi, 1, 0), jnp.where(hi, NSPAN - 1 - ctx - b, b - (NSPAN - ctx))

    ORDER = (0, 8, 1, 2, 3, 4, 5, 6, 7)
    q_i = lax.broadcasted_iota(jnp.int32, (SPAN, SPAN), 0)
    k_i = lax.broadcasted_iota(jnp.int32, (SPAN, SPAN), 1)
    causal = k_i <= q_i

    def scores(p, b):
        buf = p % 2
        qs, ks = block(b)
        kc = jnp.concatenate([k_v[ks, :, pl.ds(128 * p, 128)], kr_v[ks]], axis=1)
        for a in range(2):
            rows = pl.ds(SPAN * a, SPAN)
            s = dot_nt(qm_v[p, qs, rows, :], kc)
            if b in (0, 8):
                s = jnp.where(causal, s, NEG)
            s_v[buf, b, rows, :] = s
            m = jnp.maximum(s[:, :128], s[:, 128:])
            if b not in (0, 8):
                m = jnp.maximum(mx_v[buf, qs, rows, :], m)
            mx_v[buf, qs, rows, :] = m

    def maxima(p):
        buf = p % 2
        for qs in range(2):
            for a in range(2):
                rows = pl.ds(SPAN * a, SPAN)
                m = jnp.max(mx_v[buf, qs, rows, :], axis=1, keepdims=True)
                mb_v[qs, rows, :] = jnp.broadcast_to(m * SM_SCALE, (SPAN, 128))

    def values(p, b):
        buf = p % 2
        qs, ks = block(b)
        vb = v_v[ks, :, pl.ds(128 * p, 128)]
        for a in range(2):
            rows = pl.ds(SPAN * a, SPAN)
            m = mb_v[qs, rows, :]
            e0 = jnp.exp2(s_v[buf, b, rows, pl.ds(0, 128)] * SM_SCALE - m)
            e1 = jnp.exp2(s_v[buf, b, rows, pl.ds(128, 128)] * SM_SCALE - m)
            pv = dot(jnp.concatenate([e0.astype(BF16), e1.astype(BF16)], axis=1), vb)
            l = e0 + e1
            if b in (0, 8):
                l_v[qs, rows, :] = l
                acc_v[qs, rows, :] = pv
            else:
                l_v[qs, rows, :] += l
                acc_v[qs, rows, :] += pv

    def finish(p):
        for qs in range(2):
            o = []
            for a in range(2):
                rows = pl.ds(SPAN * a, SPAN)
                l = jnp.sum(l_v[qs, rows, :], axis=1, keepdims=True)
                o.append(acc_v[qs, rows, :] / l)
            both = jnp.where(lane < VDIM, o[0], o[1]).astype(BF16)
            os_v[p, 2 * qs] = both[:128]
            os_v[p, 2 * qs + 1] = both[128:]

    def o_z(p, d):
        to = lax.rem(z + d, MODEL)
        return remote(os_v.at[p, to], oall_v.at[dp, z, :, pl.ds(128 * p, 128)],
                      oz_ssem.at[p, d - 1], oz_rsem.at[p, d - 1], dev(m=to))

    def o_z_wait(p, d):
        src = lax.rem(z + MODEL - d, MODEL)
        remote(os_v.at[p, z], oall_v.at[dp, src, :, pl.ds(128 * p, 128)],
               oz_ssem.at[p, d - 1], oz_rsem.at[p, d - 1], dev()).wait_recv()

    def o_x(p, src_dp, to):
        part = oall_v.at[src_dp, :, :, pl.ds(128 * p, 128)]
        return remote(part, part, ox_ssem.at[p], ox_rsem.at[p], dev(d=to))

    def send_o(p):
        oall_v[dp, z, :, pl.ds(128 * p, 128)] = os_v[p, z]
        for d in (1, 2, 3):
            o_z(p, d).start()

    def pass_o(p):
        for d in (1, 2, 3):
            o_z_wait(p, d)
        o_x(p, dp, xn).start()

    for b in ORDER:
        scores(0, b)
    maxima(0)
    for p in range(PAIRS):
        for b in ORDER:
            if p + 1 < PAIRS:
                scores(p + 1, b)
            values(p, b)
        finish(p)
        if p + 1 < PAIRS:
            maxima(p + 1)
        send_o(p)
        if p >= 1:
            pass_o(p - 1)
        if p == 2:
            w_across(1)
            w_hop(2)
    w_across(2)
    w_hop(3)
    pass_o(PAIRS - 1)
    w_across(3)
    for j in (1, 2, 3):
        each_share(j, lambda s, sign: (wait_wd(s, 0), wait_wd(s, 1)))
    loads[9].wait()
    for p in range(PAIRS):
        o_x(p, xn, dp).wait_recv()

    def y_back():
        return remote(yst_v.at[0], out_h.at[:, pl.ds(pl.multiple_of(dp * NHALF, 128), NHALF)],
                      yb_ssem, yb_rsem, dev(d=xn))

    def y_local():
        return pltpu.make_async_copy(yst_v.at[1], out_h.at[:, pl.ds(pl.multiple_of(dp * NHALF, 128), NHALF)], yl_sem)

    for which in range(2):
        blk = xn if which == 0 else dp
        for n in range(NHALF // 256):
            cols = pl.ds(256 * n, 256)
            y = dot(oall_v[blk, 0], wall_v[0, :, cols])
            for s in range(1, MODEL):
                y = y + dot(oall_v[blk, s], wall_v[s, :, cols])
            yst_v[which, :, cols] = y.astype(BF16)
        if which == 0:
            y_back().start()
    y_local().start()

    kv_copy(ctx, 0, ynbr).wait_send()
    kv_copy(ctx, 1, partner).wait_send()
    kv_copy(ynbr, 2, partner).wait_send()

    @pl.when(z < MODEL - 1)
    def _():
        w_own(1).wait_send()

    @pl.when(z > 0)
    def _():
        w_own(0).wait_send()

    def sent(s, sign):
        to = z - sign

        @pl.when((to >= 0) & (to < MODEL))
        def _():
            w_fwd_z(s, to).wait_send()
        w_fwd_y(s).wait_send()
        w_fwd_d(s, 0).wait_send()
        w_fwd_d(s, 1).wait_send()

    for j in (1, 2, 3):
        each_share(j, sent)
    for p in range(PAIRS):
        for d in (1, 2, 3):
            o_z(p, d).wait_send()
        o_x(p, dp, xn).wait_send()
    y_back().wait_send()
    remote(yst_v.at[0], out_h.at[:, pl.ds(pl.multiple_of(xn * NHALF, 128), NHALF)], yb_ssem, yb_rsem, dev()).wait_recv()
    y_local().wait()


def layer(x, pos, freq, wdq, gq, wuq, wqr, wdkv, gkv, wkr, wuk, wuv, wout):
    vm = pl.BlockSpec(memory_space=pltpu.VMEM)
    hb = pl.BlockSpec(memory_space=pl.ANY)
    dma = pltpu.SemaphoreType.DMA
    return pl.pallas_call(
        kernel,
        out_shape=jax.ShapeDtypeStruct((ROWS // MODEL, HIDDEN), BF16),
        in_specs=[hb, vm, vm, vm, vm] + [hb] * 8,
        out_specs=hb,
        scratch_shapes=[
            pltpu.VMEM((ROWS, HIDDEN), BF16),
            pltpu.VMEM((HIDDEN, Q_RANK), BF16),
            pltpu.VMEM((Q_RANK, HEADS * NOPE), BF16),
            pltpu.VMEM((Q_RANK, HEADS * ROPE), BF16),
            pltpu.VMEM((HIDDEN, KV_RANK), BF16),
            pltpu.VMEM((HIDDEN, ROPE), BF16),
            pltpu.VMEM((HIDDEN, 128), BF16),
            pltpu.VMEM((KV_RANK, HEADS * NOPE), BF16),
            pltpu.VMEM((KV_RANK, HEADS * VDIM), BF16),
            pltpu.VMEM((ROWS, 128), F32),
            pltpu.VMEM((ROWS, 128), F32),
            pltpu.VMEM((KV_RANK, 1024), BF16),
            pltpu.VMEM((CTX, 2, SPAN + KRP, KV_RANK), BF16),
            pltpu.VMEM((ROWS, Q_RANK), BF16),
            pltpu.VMEM((PAIRS, 2, 2 * SPAN, 256), BF16),
            pltpu.VMEM((NSPAN, SPAN, HEADS * NOPE), BF16),
            pltpu.VMEM((NSPAN, SPAN, HEADS * VDIM), BF16),
            pltpu.VMEM((NSPAN, SPAN, 128), BF16),
            pltpu.VMEM((2, 9, 2 * SPAN, SPAN), F32),
            pltpu.VMEM((2, 2, 2 * SPAN, 128), F32),
            pltpu.VMEM((2, 2 * SPAN, 128), F32),
            pltpu.VMEM((2, 2 * SPAN, 128), F32),
            pltpu.VMEM((2, 2 * SPAN, 128), F32),
            pltpu.VMEM((PAIRS, MODEL, 128, 128), BF16),
            pltpu.VMEM((2, MODEL, 128, HV), BF16),
            pltpu.VMEM((MODEL, HV, NHALF), BF16),
            pltpu.VMEM((2, 128, NHALF), BF16),
            dma((10,)),
            dma((3,)), dma((3,)),
            dma((2,)), dma((MODEL,)), dma((MODEL,)),
            dma((MODEL,)), dma((MODEL,)),
            dma((MODEL, 2)), dma((MODEL, 2)),
            dma((PAIRS, 3)), dma((PAIRS, 3)),
            dma((PAIRS,)), dma((PAIRS,)),
            dma, dma, dma,
        ],
        compiler_params=pltpu.CompilerParams(collective_id=0, has_side_effects=True, vmem_limit_bytes=60 * 1024 * 1024),
        name='mla_layer',
    )(x, pos, freq, gq, gkv, wdq, wuq, wqr, wdkv, wkr, wuk, wuv, wout)


def solution(mesh):
    inv_freq = (ROPE_BASE ** (-(np.arange(ROPE // 2, dtype=np.float64) * 2.0 / ROPE))).astype(np.float32)
    freq = np.tile(inv_freq, 128 // (ROPE // 2))[None, :]

    def local(x_tokens, positions, w_dq, gain_q, w_uq, w_qr, w_dkv, gain_kv, w_kr, w_uk, w_uv, w_out):
        return layer(x_tokens, positions[None, :], jnp.asarray(freq), w_dq, gain_q[None, :], w_uq, w_qr, w_dkv,
                     gain_kv[None, :], w_kr, w_uk, w_uv, w_out)

    in_specs = (P(('dp', 'ctx'), None), P(('dp', 'ctx')), P(), P(), P(None, 'model'), P(None, 'model'), P(), P(), P(), P(None, 'model'), P(None, 'model'), P('model', None))
    out_specs = P(('dp', 'ctx', 'model'), None)
    return jax.shard_map(local, mesh=mesh, in_specs=in_specs, out_specs=out_specs, check_vma=False)
```

```python
import functools

import jax
import jax.numpy as jnp
import numpy as np
from jax import lax
from jax.experimental import pallas as pl
from jax.experimental.pallas import tpu as pltpu
from jax.sharding import PartitionSpec as P

MESH = pl.DeviceIdType.MESH
F32 = jnp.float32
BF16 = jnp.bfloat16

HIDDEN = 2560
Q_RANK = 768
KV_RANK = 256
HEADS = 10
PAIRS = HEADS // 2
NOPE = 64
ROPE = 32
VDIM = 64
ROWS = 512
SPAN = 256
NSPAN = 8
CTX = 4
MODEL = 4
HV = HEADS * VDIM
NHALF = HIDDEN // 2
QROWS = HV // 4
NSUB = 5
SUBC = NHALF // NSUB
KRP = SPAN // 8
EPS = 1e-6
ROPE_BASE = 10000.0
SM_SCALE = float((NOPE + ROPE) ** -0.5 * np.log2(np.e))
NEG = -1e30


def dot(a, b):
    return jnp.dot(a, b, preferred_element_type=F32)


def dot_nt(a, b):
    return lax.dot_general(a, b, (((1,), (1,)), ((), ())), preferred_element_type=F32)


def rms(h, gain):
    ms = jnp.mean(h * h, axis=-1, keepdims=True)
    return (h * lax.rsqrt(ms + EPS) * gain).astype(BF16)


def kernel(x_h, pos_h, freq_h, gq_h, gkv_h, wdq_h, wuq_h, wqr_h, wdkv_h, wkr_h, wuk_h, wuv_h, wout_h, out_h,
           pos_r, freq_r, gq_r, gkv_r, x_v, wdq_v, wuq_v, wqr_v, wdkv_v, wkr_v, wuk_v, wuv_v,
           cos_v, sin_v, tile_v, lat_v, cq_v, qm_v, k_v, v_v, kr_v, s_v, mx_v, mb_v, l_v, acc_v,
           os_v, oall_v, wall_v, yst_v,
           lsem, kv_ssem, kv_rsem, wz_own, wz_ssem, wz_rsem, wy_ssem, wy_rsem, wd_ssem, wd_rsem,
           oz_ssem, oz_rsem, ox_ssem, ox_rsem, yb_ssem, yb_rsem, yl_sem):
    dp = lax.axis_index('dp')
    z = lax.axis_index('model')
    ctx = lax.axis_index('ctx')
    partner = ctx + 1 - 2 * lax.rem(ctx, 2)
    ynbr = lax.rem(ctx + 2, CTX)
    diag = lax.rem(partner + 2, CTX)
    xn = 1 - dp

    def dev(d=None, m=None, c=None):
        return (dp if d is None else d, z if m is None else m, ctx if c is None else c)

    def remote(src, dst, ss, rs, where):
        return pltpu.make_async_remote_copy(src_ref=src, dst_ref=dst, send_sem=ss, recv_sem=rs,
                                            device_id=where, device_id_type=MESH)

    def local(src, dst, idx):
        return pltpu.make_async_copy(src, dst, lsem.at[idx])

    small = [local(pos_h, pos_r, 10), local(freq_h, freq_r, 11), local(gq_h, gq_r, 12), local(gkv_h, gkv_r, 13)]
    loads = [
        local(wkr_h, wkr_v, 0),
        local(x_h.at[pl.ds(0, SPAN)], x_v.at[pl.ds(0, SPAN)], 1),
        local(wdkv_h, wdkv_v, 2),
        local(x_h.at[pl.ds(SPAN, SPAN)], x_v.at[pl.ds(SPAN, SPAN)], 3),
        local(wdq_h, wdq_v, 4),
        local(wuq_h, wuq_v, 5),
        local(wqr_h, wqr_v, 6),
        local(wuk_h, wuk_v, 7),
        local(wuv_h, wuv_v, 8),
        local(wout_h.at[:, pl.ds(pl.multiple_of(dp * NHALF, 128), NHALF)], wall_v.at[z], 9),
    ]
    for c in small + loads:
        c.start()

    barrier = pltpu.get_barrier_semaphore()
    peers = [dev(m=lax.rem(z + d, MODEL)) for d in (1, 2, 3)] + [dev(d=xn), dev(c=partner), dev(c=ynbr)]
    for p in peers:
        pl.semaphore_signal(barrier, inc=1, device_id=p, device_id_type=MESH)
    pl.semaphore_wait(barrier, len(peers))

    def wpiece(s, c, n=None):
        rows = pl.ds(pl.multiple_of(c * QROWS, 16), QROWS)
        return wall_v.at[s, rows] if n is None else wall_v.at[s, rows, pl.ds(SUBC * n, SUBC)]

    def wsrc(n=None):
        rows = pl.ds(pl.multiple_of(ctx * QROWS, 16), QROWS)
        c0 = dp * NHALF + (0 if n is None else SUBC * n)
        return wout_h.at[rows, pl.ds(pl.multiple_of(c0, 128), NHALF if n is None else SUBC)]

    def w_own(up, n=None):
        return remote(wsrc(n), wpiece(z, ctx, n), wz_own.at[up], wz_rsem.at[z, n or 0], dev(m=z + 2 * up - 1))

    def w_fwd_z(s, to, n=None):
        return remote(wpiece(s, ctx, n), wpiece(s, ctx, n), wz_ssem.at[s], wz_rsem.at[s, n or 0], dev(m=to))

    def w_fwd_y(s, n=None):
        return remote(wpiece(s, ctx, n), wpiece(s, ctx, n), wy_ssem.at[s], wy_rsem.at[s, n or 0], dev(c=ynbr))

    def w_fwd_d(s, which, n=None):
        c = ctx if which == 0 else ynbr
        return remote(wpiece(s, c, n), wpiece(s, c, n), wd_ssem.at[s, which], wd_rsem.at[s, which, n or 0], dev(c=partner))

    def wait_wz(s, n):
        remote(wpiece(s, ctx, n), wpiece(s, ctx, n), wz_ssem.at[s], wz_rsem.at[s, n], dev()).wait_recv()

    def wait_wy(s, n):
        remote(wpiece(s, ynbr, n), wpiece(s, ynbr, n), wy_ssem.at[s], wy_rsem.at[s, n], dev()).wait_recv()

    def wait_wd(s, which, n):
        c = partner if which == 0 else diag
        remote(wpiece(s, c, n), wpiece(s, c, n), wd_ssem.at[s, which], wd_rsem.at[s, which, n], dev()).wait_recv()

    @pl.when(z < MODEL - 1)
    def _():
        for n in range(NSUB):
            w_own(1, n).start()

    @pl.when(z > 0)
    def _():
        for n in range(NSUB):
            w_own(0, n).start()

    def each_share(j, fn):
        for sign in (-1, 1):
            s = z + sign * j

            @pl.when((s >= 0) & (s < MODEL))
            def _(s=s, sign=sign):
                fn(s, sign)

    def hop(q):
        j, n = q // NSUB + 1, q % NSUB

        def step(s, sign):
            wait_wz(s, n)
            to = z - sign

            @pl.when((to >= 0) & (to < MODEL))
            def _():
                w_fwd_z(s, to, n).start()
            w_fwd_y(s, n).start()
            w_fwd_d(s, 0, n).start()
        each_share(j, step)

    def across(q):
        j, n = q // NSUB + 1, q % NSUB

        def step(s, sign):
            wait_wy(s, n)
            w_fwd_d(s, 1, n).start()
        each_share(j, step)

    lane = lax.broadcasted_iota(jnp.int32, (1, 128), 1)
    for c in small:
        c.wait()
    for g in range(ROWS // 128):
        row = pos_r[:, pl.ds(128 * g, 128)].astype(F32)
        col = jnp.transpose(jnp.broadcast_to(row, (128, 128)), (1, 0))
        ang = col * freq_r[...]
        cos_v[pl.ds(128 * g, 128), :] = jnp.cos(ang)
        sin_v[pl.ds(128 * g, 128), :] = jnp.sin(ang)
    rr = lax.broadcasted_iota(jnp.int32, (KV_RANK, 1024), 0)
    cc = lax.broadcasted_iota(jnp.int32, (KV_RANK, 1024), 1)
    tile_v[...] = jnp.where((rr // ROPE == cc // 128) & (rr % ROPE == cc % ROPE), 1.0, 0.0).astype(BF16)
    low = (lane % ROPE) < (ROPE // 2)

    def rope(v, r0):
        up = pltpu.roll(v, 128 - ROPE // 2, 1)
        dn = pltpu.roll(v, ROPE // 2, 1)
        rot = jnp.where(low, -up, dn)
        return v * cos_v[pl.ds(r0, SPAN), :] + rot * sin_v[pl.ds(r0, SPAN), :]

    def kv_copy(c, t, idx, to):
        return remote(lat_v.at[c, t], lat_v.at[c, t], kv_ssem.at[idx, t], kv_rsem.at[idx, t], dev(c=to))

    loads[0].wait()
    wkr4 = jnp.concatenate([wkr_v[...]] * 4, axis=0)
    gkv = gkv_r[...]
    for t in range(2):
        r0 = t * SPAN
        if t == 0:
            loads[1].wait()
            loads[2].wait()
        else:
            loads[3].wait()
        xs = x_v[pl.ds(r0, SPAN), :]
        lat_v[ctx, t, pl.ds(0, SPAN), :] = rms(dot(xs, wdkv_v[...]), gkv)
        kr = rope(dot_nt(xs, wkr4), r0)
        for half in range(2):
            packed = kr[128 * half:128 * half + KRP]
            for g in range(1, 4):
                a = 128 * half + KRP * g
                packed = jnp.where(lane // ROPE == g, kr[a:a + KRP], packed)
            lat_v[ctx, t, pl.ds(SPAN, KRP), pl.ds(128 * half, 128)] = packed.astype(BF16)
        if t == 0:
            kv_copy(ctx, t, 0, ynbr).start()
        else:
            @pl.when(ctx >= 2)
            def _():
                kv_copy(ctx, 1, 0, ynbr).start()
        kv_copy(ctx, t, 1, partner).start()

    loads[4].wait()
    gq = jnp.concatenate([gq_r[g:g + 1, :] for g in range(Q_RANK // 128)], axis=1)
    for t in range(2):
        cq_v[pl.ds(t * SPAN, SPAN), :] = rms(dot(x_v[pl.ds(t * SPAN, SPAN), :], wdq_v[...]), gq)
    hop(0)
    loads[5].wait()
    loads[6].wait()
    for t in range(2):
        cq = cq_v[pl.ds(t * SPAN, SPAN), :]
        qn = dot(cq, wuq_v[...]).astype(BF16)
        zero = jnp.zeros((SPAN, 128), BF16)
        for p in range(PAIRS):
            blk = qn[:, 128 * p:128 * p + 128]
            qm_v[p, t, pl.ds(0, SPAN), pl.ds(0, 128)] = jnp.where(lane < NOPE, blk, zero)
            qm_v[p, t, pl.ds(SPAN, SPAN), pl.ds(0, 128)] = jnp.where(lane < NOPE, zero, blk)
        for b in range(3):
            w = wqr_v[pl.ds(128 * b, 128), :] if b < 2 else jnp.concatenate([wqr_v[pl.ds(256, 64), :]] * 2, axis=0)
            qr = rope(dot_nt(cq, w), t * SPAN).astype(BF16)
            for h in range(4 * b, min(4 * b + 4, HEADS)):
                qm_v[h // 2, t, pl.ds(SPAN * (h % 2), SPAN), pl.ds(128, 128)] = jnp.where(lane // ROPE == h % 4, qr, zero)

    hop(1)

    def up(c, t):
        sp = c if t == 0 else NSPAN - 1 - c
        lat = lat_v[c, t, pl.ds(0, SPAN), :]
        k_v[sp] = dot(lat, wuk_v[...]).astype(BF16)
        v_v[sp] = dot(lat, wuv_v[...]).astype(BF16)
        big = dot(lat_v[c, t, pl.ds(SPAN, KRP), :], tile_v[...]).astype(BF16)
        for g in range(8):
            kr_v[sp, pl.ds(KRP * g, KRP), :] = big[:, 128 * g:128 * g + 128]

    def up_late(c):
        @pl.when(c >= ctx)
        def _():
            up(c, 1)

    loads[7].wait()
    loads[8].wait()
    up(ctx, 0)
    up(ctx, 1)
    kv_copy(partner, 0, 1, ctx).wait_recv()
    kv_copy(partner, 1, 1, ctx).wait_recv()
    up(partner, 0)
    up_late(partner)
    hop(2)
    kv_copy(ynbr, 0, 0, ctx).wait_recv()
    kv_copy(ynbr, 0, 2, partner).start()
    up(ynbr, 0)

    @pl.when(ctx < 2)
    def _():
        kv_copy(ynbr, 1, 0, ctx).wait_recv()
        kv_copy(ynbr, 1, 2, partner).start()
        up(ynbr, 1)
    hop(3)
    across(0)
    kv_copy(diag, 0, 2, ctx).wait_recv()
    up(diag, 0)

    @pl.when(ctx < 2)
    def _():
        kv_copy(diag, 1, 2, ctx).wait_recv()
        up(diag, 1)
    hop(4)
    across(1)

    def block(b):
        if b < 5:
            return 1, NSPAN - 1 - ctx - b
        if b == 8:
            return 0, ctx
        hi = b < NSPAN - ctx
        return jnp.where(hi, 1, 0), jnp.where(hi, NSPAN - 1 - ctx - b, b - (NSPAN - ctx))

    ORDER = (0, 8, 1, 2, 3, 4, 5, 6, 7)
    q_i = lax.broadcasted_iota(jnp.int32, (SPAN, SPAN), 0)
    k_i = lax.broadcasted_iota(jnp.int32, (SPAN, SPAN), 1)
    causal = k_i <= q_i

    def scores(p, b):
        buf = p % 2
        qs, ks = block(b)
        kc = jnp.concatenate([k_v[ks, :, pl.ds(128 * p, 128)], kr_v[ks]], axis=1)
        for a in range(2):
            rows = pl.ds(SPAN * a, SPAN)
            s = dot_nt(qm_v[p, qs, rows, :], kc)
            if b in (0, 8):
                s = jnp.where(causal, s, NEG)
            s_v[buf, b, rows, :] = s
            m = jnp.maximum(s[:, :128], s[:, 128:])
            if b not in (0, 8):
                m = jnp.maximum(mx_v[buf, qs, rows, :], m)
            mx_v[buf, qs, rows, :] = m

    def maxima(p):
        buf = p % 2
        for qs in range(2):
            for a in range(2):
                rows = pl.ds(SPAN * a, SPAN)
                m = jnp.max(mx_v[buf, qs, rows, :], axis=1, keepdims=True)
                mb_v[qs, rows, :] = jnp.broadcast_to(m * SM_SCALE, (SPAN, 128))

    def values(p, b):
        buf = p % 2
        qs, ks = block(b)
        vb = v_v[ks, :, pl.ds(128 * p, 128)]
        for a in range(2):
            rows = pl.ds(SPAN * a, SPAN)
            m = mb_v[qs, rows, :]
            e0 = jnp.exp2(s_v[buf, b, rows, pl.ds(0, 128)] * SM_SCALE - m)
            e1 = jnp.exp2(s_v[buf, b, rows, pl.ds(128, 128)] * SM_SCALE - m)
            pv = dot(jnp.concatenate([e0.astype(BF16), e1.astype(BF16)], axis=1), vb)
            l = e0 + e1
            if b in (0, 8):
                l_v[qs, rows, :] = l
                acc_v[qs, rows, :] = pv
            else:
                l_v[qs, rows, :] += l
                acc_v[qs, rows, :] += pv

    def finish(p):
        for qs in range(2):
            o = []
            for a in range(2):
                rows = pl.ds(SPAN * a, SPAN)
                l = jnp.sum(l_v[qs, rows, :], axis=1, keepdims=True)
                o.append(acc_v[qs, rows, :] / l)
            both = jnp.where(lane < VDIM, o[0], o[1]).astype(BF16)
            os_v[p, 2 * qs] = both[:128]
            os_v[p, 2 * qs + 1] = both[128:]

    def o_z(p, d):
        to = lax.rem(z + d, MODEL)
        return remote(os_v.at[p, to], oall_v.at[dp, z, :, pl.ds(128 * p, 128)],
                      oz_ssem.at[p, d - 1], oz_rsem.at[p, d - 1], dev(m=to))

    def o_z_wait(p, d):
        src = lax.rem(z + MODEL - d, MODEL)
        remote(os_v.at[p, z], oall_v.at[dp, src, :, pl.ds(128 * p, 128)],
               oz_ssem.at[p, d - 1], oz_rsem.at[p, d - 1], dev()).wait_recv()

    def o_x(p, src_dp, to):
        part = oall_v.at[src_dp, :, :, pl.ds(128 * p, 128)]
        return remote(part, part, ox_ssem.at[p], ox_rsem.at[p], dev(d=to))

    def send_o(p):
        oall_v[dp, z, :, pl.ds(128 * p, 128)] = os_v[p, z]
        for d in (1, 2, 3):
            o_z(p, d).start()

    def pass_o(p):
        for d in (1, 2, 3):
            o_z_wait(p, d)
        o_x(p, dp, xn).start()

    for b in ORDER:
        scores(0, b)
    maxima(0)
    hop(5)
    across(2)
    relay = {
        0: lambda: (hop(6), across(3)),
        1: lambda: (hop(7), across(4), hop(8)),
        2: lambda: (across(5), hop(9), pass_o(0)),
        3: lambda: (across(6), hop(10), pass_o(1), across(7)),
        4: lambda: (hop(11), pass_o(2), across(8)),
    }
    for p in range(PAIRS):
        for b in ORDER:
            if p + 1 < PAIRS:
                scores(p + 1, b)
            values(p, b)
        finish(p)
        if p + 1 < PAIRS:
            maxima(p + 1)
        send_o(p)
        relay[p]()
    hop(12)
    across(9)
    pass_o(3)
    hop(13)
    across(10)
    pass_o(4)
    hop(14)
    loads[9].wait()

    for t in range(2):
        kv_copy(ctx, t, 1, partner).wait_send()
    kv_copy(ctx, 0, 0, ynbr).wait_send()
    kv_copy(ynbr, 0, 2, partner).wait_send()

    @pl.when(ctx >= 2)
    def _():
        kv_copy(ctx, 1, 0, ynbr).wait_send()

    @pl.when(ctx < 2)
    def _():
        kv_copy(ynbr, 1, 2, partner).wait_send()

    @pl.when(z < MODEL - 1)
    def _():
        w_own(1).wait_send()

    @pl.when(z > 0)
    def _():
        w_own(0).wait_send()

    for p in range(PAIRS):
        for d in (1, 2, 3):
            o_z(p, d).wait_send()
    across(11)
    across(12)
    for p in range(PAIRS):
        o_x(p, xn, dp).wait_recv()

    def ycols(half, n):
        return out_h.at[:, pl.ds(pl.multiple_of(half * NHALF + SUBC * n, 128), SUBC)]

    def y_back(n):
        return remote(yst_v.at[xn, n], ycols(dp, n), yb_ssem.at[n], yb_rsem.at[n], dev(d=xn))

    def y_come(n):
        return remote(yst_v.at[xn, n], ycols(xn, n), yb_ssem.at[n], yb_rsem.at[n], dev())

    def y_local(n):
        return pltpu.make_async_copy(yst_v.at[dp, n], ycols(dp, n), yl_sem.at[n])

    def final(n):
        for j in (1, 2, 3):
            each_share(j, lambda s, sign: (wait_wd(s, 0, n), wait_wd(s, 1, n)))
        cols = pl.ds(SUBC * n, SUBC)
        y = None
        for s in range(MODEL):
            o = jnp.concatenate([oall_v[0, s], oall_v[1, s]], axis=0)
            part = dot(o, wall_v[s, :, cols])
            y = part if y is None else y + part
        yst_v[0, n] = y[:128].astype(BF16)
        yst_v[1, n] = y[128:].astype(BF16)
        y_back(n).start()
        y_local(n).start()

    final(0)
    across(13)
    final(1)
    across(14)
    final(2)
    final(3)
    final(4)

    def sent(s, sign):
        to = z - sign

        @pl.when((to >= 0) & (to < MODEL))
        def _():
            w_fwd_z(s, to).wait_send()
        w_fwd_y(s).wait_send()
        w_fwd_d(s, 0).wait_send()
        w_fwd_d(s, 1).wait_send()

    for j in (1, 2, 3):
        each_share(j, sent)
    for p in range(PAIRS):
        o_x(p, dp, xn).wait_send()
    for n in range(NSUB):
        y_back(n).wait_send()
        y_local(n).wait()
        y_come(n).wait_recv()


def layer(x, pos, freq, wdq, gq, wuq, wqr, wdkv, gkv, wkr, wuk, wuv, wout):
    hb = pl.BlockSpec(memory_space=pl.ANY)
    dma = pltpu.SemaphoreType.DMA
    return pl.pallas_call(
        kernel,
        out_shape=jax.ShapeDtypeStruct((ROWS // MODEL, HIDDEN), BF16),
        in_specs=[hb] * 13,
        out_specs=hb,
        scratch_shapes=[
            pltpu.VMEM((1, ROWS), jnp.int32),
            pltpu.VMEM((1, 128), F32),
            pltpu.VMEM((Q_RANK // 128, 128), F32),
            pltpu.VMEM((1, KV_RANK), F32),
            pltpu.VMEM((ROWS, HIDDEN), BF16),
            pltpu.VMEM((HIDDEN, Q_RANK), BF16),
            pltpu.VMEM((Q_RANK, HEADS * NOPE), BF16),
            pltpu.VMEM((HEADS * ROPE, Q_RANK), BF16),
            pltpu.VMEM((HIDDEN, KV_RANK), BF16),
            pltpu.VMEM((ROPE, HIDDEN), BF16),
            pltpu.VMEM((KV_RANK, HEADS * NOPE), BF16),
            pltpu.VMEM((KV_RANK, HEADS * VDIM), BF16),
            pltpu.VMEM((ROWS, 128), F32),
            pltpu.VMEM((ROWS, 128), F32),
            pltpu.VMEM((KV_RANK, 1024), BF16),
            pltpu.VMEM((CTX, 2, SPAN + KRP, KV_RANK), BF16),
            pltpu.VMEM((ROWS, Q_RANK), BF16),
            pltpu.VMEM((PAIRS, 2, 2 * SPAN, 256), BF16),
            pltpu.VMEM((NSPAN, SPAN, HEADS * NOPE), BF16),
            pltpu.VMEM((NSPAN, SPAN, HEADS * VDIM), BF16),
            pltpu.VMEM((NSPAN, SPAN, 128), BF16),
            pltpu.VMEM((2, 9, 2 * SPAN, SPAN), F32),
            pltpu.VMEM((2, 2, 2 * SPAN, 128), F32),
            pltpu.VMEM((2, 2 * SPAN, 128), F32),
            pltpu.VMEM((2, 2 * SPAN, 128), F32),
            pltpu.VMEM((2, 2 * SPAN, 128), F32),
            pltpu.VMEM((PAIRS, MODEL, 128, 128), BF16),
            pltpu.VMEM((2, MODEL, 128, HV), BF16),
            pltpu.VMEM((MODEL, HV, NHALF), BF16),
            pltpu.VMEM((2, NSUB, 128, SUBC), BF16),
            dma((14,)),
            dma((3, 2)), dma((3, 2)),
            dma((2,)), dma((MODEL,)), dma((MODEL, NSUB)),
            dma((MODEL,)), dma((MODEL, NSUB)),
            dma((MODEL, 2)), dma((MODEL, 2, NSUB)),
            dma((PAIRS, 3)), dma((PAIRS, 3)),
            dma((PAIRS,)), dma((PAIRS,)),
            dma((NSUB,)), dma((NSUB,)), dma((NSUB,)),
        ],
        compiler_params=pltpu.CompilerParams(collective_id=0, has_side_effects=True, vmem_limit_bytes=60 * 1024 * 1024),
        name='mla_layer',
    )(x, pos, freq, gq, gkv, wdq, wuq, wqr, wdkv, wkr, wuk, wuv, wout)


def solution(mesh):
    inv_freq = (ROPE_BASE ** (-(np.arange(ROPE // 2, dtype=np.float64) * 2.0 / ROPE))).astype(np.float32)
    freq = np.tile(inv_freq, 128 // (ROPE // 2))[None, :]

    def local(x_tokens, positions, w_dq, gain_q, w_uq, w_qr, w_dkv, gain_kv, w_kr, w_uk, w_uv, w_out):
        return layer(x_tokens, positions[None, :], jnp.asarray(freq), w_dq, gain_q.reshape(Q_RANK // 128, 128), w_uq,
                     w_qr.T, w_dkv, gain_kv[None, :], w_kr.T, w_uk, w_uv, w_out)

    in_specs = (P(('dp', 'ctx'), None), P(('dp', 'ctx')), P(), P(), P(None, 'model'), P(None, 'model'), P(), P(), P(), P(None, 'model'), P(None, 'model'), P('model', None))
    out_specs = P(('dp', 'ctx', 'model'), None)
    return jax.shard_map(local, mesh=mesh, in_specs=in_specs, out_specs=out_specs, check_vma=False)
```

```python
import functools

import jax
import jax.numpy as jnp
import numpy as np
from jax import lax
from jax.experimental import pallas as pl
from jax.experimental.pallas import tpu as pltpu
from jax.sharding import PartitionSpec as P

MESH = pl.DeviceIdType.MESH


def scoped(fn):
    @functools.wraps(fn)
    def run(*args):
        tag = "_".join(str(a) for a in args if isinstance(a, int))
        with jax.named_scope(fn.__name__ + tag):
            return fn(*args)
    return run


F32 = jnp.float32
BF16 = jnp.bfloat16

HIDDEN = 2560
Q_RANK = 768
KV_RANK = 256
HEADS = 10
PAIRS = HEADS // 2
NOPE = 64
ROPE = 32
VDIM = 64
ROWS = 512
SPAN = 256
NSPAN = 8
CTX = 4
MODEL = 4
HV = HEADS * VDIM
NHALF = HIDDEN // 2
QROWS = HV // 4
NSUB = 5
SUBC = NHALF // NSUB
KRP = SPAN // 8
EPS = 1e-6
ROPE_BASE = 10000.0
SM_SCALE = float((NOPE + ROPE) ** -0.5 * np.log2(np.e))
NEG = -1e30


def dot(a, b):
    return jnp.dot(a, b, preferred_element_type=F32)


def dot_nt(a, b):
    return lax.dot_general(a, b, (((1,), (1,)), ((), ())), preferred_element_type=F32)


def rms(h, gain):
    ms = jnp.mean(h * h, axis=-1, keepdims=True)
    return (h * lax.rsqrt(ms + EPS) * gain).astype(BF16)


def kernel(x_h, pos_h, freq_h, gq_h, gkv_h, wdq_h, wuq_h, wqr_h, wdkv_h, wkr_h, wuk_h, wuv_h, wout_h, out_h,
           pos_r, freq_r, gq_r, gkv_r, x_v, wdq_v, wuq_v, wqr_v, wdkv_v, wkr_v, wkv_v,
           cos_v, sin_v, tile_v, lat_v, cq_v, qm_v, k_v, v_v, kr_v, s_v, mx_v, mb_v, l_v, acc_v,
           os_v, oall_v, wall_v, yst_v, yacc_v,
           lsem, kv_ssem, kv_rsem, wz_own, wz_ssem, wz_rsem, wy_ssem, wy_rsem, wd_ssem, wd_rsem,
           oz_ssem, oz_rsem, ox_ssem, ox_rsem, yb_ssem, yb_rsem, yl_sem):
    dp = lax.axis_index('dp')
    z = lax.axis_index('model')
    ctx = lax.axis_index('ctx')
    partner = ctx + 1 - 2 * lax.rem(ctx, 2)
    ynbr = lax.rem(ctx + 2, CTX)
    diag = lax.rem(partner + 2, CTX)
    xn = 1 - dp

    def dev(d=None, m=None, c=None):
        return (dp if d is None else d, z if m is None else m, ctx if c is None else c)

    def remote(src, dst, ss, rs, where):
        return pltpu.make_async_remote_copy(src_ref=src, dst_ref=dst, send_sem=ss, recv_sem=rs,
                                            device_id=where, device_id_type=MESH)

    def local(src, dst, idx):
        return pltpu.make_async_copy(src, dst, lsem.at[idx])

    small = [local(pos_h, pos_r, 10), local(freq_h, freq_r, 11), local(gq_h, gq_r, 12), local(gkv_h, gkv_r, 13)]
    loads = [
        local(wkr_h, wkr_v, 0),
        local(x_h.at[pl.ds(0, SPAN)], x_v.at[pl.ds(0, SPAN)], 1),
        local(wdkv_h, wdkv_v, 2),
        local(x_h.at[pl.ds(SPAN, SPAN)], x_v.at[pl.ds(SPAN, SPAN)], 3),
        local(wdq_h, wdq_v, 4),
        local(wuq_h, wuq_v, 5),
        local(wqr_h, wqr_v, 6),
        local(wuk_h, wkv_v.at[:, pl.ds(0, HV)], 7),
        local(wuv_h, wkv_v.at[:, pl.ds(HV, HV)], 8),
        local(wout_h.at[:, pl.ds(pl.multiple_of(dp * NHALF, 128), NHALF)], wall_v.at[z], 9),
    ]
    for c in small + loads:
        c.start()

    barrier = pltpu.get_barrier_semaphore()
    peers = [dev(m=lax.rem(z + d, MODEL)) for d in (1, 2, 3)] + [dev(d=xn), dev(c=partner), dev(c=ynbr)]
    for p in peers:
        pl.semaphore_signal(barrier, inc=1, device_id=p, device_id_type=MESH)
    with jax.named_scope('barrier'):
        pl.semaphore_wait(barrier, len(peers))

    def wpiece(s, c, n=None):
        rows = pl.ds(pl.multiple_of(c * QROWS, 16), QROWS)
        return wall_v.at[s, rows] if n is None else wall_v.at[s, rows, pl.ds(SUBC * n, SUBC)]

    def wsrc(n=None):
        rows = pl.ds(pl.multiple_of(ctx * QROWS, 16), QROWS)
        c0 = dp * NHALF + (0 if n is None else SUBC * n)
        return wout_h.at[rows, pl.ds(pl.multiple_of(c0, 128), NHALF if n is None else SUBC)]

    def w_own(up, n=None):
        return remote(wsrc(n), wpiece(z, ctx, n), wz_own.at[up], wz_rsem.at[z, n or 0], dev(m=z + 2 * up - 1))

    def w_fwd_z(s, to, n=None):
        return remote(wpiece(s, ctx, n), wpiece(s, ctx, n), wz_ssem.at[s], wz_rsem.at[s, n or 0], dev(m=to))

    def w_fwd_y(s, n=None):
        return remote(wpiece(s, ctx, n), wpiece(s, ctx, n), wy_ssem.at[s], wy_rsem.at[s, n or 0], dev(c=ynbr))

    def w_fwd_d(s, which, n=None):
        c = ctx if which == 0 else ynbr
        return remote(wpiece(s, c, n), wpiece(s, c, n), wd_ssem.at[s, which], wd_rsem.at[s, which, n or 0], dev(c=partner))

    def wait_wz(s, n):
        remote(wpiece(s, ctx, n), wpiece(s, ctx, n), wz_ssem.at[s], wz_rsem.at[s, n], dev()).wait_recv()

    def wait_wy(s, n):
        remote(wpiece(s, ynbr, n), wpiece(s, ynbr, n), wy_ssem.at[s], wy_rsem.at[s, n], dev()).wait_recv()

    def wait_wd(s, which, n):
        c = partner if which == 0 else diag
        remote(wpiece(s, c, n), wpiece(s, c, n), wd_ssem.at[s, which], wd_rsem.at[s, which, n], dev()).wait_recv()

    @pl.when(z < MODEL - 1)
    def _():
        for n in range(NSUB):
            w_own(1, n).start()

    @pl.when(z > 0)
    def _():
        for n in range(NSUB):
            w_own(0, n).start()

    def each_share(j, fn):
        for sign in (-1, 1):
            s = z + sign * j

            @pl.when((s >= 0) & (s < MODEL))
            def _(s=s, sign=sign):
                fn(s, sign)

    @scoped
    def hop(q):
        j, n = q // NSUB + 1, q % NSUB

        def step(s, sign):
            wait_wz(s, n)
            to = z - sign

            @pl.when((to >= 0) & (to < MODEL))
            def _():
                w_fwd_z(s, to, n).start()
            w_fwd_y(s, n).start()
            w_fwd_d(s, 0, n).start()
        each_share(j, step)

    @scoped
    def across(q):
        j, n = q // NSUB + 1, q % NSUB

        def step(s, sign):
            wait_wy(s, n)
            w_fwd_d(s, 1, n).start()
        each_share(j, step)

    lane = lax.broadcasted_iota(jnp.int32, (1, 128), 1)
    with jax.named_scope('small'):
        for c in small:
            c.wait()
    with jax.named_scope('tables'):
        for g in range(ROWS // 128):
            row = pos_r[:, pl.ds(128 * g, 128)].astype(F32)
            col = jnp.transpose(jnp.broadcast_to(row, (128, 128)), (1, 0))
            ang = col * freq_r[...]
            cos_v[pl.ds(128 * g, 128), :] = jnp.cos(ang)
            sin_v[pl.ds(128 * g, 128), :] = jnp.sin(ang)
    rr = lax.broadcasted_iota(jnp.int32, (KV_RANK, 1024), 0)
    cc = lax.broadcasted_iota(jnp.int32, (KV_RANK, 1024), 1)
    tile_v[...] = jnp.where((rr // ROPE == cc // 128) & (rr % ROPE == cc % ROPE), 1.0, 0.0).astype(BF16)
    low = (lane % ROPE) < (ROPE // 2)

    def rope(v, r0):
        up = pltpu.roll(v, 128 - ROPE // 2, 1)
        dn = pltpu.roll(v, ROPE // 2, 1)
        rot = jnp.where(low, -up, dn)
        return v * cos_v[pl.ds(r0, SPAN), :] + rot * sin_v[pl.ds(r0, SPAN), :]

    def kv_copy(c, t, idx, to):
        return remote(lat_v.at[c, t], lat_v.at[c, t], kv_ssem.at[idx, t], kv_rsem.at[idx, t], dev(c=to))

    loads[0].wait()
    wkr4 = jnp.concatenate([wkr_v[...]] * 4, axis=0)
    gkv = gkv_r[...]
    with jax.named_scope('ckv'):
        for t in range(2):
            r0 = t * SPAN
            if t == 0:
                loads[1].wait()
                loads[2].wait()
            else:
                loads[3].wait()
            xs = x_v[pl.ds(r0, SPAN), :]
            lat_v[ctx, t, pl.ds(0, SPAN), :] = rms(dot(xs, wdkv_v[...]), gkv)
            kr = rope(dot_nt(xs, wkr4), r0)
            for half in range(2):
                packed = kr[128 * half:128 * half + KRP]
                for g in range(1, 4):
                    a = 128 * half + KRP * g
                    packed = jnp.where(lane // ROPE == g, kr[a:a + KRP], packed)
                lat_v[ctx, t, pl.ds(SPAN, KRP), pl.ds(128 * half, 128)] = packed.astype(BF16)
            if t == 0:
                kv_copy(ctx, t, 0, ynbr).start()
            else:
                @pl.when(ctx >= 2)
                def _():
                    kv_copy(ctx, 1, 0, ynbr).start()
            kv_copy(ctx, t, 1, partner).start()

    with jax.named_scope('ld4'):
        loads[4].wait()
    gq = jnp.concatenate([gq_r[g:g + 1, :] for g in range(Q_RANK // 128)], axis=1)
    with jax.named_scope('cq'):
        for t in range(2):
            cq_v[pl.ds(t * SPAN, SPAN), :] = rms(dot(x_v[pl.ds(t * SPAN, SPAN), :], wdq_v[...]), gq)
    hop(0)
    loads[5].wait()
    loads[6].wait()
    with jax.named_scope('qup'):
        for t in range(2):
            cq = cq_v[pl.ds(t * SPAN, SPAN), :]
            qn = dot(cq, wuq_v[...]).astype(BF16)
            zero = jnp.zeros((SPAN, 128), BF16)
            for p in range(PAIRS):
                blk = qn[:, 128 * p:128 * p + 128]
                qm_v[p, t, pl.ds(0, SPAN), pl.ds(0, 128)] = jnp.where(lane < NOPE, blk, zero)
                qm_v[p, t, pl.ds(SPAN, SPAN), pl.ds(0, 128)] = jnp.where(lane < NOPE, zero, blk)
            for b in range(3):
                w = wqr_v[pl.ds(128 * b, 128), :] if b < 2 else jnp.concatenate([wqr_v[pl.ds(256, 64), :]] * 2, axis=0)
                qr = rope(dot_nt(cq, w), t * SPAN).astype(BF16)
                for h in range(4 * b, min(4 * b + 4, HEADS)):
                    qm_v[h // 2, t, pl.ds(SPAN * (h % 2), SPAN), pl.ds(128, 128)] = jnp.where(lane // ROPE == h % 4, qr, zero)

    hop(1)

    @scoped
    def up(c, t):
        sp = c if t == 0 else NSPAN - 1 - c
        lat = lat_v[c, t, pl.ds(0, SPAN), :]
        kv = dot(lat, wkv_v[...]).astype(BF16)
        k_v[sp] = kv[:, :HV]
        v_v[sp] = kv[:, HV:]
        big = dot(lat_v[c, t, pl.ds(SPAN, KRP), :], tile_v[...]).astype(BF16)
        for g in range(8):
            kr_v[sp, pl.ds(KRP * g, KRP), :] = big[:, 128 * g:128 * g + 128]

    def up_late(c):
        @pl.when(c >= ctx)
        def _():
            up(c, 1)

    loads[7].wait()
    loads[8].wait()
    up(ctx, 0)
    up(ctx, 1)
    with jax.named_scope('kvw_partner'):
        kv_copy(partner, 0, 1, ctx).wait_recv()
        kv_copy(partner, 1, 1, ctx).wait_recv()
    up(partner, 0)
    up_late(partner)
    hop(2)
    with jax.named_scope('kvw_ynbr'):
        kv_copy(ynbr, 0, 0, ctx).wait_recv()
    kv_copy(ynbr, 0, 2, partner).start()
    up(ynbr, 0)

    @pl.when(ctx < 2)
    def _():
        kv_copy(ynbr, 1, 0, ctx).wait_recv()
        kv_copy(ynbr, 1, 2, partner).start()
        up(ynbr, 1)
    hop(3)
    with jax.named_scope('kvw_diag'):
        kv_copy(diag, 0, 2, ctx).wait_recv()
    up(diag, 0)

    @pl.when(ctx < 2)
    def _():
        kv_copy(diag, 1, 2, ctx).wait_recv()
        up(diag, 1)
    hop(4)

    def block(b):
        if b < 5:
            return 1, NSPAN - 1 - ctx - b
        if b == 8:
            return 0, ctx
        hi = b < NSPAN - ctx
        return jnp.where(hi, 1, 0), jnp.where(hi, NSPAN - 1 - ctx - b, b - (NSPAN - ctx))

    ORDER = (0, 8, 1, 2, 3, 4, 5, 6, 7)
    q_i = lax.broadcasted_iota(jnp.int32, (SPAN, SPAN), 0)
    k_i = lax.broadcasted_iota(jnp.int32, (SPAN, SPAN), 1)
    causal = k_i <= q_i

    def scores(p, b):
        buf = p % 2
        qs, ks = block(b)
        kc = jnp.concatenate([k_v[ks, :, pl.ds(128 * p, 128)], kr_v[ks]], axis=1)
        for a in range(2):
            rows = pl.ds(SPAN * a, SPAN)
            s = dot_nt(qm_v[p, qs, rows, :], kc)
            if b in (0, 8):
                s = jnp.where(causal, s, NEG)
            s_v[buf, b, rows, :] = s
            m = jnp.maximum(s[:, :128], s[:, 128:])
            if b not in (0, 8):
                m = jnp.maximum(mx_v[buf, qs, rows, :], m)
            mx_v[buf, qs, rows, :] = m

    @scoped
    def maxima(p):
        buf = p % 2
        for qs in range(2):
            for a in range(2):
                rows = pl.ds(SPAN * a, SPAN)
                m = jnp.max(mx_v[buf, qs, rows, :], axis=1, keepdims=True)
                mb_v[qs, rows, :] = jnp.broadcast_to(m * SM_SCALE, (SPAN, 128))

    def values(p, b):
        buf = p % 2
        qs, ks = block(b)
        vb = v_v[ks, :, pl.ds(128 * p, 128)]
        for a in range(2):
            rows = pl.ds(SPAN * a, SPAN)
            m = mb_v[qs, rows, :]
            e0 = jnp.exp2(s_v[buf, b, rows, pl.ds(0, 128)] * SM_SCALE - m)
            e1 = jnp.exp2(s_v[buf, b, rows, pl.ds(128, 128)] * SM_SCALE - m)
            pv = dot(jnp.concatenate([e0.astype(BF16), e1.astype(BF16)], axis=1), vb)
            l = e0 + e1
            if b in (0, 8):
                l_v[qs, rows, :] = l
                acc_v[qs, rows, :] = pv
            else:
                l_v[qs, rows, :] += l
                acc_v[qs, rows, :] += pv

    @scoped
    def finish(p):
        for qs in range(2):
            o = []
            for a in range(2):
                rows = pl.ds(SPAN * a, SPAN)
                l = jnp.sum(l_v[qs, rows, :], axis=1, keepdims=True)
                o.append(acc_v[qs, rows, :] / l)
            both = jnp.where(lane < VDIM, o[0], o[1]).astype(BF16)
            os_v[p, 2 * qs] = both[:128]
            os_v[p, 2 * qs + 1] = both[128:]

    def oblk(blk, p, src):
        return oall_v.at[pl.ds(pl.multiple_of(128 * blk, 128), 128), pl.ds(pl.multiple_of(512 * p + 128 * src, 128), 128)]

    def o_z(p, d):
        to = lax.rem(z + d, MODEL)
        return remote(os_v.at[p, to], oblk(dp, p, z),
                      oz_ssem.at[p, d - 1], oz_rsem.at[p, d - 1], dev(m=to))

    def o_z_wait(p, d):
        src = lax.rem(z + MODEL - d, MODEL)
        remote(os_v.at[p, z], oblk(dp, p, src),
               oz_ssem.at[p, d - 1], oz_rsem.at[p, d - 1], dev()).wait_recv()

    def o_x(p, src_dp, to):
        part = oall_v.at[pl.ds(pl.multiple_of(128 * src_dp, 128), 128), pl.ds(512 * p, 512)]
        return remote(part, part, ox_ssem.at[p], ox_rsem.at[p], dev(d=to))

    @scoped
    def send_o(p):
        oblk(dp, p, z)[...] = os_v[p, z]
        for d in (1, 2, 3):
            o_z(p, d).start()

    @scoped
    def pass_o(p):
        for d in (1, 2, 3):
            o_z_wait(p, d)
        o_x(p, dp, xn).start()

    with jax.named_scope('scores0'):
        for b in ORDER:
            scores(0, b)
    maxima(0)
    hop(5)
    relay = {
        0: lambda: (hop(6),),
        1: lambda: (hop(7), hop(8)),
        2: lambda: (hop(9), pass_o(0)),
        3: lambda: (hop(10), pass_o(1)),
        4: lambda: (hop(11), pass_o(2)),
    }
    for p in range(PAIRS):
        with jax.named_scope('attn%d' % p):
            for b in ORDER:
                if p + 1 < PAIRS:
                    scores(p + 1, b)
                values(p, b)
        finish(p)
        if p + 1 < PAIRS:
            maxima(p + 1)
        send_o(p)
        relay[p]()
    for q in range(5):
        across(q)
    hop(12)
    pass_o(3)
    for q in range(5, 10):
        across(q)
    hop(13)
    pass_o(4)
    hop(14)
    loads[9].wait()

    with jax.named_scope('drain1'):
        for t in range(2):
            kv_copy(ctx, t, 1, partner).wait_send()
        kv_copy(ctx, 0, 0, ynbr).wait_send()
        kv_copy(ynbr, 0, 2, partner).wait_send()

        @pl.when(ctx >= 2)
        def _():
            kv_copy(ctx, 1, 0, ynbr).wait_send()

        @pl.when(ctx < 2)
        def _():
            kv_copy(ynbr, 1, 2, partner).wait_send()

        @pl.when(z < MODEL - 1)
        def _():
            w_own(1).wait_send()

        @pl.when(z > 0)
        def _():
            w_own(0).wait_send()

        for p in range(PAIRS):
            for d in (1, 2, 3):
                o_z(p, d).wait_send()
    def ycols(half, n):
        return out_h.at[:, pl.ds(pl.multiple_of(half * NHALF + SUBC * n, 128), SUBC)]

    def y_back(n):
        return remote(yst_v.at[xn, n], ycols(dp, n), yb_ssem.at[n], yb_rsem.at[n], dev(d=xn))

    def y_come(n):
        return remote(yst_v.at[xn, n], ycols(xn, n), yb_ssem.at[n], yb_rsem.at[n], dev())

    def y_local(n):
        return pltpu.make_async_copy(yst_v.at[dp, n], ycols(dp, n), yl_sem.at[n])

    def wcols(ps, n):
        return jnp.concatenate([wall_v[s, pl.ds(128 * p, 128), pl.ds(SUBC * n, SUBC)] for p in ps for s in range(MODEL)], axis=0)

    def have_w(n):
        across(2 * NSUB + n)
        with jax.named_scope('wdwait'):
            for j in (1, 2, 3):
                each_share(j, lambda s, sign: (wait_wd(s, 0, n), wait_wd(s, 1, n)))

    def finish_y(n, y):
        yst_v[0, n] = y[:128].astype(BF16)
        yst_v[1, n] = y[128:].astype(BF16)
        y_back(n).start()
        y_local(n).start()

    EARLY = 2
    with jax.named_scope('oxwait'):
        for p in range(PAIRS - 1):
            o_x(p, xn, dp).wait_recv()
    for n in range(EARLY):
        have_w(n)
        with jax.named_scope('finala%d' % n):
            yacc_v[n] = dot(oall_v[:, pl.ds(0, 2048)], wcols(range(PAIRS - 1), n))
    with jax.named_scope('oxwait4'):
        o_x(PAIRS - 1, xn, dp).wait_recv()
    for n in range(EARLY):
        with jax.named_scope('finalb%d' % n):
            finish_y(n, yacc_v[n] + dot(oall_v[:, pl.ds(2048, 512)], wcols((PAIRS - 1,), n)))
    for n in range(EARLY, NSUB):
        have_w(n)
        with jax.named_scope('final%d' % n):
            finish_y(n, dot(oall_v[...], wcols(range(PAIRS), n)))

    def sent(s, sign):
        to = z - sign

        @pl.when((to >= 0) & (to < MODEL))
        def _():
            w_fwd_z(s, to).wait_send()
        w_fwd_y(s).wait_send()
        w_fwd_d(s, 0).wait_send()
        w_fwd_d(s, 1).wait_send()

    with jax.named_scope('drain2'):
        for j in (1, 2, 3):
            each_share(j, sent)
        for p in range(PAIRS):
            o_x(p, dp, xn).wait_send()
        for n in range(NSUB):
            y_back(n).wait_send()
            y_local(n).wait()
            y_come(n).wait_recv()


def layer(x, pos, freq, wdq, gq, wuq, wqr, wdkv, gkv, wkr, wuk, wuv, wout):
    hb = pl.BlockSpec(memory_space=pl.ANY)
    dma = pltpu.SemaphoreType.DMA
    return pl.pallas_call(
        kernel,
        out_shape=jax.ShapeDtypeStruct((ROWS // MODEL, HIDDEN), BF16),
        in_specs=[hb] * 13,
        out_specs=hb,
        scratch_shapes=[
            pltpu.VMEM((1, ROWS), jnp.int32),
            pltpu.VMEM((1, 128), F32),
            pltpu.VMEM((Q_RANK // 128, 128), F32),
            pltpu.VMEM((1, KV_RANK), F32),
            pltpu.VMEM((ROWS, HIDDEN), BF16),
            pltpu.VMEM((HIDDEN, Q_RANK), BF16),
            pltpu.VMEM((Q_RANK, HEADS * NOPE), BF16),
            pltpu.VMEM((HEADS * ROPE, Q_RANK), BF16),
            pltpu.VMEM((HIDDEN, KV_RANK), BF16),
            pltpu.VMEM((ROPE, HIDDEN), BF16),
            pltpu.VMEM((KV_RANK, 2 * HV), BF16),
            pltpu.VMEM((ROWS, 128), F32),
            pltpu.VMEM((ROWS, 128), F32),
            pltpu.VMEM((KV_RANK, 1024), BF16),
            pltpu.VMEM((CTX, 2, SPAN + KRP, KV_RANK), BF16),
            pltpu.VMEM((ROWS, Q_RANK), BF16),
            pltpu.VMEM((PAIRS, 2, 2 * SPAN, 256), BF16),
            pltpu.VMEM((NSPAN, SPAN, HEADS * NOPE), BF16),
            pltpu.VMEM((NSPAN, SPAN, HEADS * VDIM), BF16),
            pltpu.VMEM((NSPAN, SPAN, 128), BF16),
            pltpu.VMEM((2, 9, 2 * SPAN, SPAN), F32),
            pltpu.VMEM((2, 2, 2 * SPAN, 128), F32),
            pltpu.VMEM((2, 2 * SPAN, 128), F32),
            pltpu.VMEM((2, 2 * SPAN, 128), F32),
            pltpu.VMEM((2, 2 * SPAN, 128), F32),
            pltpu.VMEM((PAIRS, MODEL, 128, 128), BF16),
            pltpu.VMEM((2 * 128, HIDDEN), BF16),
            pltpu.VMEM((MODEL, HV, NHALF), BF16),
            pltpu.VMEM((2, NSUB, 128, SUBC), BF16),
            pltpu.VMEM((2, 256, SUBC), F32),
            dma((14,)),
            dma((3, 2)), dma((3, 2)),
            dma((2,)), dma((MODEL,)), dma((MODEL, NSUB)),
            dma((MODEL,)), dma((MODEL, NSUB)),
            dma((MODEL, 2)), dma((MODEL, 2, NSUB)),
            dma((PAIRS, 3)), dma((PAIRS, 3)),
            dma((PAIRS,)), dma((PAIRS,)),
            dma((NSUB,)), dma((NSUB,)), dma((NSUB,)),
        ],
        compiler_params=pltpu.CompilerParams(collective_id=0, has_side_effects=True, vmem_limit_bytes=60 * 1024 * 1024),
        name='mla_layer',
    )(x, pos, freq, gq, gkv, wdq, wuq, wqr, wdkv, wkr, wuk, wuv, wout)


def solution(mesh):
    inv_freq = (ROPE_BASE ** (-(np.arange(ROPE // 2, dtype=np.float64) * 2.0 / ROPE))).astype(np.float32)
    freq = np.tile(inv_freq, 128 // (ROPE // 2))[None, :]

    def local(x_tokens, positions, w_dq, gain_q, w_uq, w_qr, w_dkv, gain_kv, w_kr, w_uk, w_uv, w_out):
        return layer(x_tokens, positions[None, :], jnp.asarray(freq), w_dq, gain_q.reshape(Q_RANK // 128, 128), w_uq,
                     w_qr.T, w_dkv, gain_kv[None, :], w_kr.T, w_uk, w_uv, w_out)

    in_specs = (P(('dp', 'ctx'), None), P(('dp', 'ctx')), P(), P(), P(None, 'model'), P(None, 'model'), P(), P(), P(), P(None, 'model'), P(None, 'model'), P('model', None))
    out_specs = P(('dp', 'ctx', 'model'), None)
    return jax.shard_map(local, mesh=mesh, in_specs=in_specs, out_specs=out_specs, check_vma=False)
```

```python
import functools

import jax
import jax.numpy as jnp
import numpy as np
from jax import lax
from jax.experimental import pallas as pl
from jax.experimental.pallas import tpu as pltpu
from jax.sharding import PartitionSpec as P

MESH = pl.DeviceIdType.MESH


def scoped(fn):
    @functools.wraps(fn)
    def run(*args):
        tag = "_".join(str(a) for a in args if isinstance(a, int))
        with jax.named_scope(fn.__name__ + tag):
            return fn(*args)
    return run


F32 = jnp.float32
BF16 = jnp.bfloat16

HIDDEN = 2560
Q_RANK = 768
KV_RANK = 256
HEADS = 10
PAIRS = HEADS // 2
NOPE = 64
ROPE = 32
VDIM = 64
ROWS = 512
SPAN = 256
NSPAN = 8
CTX = 4
MODEL = 4
HV = HEADS * VDIM
NHALF = HIDDEN // 2
QROWS = HV // 4
NSUB = 5
SUBC = NHALF // NSUB
KRP = SPAN // 8
EPS = 1e-6
ROPE_BASE = 10000.0
SM_SCALE = float((NOPE + ROPE) ** -0.5 * np.log2(np.e))
NEG = -1e30


def dot(a, b):
    return jnp.dot(a, b, preferred_element_type=F32)


def dot_nt(a, b):
    return lax.dot_general(a, b, (((1,), (1,)), ((), ())), preferred_element_type=F32)


def rms(h, gain):
    ms = jnp.mean(h * h, axis=-1, keepdims=True)
    return (h * lax.rsqrt(ms + EPS) * gain).astype(BF16)


def kernel(x_h, pos_h, freq_h, gq_h, gkv_h, wdq_h, wuq_h, wqr_h, wdkv_h, wkr_h, wuk_h, wuv_h, wout_h, out_h,
           pos_r, freq_r, gq_r, gkv_r, x_v, wdq_v, wuq_v, wqr_v, wdkv_v, wkr_v, wkv_v,
           cos_v, sin_v, tile_v, lat_v, cq_v, qm_v, k_v, v_v, kr_v, s_v, mx_v, mb_v, l_v, acc_v,
           os_v, oall_v, wall_v, yst_v, yacc_v,
           lsem, kv_ssem, kv_rsem, wz_own, wz_ssem, wz_rsem, wy_ssem, wy_rsem, wd_ssem, wd_rsem,
           oz_ssem, oz_rsem, ox_ssem, ox_rsem, yb_ssem, yb_rsem, yl_sem):
    dp = lax.axis_index('dp')
    z = lax.axis_index('model')
    ctx = lax.axis_index('ctx')
    partner = ctx + 1 - 2 * lax.rem(ctx, 2)
    ynbr = lax.rem(ctx + 2, CTX)
    diag = lax.rem(partner + 2, CTX)
    xn = 1 - dp

    def dev(d=None, m=None, c=None):
        return (dp if d is None else d, z if m is None else m, ctx if c is None else c)

    def remote(src, dst, ss, rs, where):
        return pltpu.make_async_remote_copy(src_ref=src, dst_ref=dst, send_sem=ss, recv_sem=rs,
                                            device_id=where, device_id_type=MESH)

    def local(src, dst, idx):
        return pltpu.make_async_copy(src, dst, lsem.at[idx])

    small = [local(pos_h, pos_r, 10), local(freq_h, freq_r, 11), local(gq_h, gq_r, 12), local(gkv_h, gkv_r, 13)]
    loads = [
        local(wkr_h, wkr_v, 0),
        local(x_h.at[pl.ds(0, SPAN)], x_v.at[pl.ds(0, SPAN)], 1),
        local(wdkv_h, wdkv_v, 2),
        local(x_h.at[pl.ds(SPAN, SPAN)], x_v.at[pl.ds(SPAN, SPAN)], 3),
        local(wdq_h, wdq_v, 4),
        local(wuq_h, wuq_v, 5),
        local(wqr_h, wqr_v, 6),
        local(wuk_h, wkv_v.at[:, pl.ds(0, HV)], 7),
        local(wuv_h, wkv_v.at[:, pl.ds(HV, HV)], 8),
        local(wout_h.at[:, pl.ds(pl.multiple_of(dp * NHALF, 128), NHALF)], wall_v.at[z], 9),
    ]
    for c in small + loads:
        c.start()

    barrier = pltpu.get_barrier_semaphore()
    peers = [dev(m=lax.rem(z + d, MODEL)) for d in (1, 2, 3)] + [dev(d=xn), dev(c=partner), dev(c=ynbr)]
    for p in peers:
        pl.semaphore_signal(barrier, inc=1, device_id=p, device_id_type=MESH)
    with jax.named_scope('barrier'):
        pl.semaphore_wait(barrier, len(peers))

    def wpiece(s, c, n=None):
        rows = pl.ds(pl.multiple_of(c * QROWS, 16), QROWS)
        return wall_v.at[s, rows] if n is None else wall_v.at[s, rows, pl.ds(SUBC * n, SUBC)]

    def wsrc(n=None):
        rows = pl.ds(pl.multiple_of(ctx * QROWS, 16), QROWS)
        c0 = dp * NHALF + (0 if n is None else SUBC * n)
        return wout_h.at[rows, pl.ds(pl.multiple_of(c0, 128), NHALF if n is None else SUBC)]

    def w_own(up, n=None):
        return remote(wsrc(n), wpiece(z, ctx, n), wz_own.at[up], wz_rsem.at[z, n or 0], dev(m=z + 2 * up - 1))

    def w_fwd_z(s, to, n=None):
        return remote(wpiece(s, ctx, n), wpiece(s, ctx, n), wz_ssem.at[s], wz_rsem.at[s, n or 0], dev(m=to))

    def w_fwd_y(s, n=None):
        return remote(wpiece(s, ctx, n), wpiece(s, ctx, n), wy_ssem.at[s], wy_rsem.at[s, n or 0], dev(c=ynbr))

    def w_fwd_d(s, which, n=None):
        c = ctx if which == 0 else ynbr
        return remote(wpiece(s, c, n), wpiece(s, c, n), wd_ssem.at[s, which], wd_rsem.at[s, which, n or 0], dev(c=partner))

    def wait_wz(s, n):
        remote(wpiece(s, ctx, n), wpiece(s, ctx, n), wz_ssem.at[s], wz_rsem.at[s, n], dev()).wait_recv()

    def wait_wy(s, n):
        remote(wpiece(s, ynbr, n), wpiece(s, ynbr, n), wy_ssem.at[s], wy_rsem.at[s, n], dev()).wait_recv()

    def wait_wd(s, which, n):
        c = partner if which == 0 else diag
        remote(wpiece(s, c, n), wpiece(s, c, n), wd_ssem.at[s, which], wd_rsem.at[s, which, n], dev()).wait_recv()

    @pl.when(z < MODEL - 1)
    def _():
        for n in range(NSUB):
            w_own(1, n).start()

    @pl.when(z > 0)
    def _():
        for n in range(NSUB):
            w_own(0, n).start()

    def each_share(j, fn):
        for sign in (-1, 1):
            s = z + sign * j

            @pl.when((s >= 0) & (s < MODEL))
            def _(s=s, sign=sign):
                fn(s, sign)

    @scoped
    def zfwd(q):
        j, n = q // NSUB + 1, q % NSUB

        def step(s, sign):
            to = z - sign

            @pl.when((to >= 0) & (to < MODEL))
            def _():
                w_fwd_z(s, to, n).start()
        each_share(j, step)

    @scoped
    def hop(q, forward=True):
        j, n = q // NSUB + 1, q % NSUB

        def step(s, sign):
            wait_wz(s, n)
            to = z - sign
            if forward:
                @pl.when((to >= 0) & (to < MODEL))
                def _():
                    w_fwd_z(s, to, n).start()
            w_fwd_y(s, n).start()
            w_fwd_d(s, 0, n).start()
        each_share(j, step)

    @scoped
    def across(q):
        j, n = q // NSUB + 1, q % NSUB

        def step(s, sign):
            wait_wy(s, n)
            w_fwd_d(s, 1, n).start()
        each_share(j, step)

    lane = lax.broadcasted_iota(jnp.int32, (1, 128), 1)
    with jax.named_scope('small'):
        for c in small:
            c.wait()
    with jax.named_scope('tables'):
        for g in range(ROWS // 128):
            row = pos_r[:, pl.ds(128 * g, 128)].astype(F32)
            col = jnp.transpose(jnp.broadcast_to(row, (128, 128)), (1, 0))
            ang = col * freq_r[...]
            cos_v[pl.ds(128 * g, 128), :] = jnp.cos(ang)
            sin_v[pl.ds(128 * g, 128), :] = jnp.sin(ang)
    rr = lax.broadcasted_iota(jnp.int32, (KV_RANK, 1024), 0)
    cc = lax.broadcasted_iota(jnp.int32, (KV_RANK, 1024), 1)
    tile_v[...] = jnp.where((rr // ROPE == cc // 128) & (rr % ROPE == cc % ROPE), 1.0, 0.0).astype(BF16)
    low = (lane % ROPE) < (ROPE // 2)

    def rope(v, r0):
        up = pltpu.roll(v, 128 - ROPE // 2, 1)
        dn = pltpu.roll(v, ROPE // 2, 1)
        rot = jnp.where(low, -up, dn)
        return v * cos_v[pl.ds(r0, SPAN), :] + rot * sin_v[pl.ds(r0, SPAN), :]

    def kv_copy(c, t, idx, to):
        return remote(lat_v.at[c, t], lat_v.at[c, t], kv_ssem.at[idx, t], kv_rsem.at[idx, t], dev(c=to))

    loads[0].wait()
    wkr4 = jnp.concatenate([wkr_v[...]] * 4, axis=0)
    gkv = gkv_r[...]
    with jax.named_scope('ckv'):
        for t in range(2):
            r0 = t * SPAN
            if t == 0:
                loads[1].wait()
                loads[2].wait()
            else:
                loads[3].wait()
            xs = x_v[pl.ds(r0, SPAN), :]
            lat_v[ctx, t, pl.ds(0, SPAN), :] = rms(dot(xs, wdkv_v[...]), gkv)
            kr = rope(dot_nt(xs, wkr4), r0)
            for half in range(2):
                packed = kr[128 * half:128 * half + KRP]
                for g in range(1, 4):
                    a = 128 * half + KRP * g
                    packed = jnp.where(lane // ROPE == g, kr[a:a + KRP], packed)
                lat_v[ctx, t, pl.ds(SPAN, KRP), pl.ds(128 * half, 128)] = packed.astype(BF16)
            if t == 0:
                kv_copy(ctx, t, 0, ynbr).start()
            else:
                @pl.when(ctx >= 2)
                def _():
                    kv_copy(ctx, 1, 0, ynbr).start()
            kv_copy(ctx, t, 1, partner).start()

    with jax.named_scope('ld4'):
        loads[4].wait()
    gq = jnp.concatenate([gq_r[g:g + 1, :] for g in range(Q_RANK // 128)], axis=1)
    with jax.named_scope('cq'):
        for t in range(2):
            cq_v[pl.ds(t * SPAN, SPAN), :] = rms(dot(x_v[pl.ds(t * SPAN, SPAN), :], wdq_v[...]), gq)
    hop(0)
    loads[5].wait()
    loads[6].wait()
    with jax.named_scope('qup'):
        for t in range(2):
            cq = cq_v[pl.ds(t * SPAN, SPAN), :]
            qn = dot(cq, wuq_v[...]).astype(BF16)
            zero = jnp.zeros((SPAN, 128), BF16)
            for p in range(PAIRS):
                blk = qn[:, 128 * p:128 * p + 128]
                qm_v[p, t, pl.ds(0, SPAN), pl.ds(0, 128)] = jnp.where(lane < NOPE, blk, zero)
                qm_v[p, t, pl.ds(SPAN, SPAN), pl.ds(0, 128)] = jnp.where(lane < NOPE, zero, blk)
            for b in range(3):
                w = wqr_v[pl.ds(128 * b, 128), :] if b < 2 else jnp.concatenate([wqr_v[pl.ds(256, 64), :]] * 2, axis=0)
                qr = rope(dot_nt(cq, w), t * SPAN).astype(BF16)
                for h in range(4 * b, min(4 * b + 4, HEADS)):
                    qm_v[h // 2, t, pl.ds(SPAN * (h % 2), SPAN), pl.ds(128, 128)] = jnp.where(lane // ROPE == h % 4, qr, zero)

    hop(1)

    @scoped
    def up(c, t):
        sp = c if t == 0 else NSPAN - 1 - c
        lat = lat_v[c, t, pl.ds(0, SPAN), :]
        kv = dot(lat, wkv_v[...]).astype(BF16)
        k_v[sp] = kv[:, :HV]
        v_v[sp] = kv[:, HV:]
        big = dot(lat_v[c, t, pl.ds(SPAN, KRP), :], tile_v[...]).astype(BF16)
        for g in range(8):
            kr_v[sp, pl.ds(KRP * g, KRP), :] = big[:, 128 * g:128 * g + 128]

    def up_late(c):
        @pl.when(c >= ctx)
        def _():
            up(c, 1)

    loads[7].wait()
    loads[8].wait()
    up(ctx, 0)
    up(ctx, 1)
    with jax.named_scope('kvw_partner'):
        kv_copy(partner, 0, 1, ctx).wait_recv()
        kv_copy(partner, 1, 1, ctx).wait_recv()
    up(partner, 0)
    up_late(partner)
    hop(2)
    with jax.named_scope('kvw_ynbr'):
        kv_copy(ynbr, 0, 0, ctx).wait_recv()
    kv_copy(ynbr, 0, 2, partner).start()
    up(ynbr, 0)

    @pl.when(ctx < 2)
    def _():
        kv_copy(ynbr, 1, 0, ctx).wait_recv()
        kv_copy(ynbr, 1, 2, partner).start()
        up(ynbr, 1)
    hop(3)
    with jax.named_scope('kvw_diag'):
        kv_copy(diag, 0, 2, ctx).wait_recv()
    up(diag, 0)

    @pl.when(ctx < 2)
    def _():
        kv_copy(diag, 1, 2, ctx).wait_recv()
        up(diag, 1)
    hop(4)

    def block(b):
        if b < 5:
            return 1, NSPAN - 1 - ctx - b
        if b == 8:
            return 0, ctx
        hi = b < NSPAN - ctx
        return jnp.where(hi, 1, 0), jnp.where(hi, NSPAN - 1 - ctx - b, b - (NSPAN - ctx))

    ORDER = (0, 8, 1, 2, 3, 4, 5, 6, 7)
    q_i = lax.broadcasted_iota(jnp.int32, (SPAN, SPAN), 0)
    k_i = lax.broadcasted_iota(jnp.int32, (SPAN, SPAN), 1)
    causal = k_i <= q_i

    def scores(p, b):
        buf = p % 2
        qs, ks = block(b)
        kc = jnp.concatenate([k_v[ks, :, pl.ds(128 * p, 128)], kr_v[ks]], axis=1)
        for a in range(2):
            rows = pl.ds(SPAN * a, SPAN)
            s = dot_nt(qm_v[p, qs, rows, :], kc)
            if b in (0, 8):
                s = jnp.where(causal, s, NEG)
            s_v[buf, b, rows, :] = s
            m = jnp.maximum(s[:, :128], s[:, 128:])
            if b not in (0, 8):
                m = jnp.maximum(mx_v[buf, qs, rows, :], m)
            mx_v[buf, qs, rows, :] = m

    @scoped
    def maxima(p):
        buf = p % 2
        for qs in range(2):
            for a in range(2):
                rows = pl.ds(SPAN * a, SPAN)
                m = jnp.max(mx_v[buf, qs, rows, :], axis=1, keepdims=True)
                mb_v[qs, rows, :] = jnp.broadcast_to(m * SM_SCALE, (SPAN, 128))

    def values(p, b):
        buf = p % 2
        qs, ks = block(b)
        vb = v_v[ks, :, pl.ds(128 * p, 128)]
        for a in range(2):
            rows = pl.ds(SPAN * a, SPAN)
            m = mb_v[qs, rows, :]
            e0 = jnp.exp2(s_v[buf, b, rows, pl.ds(0, 128)] * SM_SCALE - m)
            e1 = jnp.exp2(s_v[buf, b, rows, pl.ds(128, 128)] * SM_SCALE - m)
            pv = dot(jnp.concatenate([e0.astype(BF16), e1.astype(BF16)], axis=1), vb)
            l = e0 + e1
            if b in (0, 8):
                l_v[qs, rows, :] = l
                acc_v[qs, rows, :] = pv
            else:
                l_v[qs, rows, :] += l
                acc_v[qs, rows, :] += pv

    @scoped
    def finish(p):
        for qs in range(2):
            o = []
            for a in range(2):
                rows = pl.ds(SPAN * a, SPAN)
                l = jnp.sum(l_v[qs, rows, :], axis=1, keepdims=True)
                o.append(acc_v[qs, rows, :] / l)
            both = jnp.where(lane < VDIM, o[0], o[1]).astype(BF16)
            os_v[p, 2 * qs] = both[:128]
            os_v[p, 2 * qs + 1] = both[128:]

    def oblk(blk, p, src):
        return oall_v.at[pl.ds(pl.multiple_of(128 * blk, 128), 128), pl.ds(pl.multiple_of(512 * p + 128 * src, 128), 128)]

    def o_z(p, d):
        to = lax.rem(z + d, MODEL)
        return remote(os_v.at[p, to], oblk(dp, p, z),
                      oz_ssem.at[p, d - 1], oz_rsem.at[p, d - 1], dev(m=to))

    def o_z_wait(p, d):
        src = lax.rem(z + MODEL - d, MODEL)
        remote(os_v.at[p, z], oblk(dp, p, src),
               oz_ssem.at[p, d - 1], oz_rsem.at[p, d - 1], dev()).wait_recv()

    def o_x(p, src_dp, to):
        part = oall_v.at[pl.ds(pl.multiple_of(128 * src_dp, 128), 128), pl.ds(512 * p, 512)]
        return remote(part, part, ox_ssem.at[p], ox_rsem.at[p], dev(d=to))

    @scoped
    def send_o(p):
        oblk(dp, p, z)[...] = os_v[p, z]
        for d in (1, 2, 3):
            o_z(p, d).start()

    @scoped
    def pass_o(p):
        for d in (1, 2, 3):
            o_z_wait(p, d)
        o_x(p, dp, xn).start()

    with jax.named_scope('scores0'):
        for b in ORDER:
            scores(0, b)
    maxima(0)
    hop(5)
    relay = {
        0: lambda: (hop(6),),
        1: lambda: (hop(7, False),),
        2: lambda: (hop(8, False), pass_o(0)),
        3: lambda: (hop(9, False), pass_o(1), hop(10)),
        4: lambda: (zfwd(7), zfwd(8), zfwd(9), hop(11), pass_o(2)),
    }
    for p in range(PAIRS):
        with jax.named_scope('attn%d' % p):
            for b in ORDER:
                if p + 1 < PAIRS:
                    scores(p + 1, b)
                values(p, b)
        finish(p)
        if p + 1 < PAIRS:
            maxima(p + 1)
        send_o(p)
        relay[p]()
    for q in range(5):
        across(q)
    pass_o(3)
    pass_o(4)
    hop(12)
    for q in range(5, 8):
        across(q)
    hop(13)
    across(8)
    hop(14)
    across(9)
    loads[9].wait()

    with jax.named_scope('drain1'):
        for t in range(2):
            kv_copy(ctx, t, 1, partner).wait_send()
        kv_copy(ctx, 0, 0, ynbr).wait_send()
        kv_copy(ynbr, 0, 2, partner).wait_send()

        @pl.when(ctx >= 2)
        def _():
            kv_copy(ctx, 1, 0, ynbr).wait_send()

        @pl.when(ctx < 2)
        def _():
            kv_copy(ynbr, 1, 2, partner).wait_send()

        @pl.when(z < MODEL - 1)
        def _():
            w_own(1).wait_send()

        @pl.when(z > 0)
        def _():
            w_own(0).wait_send()

        for p in range(PAIRS):
            for d in (1, 2, 3):
                o_z(p, d).wait_send()
    def ycols(half, n):
        return out_h.at[:, pl.ds(pl.multiple_of(half * NHALF + SUBC * n, 128), SUBC)]

    def y_back(n):
        return remote(yst_v.at[xn, n], ycols(dp, n), yb_ssem.at[n], yb_rsem.at[n], dev(d=xn))

    def y_come(n):
        return remote(yst_v.at[xn, n], ycols(xn, n), yb_ssem.at[n], yb_rsem.at[n], dev())

    def y_local(n):
        return pltpu.make_async_copy(yst_v.at[dp, n], ycols(dp, n), yl_sem.at[n])

    def wcols(ps, n):
        return jnp.concatenate([wall_v[s, pl.ds(128 * p, 128), pl.ds(SUBC * n, SUBC)] for p in ps for s in range(MODEL)], axis=0)

    def have_w(n):
        across(2 * NSUB + n)
        with jax.named_scope('wdwait'):
            for j in (1, 2, 3):
                each_share(j, lambda s, sign: (wait_wd(s, 0, n), wait_wd(s, 1, n)))

    def finish_y(n, y):
        yst_v[0, n] = y[:128].astype(BF16)
        yst_v[1, n] = y[128:].astype(BF16)
        y_back(n).start()
        y_local(n).start()

    EARLY = 2
    with jax.named_scope('oxwait'):
        for p in range(PAIRS - 1):
            o_x(p, xn, dp).wait_recv()
    for n in range(EARLY):
        have_w(n)
        with jax.named_scope('finala%d' % n):
            yacc_v[n] = dot(oall_v[:, pl.ds(0, 2048)], wcols(range(PAIRS - 1), n))
    with jax.named_scope('oxwait4'):
        o_x(PAIRS - 1, xn, dp).wait_recv()
    for n in range(EARLY):
        with jax.named_scope('finalb%d' % n):
            finish_y(n, yacc_v[n] + dot(oall_v[:, pl.ds(2048, 512)], wcols((PAIRS - 1,), n)))
    for n in range(EARLY, NSUB):
        have_w(n)
        with jax.named_scope('final%d' % n):
            finish_y(n, dot(oall_v[...], wcols(range(PAIRS), n)))

    def sent(s, sign):
        to = z - sign

        @pl.when((to >= 0) & (to < MODEL))
        def _():
            w_fwd_z(s, to).wait_send()
        w_fwd_y(s).wait_send()
        w_fwd_d(s, 0).wait_send()
        w_fwd_d(s, 1).wait_send()

    with jax.named_scope('drain2'):
        for j in (1, 2, 3):
            each_share(j, sent)
        for p in range(PAIRS):
            o_x(p, dp, xn).wait_send()
        for n in range(NSUB):
            y_back(n).wait_send()
            y_local(n).wait()
            y_come(n).wait_recv()


def layer(x, pos, freq, wdq, gq, wuq, wqr, wdkv, gkv, wkr, wuk, wuv, wout):
    hb = pl.BlockSpec(memory_space=pl.ANY)
    dma = pltpu.SemaphoreType.DMA
    return pl.pallas_call(
        kernel,
        out_shape=jax.ShapeDtypeStruct((ROWS // MODEL, HIDDEN), BF16),
        in_specs=[hb] * 13,
        out_specs=hb,
        scratch_shapes=[
            pltpu.VMEM((1, ROWS), jnp.int32),
            pltpu.VMEM((1, 128), F32),
            pltpu.VMEM((Q_RANK // 128, 128), F32),
            pltpu.VMEM((1, KV_RANK), F32),
            pltpu.VMEM((ROWS, HIDDEN), BF16),
            pltpu.VMEM((HIDDEN, Q_RANK), BF16),
            pltpu.VMEM((Q_RANK, HEADS * NOPE), BF16),
            pltpu.VMEM((HEADS * ROPE, Q_RANK), BF16),
            pltpu.VMEM((HIDDEN, KV_RANK), BF16),
            pltpu.VMEM((ROPE, HIDDEN), BF16),
            pltpu.VMEM((KV_RANK, 2 * HV), BF16),
            pltpu.VMEM((ROWS, 128), F32),
            pltpu.VMEM((ROWS, 128), F32),
            pltpu.VMEM((KV_RANK, 1024), BF16),
            pltpu.VMEM((CTX, 2, SPAN + KRP, KV_RANK), BF16),
            pltpu.VMEM((ROWS, Q_RANK), BF16),
            pltpu.VMEM((PAIRS, 2, 2 * SPAN, 256), BF16),
            pltpu.VMEM((NSPAN, SPAN, HEADS * NOPE), BF16),
            pltpu.VMEM((NSPAN, SPAN, HEADS * VDIM), BF16),
            pltpu.VMEM((NSPAN, SPAN, 128), BF16),
            pltpu.VMEM((2, 9, 2 * SPAN, SPAN), F32),
            pltpu.VMEM((2, 2, 2 * SPAN, 128), F32),
            pltpu.VMEM((2, 2 * SPAN, 128), F32),
            pltpu.VMEM((2, 2 * SPAN, 128), F32),
            pltpu.VMEM((2, 2 * SPAN, 128), F32),
            pltpu.VMEM((PAIRS, MODEL, 128, 128), BF16),
            pltpu.VMEM((2 * 128, HIDDEN), BF16),
            pltpu.VMEM((MODEL, HV, NHALF), BF16),
            pltpu.VMEM((2, NSUB, 128, SUBC), BF16),
            pltpu.VMEM((2, 256, SUBC), F32),
            dma((14,)),
            dma((3, 2)), dma((3, 2)),
            dma((2,)), dma((MODEL,)), dma((MODEL, NSUB)),
            dma((MODEL,)), dma((MODEL, NSUB)),
            dma((MODEL, 2)), dma((MODEL, 2, NSUB)),
            dma((PAIRS, 3)), dma((PAIRS, 3)),
            dma((PAIRS,)), dma((PAIRS,)),
            dma((NSUB,)), dma((NSUB,)), dma((NSUB,)),
        ],
        compiler_params=pltpu.CompilerParams(collective_id=0, has_side_effects=True, vmem_limit_bytes=60 * 1024 * 1024),
        name='mla_layer',
    )(x, pos, freq, gq, gkv, wdq, wuq, wqr, wdkv, wkr, wuk, wuv, wout)


def solution(mesh):
    inv_freq = (ROPE_BASE ** (-(np.arange(ROPE // 2, dtype=np.float64) * 2.0 / ROPE))).astype(np.float32)
    freq = np.tile(inv_freq, 128 // (ROPE // 2))[None, :]

    def local(x_tokens, positions, w_dq, gain_q, w_uq, w_qr, w_dkv, gain_kv, w_kr, w_uk, w_uv, w_out):
        return layer(x_tokens, positions[None, :], jnp.asarray(freq), w_dq, gain_q.reshape(Q_RANK // 128, 128), w_uq,
                     w_qr.T, w_dkv, gain_kv[None, :], w_kr.T, w_uk, w_uv, w_out)

    in_specs = (P(('dp', 'ctx'), None), P(('dp', 'ctx')), P(), P(), P(None, 'model'), P(None, 'model'), P(), P(), P(), P(None, 'model'), P(None, 'model'), P('model', None))
    out_specs = P(('dp', 'ctx', 'model'), None)
    return jax.shard_map(local, mesh=mesh, in_specs=in_specs, out_specs=out_specs, check_vma=False)
```

```python
import functools

import jax
import jax.numpy as jnp
import numpy as np
from jax import lax
from jax.experimental import pallas as pl
from jax.experimental.pallas import tpu as pltpu
from jax.sharding import PartitionSpec as P

MESH = pl.DeviceIdType.MESH


def scoped(fn):
    @functools.wraps(fn)
    def run(*args):
        tag = "_".join(str(a) for a in args if isinstance(a, int))
        with jax.named_scope(fn.__name__ + tag):
            return fn(*args)
    return run


F32 = jnp.float32
BF16 = jnp.bfloat16

HIDDEN = 2560
Q_RANK = 768
KV_RANK = 256
HEADS = 10
PAIRS = HEADS // 2
NOPE = 64
ROPE = 32
VDIM = 64
ROWS = 512
SPAN = 256
NSPAN = 8
CTX = 4
MODEL = 4
HV = HEADS * VDIM
NHALF = HIDDEN // 2
QROWS = HV // 4
NSUB = 5
SUBC = NHALF // NSUB
KRP = SPAN // 8
EPS = 1e-6
ROPE_BASE = 10000.0
SM_SCALE = float((NOPE + ROPE) ** -0.5 * np.log2(np.e))
NEG = -1e30


def dot(a, b):
    return jnp.dot(a, b, preferred_element_type=F32)


def dot_nt(a, b):
    return lax.dot_general(a, b, (((1,), (1,)), ((), ())), preferred_element_type=F32)


def rms(h, gain):
    ms = jnp.mean(h * h, axis=-1, keepdims=True)
    return (h * lax.rsqrt(ms + EPS) * gain).astype(BF16)


def kernel(x_h, pos_h, freq_h, gq_h, gkv_h, wdq_h, wuq_h, wqr_h, wdkv_h, wkr_h, wuk_h, wuv_h, wout_h, out_h,
           pos_r, freq_r, gq_r, gkv_r, x_v, wdq_v, wuq_v, wqr_v, wdkv_v, wkr_v, wkv_v,
           cos_v, sin_v, tile_v, lat_v, cq_v, qm_v, k_v, v_v, kr_v, s_v, mx_v, mb_v, l_v, acc_v,
           os_v, oall_v, wall_v, yst_v, yacc_v,
           lsem, kv_ssem, kv_rsem, wz_own, wz_ssem, wz_rsem, wy_ssem, wy_rsem, wd_ssem, wd_rsem,
           oz_ssem, oz_rsem, ox_ssem, ox_rsem, yb_ssem, yb_rsem, yl_sem):
    dp = lax.axis_index('dp')
    z = lax.axis_index('model')
    ctx = lax.axis_index('ctx')
    partner = ctx + 1 - 2 * lax.rem(ctx, 2)
    ynbr = lax.rem(ctx + 2, CTX)
    diag = lax.rem(partner + 2, CTX)
    xn = 1 - dp

    def dev(d=None, m=None, c=None):
        return (dp if d is None else d, z if m is None else m, ctx if c is None else c)

    def remote(src, dst, ss, rs, where):
        return pltpu.make_async_remote_copy(src_ref=src, dst_ref=dst, send_sem=ss, recv_sem=rs,
                                            device_id=where, device_id_type=MESH)

    def local(src, dst, idx):
        return pltpu.make_async_copy(src, dst, lsem.at[idx])

    small = [local(pos_h, pos_r, 14), local(freq_h, freq_r, 15), local(gq_h, gq_r, 16), local(gkv_h, gkv_r, 17)]
    loads = [
        local(wkr_h, wkr_v, 0),
        local(x_h.at[pl.ds(0, SPAN)], x_v.at[pl.ds(0, SPAN)], 1),
        local(wdkv_h, wdkv_v, 2),
        local(x_h.at[pl.ds(SPAN, SPAN)], x_v.at[pl.ds(SPAN, SPAN)], 3),
        local(wdq_h, wdq_v, 4),
        local(wuq_h, wuq_v, 5),
        local(wqr_h, wqr_v, 6),
        local(wuk_h, wkv_v.at[:, pl.ds(0, HV)], 7),
        local(wuv_h, wkv_v.at[:, pl.ds(HV, HV)], 8),
    ] + [
        local(wout_h.at[:, pl.ds(pl.multiple_of(dp * NHALF + SUBC * n, 128), SUBC)], wall_v.at[z, n], 9 + n)
        for n in range(NSUB)
    ]
    for c in small + loads:
        c.start()

    barrier = pltpu.get_barrier_semaphore()
    peers = [dev(m=lax.rem(z + d, MODEL)) for d in (1, 2, 3)] + [dev(d=xn), dev(c=partner), dev(c=ynbr)]
    for p in peers:
        pl.semaphore_signal(barrier, inc=1, device_id=p, device_id_type=MESH)
    with jax.named_scope('barrier'):
        pl.semaphore_wait(barrier, len(peers))

    def wpiece(s, c, n=None):
        rows = pl.ds(pl.multiple_of(c * QROWS, 16), QROWS)
        return wall_v.at[s, :, rows] if n is None else wall_v.at[s, n, rows]

    def wsrc(n):
        rows = pl.ds(pl.multiple_of(ctx * QROWS, 16), QROWS)
        return wout_h.at[rows, pl.ds(pl.multiple_of(dp * NHALF + SUBC * n, 128), SUBC)]

    def w_own(up, n=None):
        src = wpiece(z, ctx) if n is None else wsrc(n)
        return remote(src, wpiece(z, ctx, n), wz_own.at[up], wz_rsem.at[z, n or 0], dev(m=z + 2 * up - 1))

    def w_fwd_z(s, to, n=None):
        return remote(wpiece(s, ctx, n), wpiece(s, ctx, n), wz_ssem.at[s], wz_rsem.at[s, n or 0], dev(m=to))

    def w_fwd_y(s, n=None):
        return remote(wpiece(s, ctx, n), wpiece(s, ctx, n), wy_ssem.at[s], wy_rsem.at[s, n or 0], dev(c=ynbr))

    def w_fwd_d(s, which, n=None):
        c = ctx if which == 0 else ynbr
        return remote(wpiece(s, c, n), wpiece(s, c, n), wd_ssem.at[s, which], wd_rsem.at[s, which, n or 0], dev(c=partner))

    def wait_wz(s, n):
        remote(wpiece(s, ctx, n), wpiece(s, ctx, n), wz_ssem.at[s], wz_rsem.at[s, n], dev()).wait_recv()

    def wait_wy(s, n):
        remote(wpiece(s, ynbr, n), wpiece(s, ynbr, n), wy_ssem.at[s], wy_rsem.at[s, n], dev()).wait_recv()

    def wait_wd(s, which, n):
        c = partner if which == 0 else diag
        remote(wpiece(s, c, n), wpiece(s, c, n), wd_ssem.at[s, which], wd_rsem.at[s, which, n], dev()).wait_recv()

    @pl.when(z < MODEL - 1)
    def _():
        for n in range(NSUB):
            w_own(1, n).start()

    @pl.when(z > 0)
    def _():
        for n in range(NSUB):
            w_own(0, n).start()

    def each_share(j, fn):
        for sign in (-1, 1):
            s = z + sign * j

            @pl.when((s >= 0) & (s < MODEL))
            def _(s=s, sign=sign):
                fn(s, sign)

    @scoped
    def zfwd(q):
        j, n = q // NSUB + 1, q % NSUB

        def step(s, sign):
            to = z - sign

            @pl.when((to >= 0) & (to < MODEL))
            def _():
                w_fwd_z(s, to, n).start()
        each_share(j, step)

    @scoped
    def hop(q, forward=True):
        j, n = q // NSUB + 1, q % NSUB

        def step(s, sign):
            wait_wz(s, n)
            to = z - sign
            if forward:
                @pl.when((to >= 0) & (to < MODEL))
                def _():
                    w_fwd_z(s, to, n).start()
            w_fwd_y(s, n).start()
            w_fwd_d(s, 0, n).start()
        each_share(j, step)

    @scoped
    def across(q):
        j, n = q // NSUB + 1, q % NSUB

        def step(s, sign):
            wait_wy(s, n)
            w_fwd_d(s, 1, n).start()
        each_share(j, step)

    lane = lax.broadcasted_iota(jnp.int32, (1, 128), 1)
    with jax.named_scope('small'):
        for c in small:
            c.wait()
    with jax.named_scope('tables'):
        for g in range(ROWS // 128):
            row = pos_r[:, pl.ds(128 * g, 128)].astype(F32)
            col = jnp.transpose(jnp.broadcast_to(row, (128, 128)), (1, 0))
            ang = col * freq_r[...]
            cos_v[pl.ds(128 * g, 128), :] = jnp.cos(ang)
            sin_v[pl.ds(128 * g, 128), :] = jnp.sin(ang)
    rr = lax.broadcasted_iota(jnp.int32, (KV_RANK, 1024), 0)
    cc = lax.broadcasted_iota(jnp.int32, (KV_RANK, 1024), 1)
    tile_v[...] = jnp.where((rr // ROPE == cc // 128) & (rr % ROPE == cc % ROPE), 1.0, 0.0).astype(BF16)
    low = (lane % ROPE) < (ROPE // 2)

    def rope(v, r0):
        up = pltpu.roll(v, 128 - ROPE // 2, 1)
        dn = pltpu.roll(v, ROPE // 2, 1)
        rot = jnp.where(low, -up, dn)
        return v * cos_v[pl.ds(r0, SPAN), :] + rot * sin_v[pl.ds(r0, SPAN), :]

    def kv_copy(c, t, idx, to):
        return remote(lat_v.at[c, t], lat_v.at[c, t], kv_ssem.at[idx, t], kv_rsem.at[idx, t], dev(c=to))

    loads[0].wait()
    wkr4 = jnp.concatenate([wkr_v[...]] * 4, axis=0)
    gkv = gkv_r[...]
    with jax.named_scope('ckv'):
        for t in range(2):
            r0 = t * SPAN
            if t == 0:
                loads[1].wait()
                loads[2].wait()
            else:
                loads[3].wait()
            xs = x_v[pl.ds(r0, SPAN), :]
            lat_v[ctx, t, pl.ds(0, SPAN), :] = rms(dot(xs, wdkv_v[...]), gkv)
            kr = rope(dot_nt(xs, wkr4), r0)
            for half in range(2):
                packed = kr[128 * half:128 * half + KRP]
                for g in range(1, 4):
                    a = 128 * half + KRP * g
                    packed = jnp.where(lane // ROPE == g, kr[a:a + KRP], packed)
                lat_v[ctx, t, pl.ds(SPAN, KRP), pl.ds(128 * half, 128)] = packed.astype(BF16)
            if t == 0:
                kv_copy(ctx, t, 0, ynbr).start()
            else:
                @pl.when(ctx >= 2)
                def _():
                    kv_copy(ctx, 1, 0, ynbr).start()
            kv_copy(ctx, t, 1, partner).start()

    with jax.named_scope('ld4'):
        loads[4].wait()
    gq = jnp.concatenate([gq_r[g:g + 1, :] for g in range(Q_RANK // 128)], axis=1)
    with jax.named_scope('cq'):
        for t in range(2):
            cq_v[pl.ds(t * SPAN, SPAN), :] = rms(dot(x_v[pl.ds(t * SPAN, SPAN), :], wdq_v[...]), gq)
    hop(0)
    loads[5].wait()
    loads[6].wait()
    with jax.named_scope('qup'):
        for t in range(2):
            cq = cq_v[pl.ds(t * SPAN, SPAN), :]
            qn = dot(cq, wuq_v[...]).astype(BF16)
            zero = jnp.zeros((SPAN, 128), BF16)
            for p in range(PAIRS):
                blk = qn[:, 128 * p:128 * p + 128]
                qm_v[p, t, pl.ds(0, SPAN), pl.ds(0, 128)] = jnp.where(lane < NOPE, blk, zero)
                qm_v[p, t, pl.ds(SPAN, SPAN), pl.ds(0, 128)] = jnp.where(lane < NOPE, zero, blk)
            for b in range(3):
                w = wqr_v[pl.ds(128 * b, 128), :] if b < 2 else jnp.concatenate([wqr_v[pl.ds(256, 64), :]] * 2, axis=0)
                qr = rope(dot_nt(cq, w), t * SPAN).astype(BF16)
                for h in range(4 * b, min(4 * b + 4, HEADS)):
                    qm_v[h // 2, t, pl.ds(SPAN * (h % 2), SPAN), pl.ds(128, 128)] = jnp.where(lane // ROPE == h % 4, qr, zero)

    hop(1)

    @scoped
    def up(c, t):
        sp = c if t == 0 else NSPAN - 1 - c
        lat = lat_v[c, t, pl.ds(0, SPAN), :]
        kv = dot(lat, wkv_v[...]).astype(BF16)
        k_v[sp] = kv[:, :HV]
        v_v[sp] = kv[:, HV:]
        big = dot(lat_v[c, t, pl.ds(SPAN, KRP), :], tile_v[...]).astype(BF16)
        for g in range(8):
            kr_v[sp, pl.ds(KRP * g, KRP), :] = big[:, 128 * g:128 * g + 128]

    def up_late(c):
        @pl.when(c >= ctx)
        def _():
            up(c, 1)

    loads[7].wait()
    loads[8].wait()
    up(ctx, 0)
    up(ctx, 1)
    with jax.named_scope('kvw_partner'):
        kv_copy(partner, 0, 1, ctx).wait_recv()
        kv_copy(partner, 1, 1, ctx).wait_recv()
    up(partner, 0)
    up_late(partner)
    hop(2)
    with jax.named_scope('kvw_ynbr'):
        kv_copy(ynbr, 0, 0, ctx).wait_recv()
    kv_copy(ynbr, 0, 2, partner).start()
    up(ynbr, 0)

    @pl.when(ctx < 2)
    def _():
        kv_copy(ynbr, 1, 0, ctx).wait_recv()
        kv_copy(ynbr, 1, 2, partner).start()
        up(ynbr, 1)
    hop(3)
    with jax.named_scope('kvw_diag'):
        kv_copy(diag, 0, 2, ctx).wait_recv()
    up(diag, 0)

    @pl.when(ctx < 2)
    def _():
        kv_copy(diag, 1, 2, ctx).wait_recv()
        up(diag, 1)
    hop(4)

    def block(b):
        if b < 5:
            return 1, NSPAN - 1 - ctx - b
        if b == 8:
            return 0, ctx
        hi = b < NSPAN - ctx
        return jnp.where(hi, 1, 0), jnp.where(hi, NSPAN - 1 - ctx - b, b - (NSPAN - ctx))

    ORDER = (0, 8, 1, 2, 3, 4, 5, 6, 7)
    q_i = lax.broadcasted_iota(jnp.int32, (SPAN, SPAN), 0)
    k_i = lax.broadcasted_iota(jnp.int32, (SPAN, SPAN), 1)
    causal = k_i <= q_i

    def scores(p, b):
        buf = p % 2
        qs, ks = block(b)
        kc = jnp.concatenate([k_v[ks, :, pl.ds(128 * p, 128)], kr_v[ks]], axis=1)
        for a in range(2):
            rows = pl.ds(SPAN * a, SPAN)
            s = dot_nt(qm_v[p, qs, rows, :], kc)
            if b in (0, 8):
                s = jnp.where(causal, s, NEG)
            s_v[buf, b, rows, :] = s
            m = jnp.maximum(s[:, :128], s[:, 128:])
            if b not in (0, 8):
                m = jnp.maximum(mx_v[buf, qs, rows, :], m)
            mx_v[buf, qs, rows, :] = m

    @scoped
    def maxima(p):
        buf = p % 2
        for qs in range(2):
            for a in range(2):
                rows = pl.ds(SPAN * a, SPAN)
                m = jnp.max(mx_v[buf, qs, rows, :], axis=1, keepdims=True)
                mb_v[qs, rows, :] = jnp.broadcast_to(m * SM_SCALE, (SPAN, 128))

    def values(p, b):
        buf = p % 2
        qs, ks = block(b)
        vb = v_v[ks, :, pl.ds(128 * p, 128)]
        for a in range(2):
            rows = pl.ds(SPAN * a, SPAN)
            m = mb_v[qs, rows, :]
            e0 = jnp.exp2(s_v[buf, b, rows, pl.ds(0, 128)] * SM_SCALE - m)
            e1 = jnp.exp2(s_v[buf, b, rows, pl.ds(128, 128)] * SM_SCALE - m)
            pv = dot(jnp.concatenate([e0.astype(BF16), e1.astype(BF16)], axis=1), vb)
            l = e0 + e1
            if b in (0, 8):
                l_v[qs, rows, :] = l
                acc_v[qs, rows, :] = pv
            else:
                l_v[qs, rows, :] += l
                acc_v[qs, rows, :] += pv

    @scoped
    def finish(p):
        for qs in range(2):
            o = []
            for a in range(2):
                rows = pl.ds(SPAN * a, SPAN)
                l = jnp.sum(l_v[qs, rows, :], axis=1, keepdims=True)
                o.append(acc_v[qs, rows, :] / l)
            both = jnp.where(lane < VDIM, o[0], o[1]).astype(BF16)
            os_v[p, 2 * qs] = both[:128]
            os_v[p, 2 * qs + 1] = both[128:]

    def oblk(blk, p, src):
        return oall_v.at[blk, p, src]

    def o_z(p, d):
        to = lax.rem(z + d, MODEL)
        return remote(os_v.at[p, to], oblk(dp, p, z),
                      oz_ssem.at[p, d - 1], oz_rsem.at[p, d - 1], dev(m=to))

    def o_z_wait(p, d):
        src = lax.rem(z + MODEL - d, MODEL)
        remote(os_v.at[p, z], oblk(dp, p, src),
               oz_ssem.at[p, d - 1], oz_rsem.at[p, d - 1], dev()).wait_recv()

    def o_x(p, src_dp, to):
        part = oall_v.at[src_dp, p]
        return remote(part, part, ox_ssem.at[p], ox_rsem.at[p], dev(d=to))

    @scoped
    def send_o(p):
        oblk(dp, p, z)[...] = os_v[p, z]
        for d in (1, 2, 3):
            o_z(p, d).start()

    @scoped
    def pass_o(p):
        for d in (1, 2, 3):
            o_z_wait(p, d)
        o_x(p, dp, xn).start()

    with jax.named_scope('scores0'):
        for b in ORDER:
            scores(0, b)
    maxima(0)
    hop(5)
    relay = {
        0: lambda: (hop(6),),
        1: lambda: (hop(7, False),),
        2: lambda: (hop(8, False),),
        3: lambda: (hop(9, False), pass_o(0), hop(10)),
        4: lambda: (zfwd(7), zfwd(8), zfwd(9), hop(11), pass_o(1), pass_o(2)),
    }
    for p in range(PAIRS):
        with jax.named_scope('attn%d' % p):
            for b in ORDER:
                if p + 1 < PAIRS:
                    scores(p + 1, b)
                values(p, b)
        finish(p)
        if p + 1 < PAIRS:
            maxima(p + 1)
        send_o(p)
        relay[p]()
    for q in range(5):
        across(q)
    pass_o(3)
    pass_o(4)
    hop(12)
    for q in range(5, 8):
        across(q)
    hop(13)
    across(8)
    hop(14)
    across(9)
    for n in range(NSUB):
        loads[9 + n].wait()

    with jax.named_scope('drain1'):
        for t in range(2):
            kv_copy(ctx, t, 1, partner).wait_send()
        kv_copy(ctx, 0, 0, ynbr).wait_send()
        kv_copy(ynbr, 0, 2, partner).wait_send()

        @pl.when(ctx >= 2)
        def _():
            kv_copy(ctx, 1, 0, ynbr).wait_send()

        @pl.when(ctx < 2)
        def _():
            kv_copy(ynbr, 1, 2, partner).wait_send()

        @pl.when(z < MODEL - 1)
        def _():
            w_own(1).wait_send()

        @pl.when(z > 0)
        def _():
            w_own(0).wait_send()

        for p in range(PAIRS):
            for d in (1, 2, 3):
                o_z(p, d).wait_send()
    def ycols(half, n):
        return out_h.at[:, pl.ds(pl.multiple_of(half * NHALF + SUBC * n, 128), SUBC)]

    def y_back(n):
        return remote(yst_v.at[xn, n], ycols(dp, n), yb_ssem.at[n], yb_rsem.at[n], dev(d=xn))

    def y_come(n):
        return remote(yst_v.at[xn, n], ycols(xn, n), yb_ssem.at[n], yb_rsem.at[n], dev())

    def y_local(n):
        return pltpu.make_async_copy(yst_v.at[dp, n], ycols(dp, n), yl_sem.at[n])

    def wcols(ps, n):
        return jnp.concatenate([wall_v[s, n, pl.ds(128 * p, 128), :] for p in ps for s in range(MODEL)], axis=0)

    def orows(ps):
        return jnp.concatenate([jnp.concatenate([oall_v[blk, p, s] for p in ps for s in range(MODEL)], axis=1) for blk in range(2)], axis=0)

    def have_w(n):
        with jax.named_scope('wdwait'):
            for j in (1, 2, 3):
                each_share(j, lambda s, sign: (wait_wd(s, 0, n), wait_wd(s, 1, n)))

    def finish_y(n, y):
        yst_v[0, n] = y[:128].astype(BF16)
        yst_v[1, n] = y[128:].astype(BF16)
        y_back(n).start()
        y_local(n).start()

    early, last = range(PAIRS - 1), (PAIRS - 1,)

    def final_a(n):
        have_w(n)
        with jax.named_scope('finala%d' % n):
            yacc_v[n] = dot(orows(early), wcols(early, n))

    def final_b(n):
        with jax.named_scope('finalb%d' % n):
            finish_y(n, yacc_v[n] + dot(orows(last), wcols(last, n)))

    def final(n):
        have_w(n)
        with jax.named_scope('final%d' % n):
            finish_y(n, dot(orows(range(PAIRS)), wcols(range(PAIRS), n)))

    across(10)
    across(11)
    with jax.named_scope('oxwait'):
        for p in early:
            o_x(p, xn, dp).wait_recv()
    final_a(0)
    across(12)
    final_a(1)
    with jax.named_scope('oxwait4'):
        o_x(PAIRS - 1, xn, dp).wait_recv()
    final_b(0)
    across(13)
    final_b(1)
    across(14)
    final(2)
    final(3)
    final(4)

    def sent(s, sign):
        to = z - sign

        @pl.when((to >= 0) & (to < MODEL))
        def _():
            w_fwd_z(s, to).wait_send()
        w_fwd_y(s).wait_send()
        w_fwd_d(s, 0).wait_send()
        w_fwd_d(s, 1).wait_send()

    with jax.named_scope('drain2'):
        for j in (1, 2, 3):
            each_share(j, sent)
        for p in range(PAIRS):
            o_x(p, dp, xn).wait_send()
        for n in range(NSUB):
            y_back(n).wait_send()
            y_local(n).wait()
            y_come(n).wait_recv()


def layer(x, pos, freq, wdq, gq, wuq, wqr, wdkv, gkv, wkr, wuk, wuv, wout):
    hb = pl.BlockSpec(memory_space=pl.ANY)
    dma = pltpu.SemaphoreType.DMA
    return pl.pallas_call(
        kernel,
        out_shape=jax.ShapeDtypeStruct((ROWS // MODEL, HIDDEN), BF16),
        in_specs=[hb] * 13,
        out_specs=hb,
        scratch_shapes=[
            pltpu.VMEM((1, ROWS), jnp.int32),
            pltpu.VMEM((1, 128), F32),
            pltpu.VMEM((Q_RANK // 128, 128), F32),
            pltpu.VMEM((1, KV_RANK), F32),
            pltpu.VMEM((ROWS, HIDDEN), BF16),
            pltpu.VMEM((HIDDEN, Q_RANK), BF16),
            pltpu.VMEM((Q_RANK, HEADS * NOPE), BF16),
            pltpu.VMEM((HEADS * ROPE, Q_RANK), BF16),
            pltpu.VMEM((HIDDEN, KV_RANK), BF16),
            pltpu.VMEM((ROPE, HIDDEN), BF16),
            pltpu.VMEM((KV_RANK, 2 * HV), BF16),
            pltpu.VMEM((ROWS, 128), F32),
            pltpu.VMEM((ROWS, 128), F32),
            pltpu.VMEM((KV_RANK, 1024), BF16),
            pltpu.VMEM((CTX, 2, SPAN + KRP, KV_RANK), BF16),
            pltpu.VMEM((ROWS, Q_RANK), BF16),
            pltpu.VMEM((PAIRS, 2, 2 * SPAN, 256), BF16),
            pltpu.VMEM((NSPAN, SPAN, HEADS * NOPE), BF16),
            pltpu.VMEM((NSPAN, SPAN, HEADS * VDIM), BF16),
            pltpu.VMEM((NSPAN, SPAN, 128), BF16),
            pltpu.VMEM((2, 9, 2 * SPAN, SPAN), F32),
            pltpu.VMEM((2, 2, 2 * SPAN, 128), F32),
            pltpu.VMEM((2, 2 * SPAN, 128), F32),
            pltpu.VMEM((2, 2 * SPAN, 128), F32),
            pltpu.VMEM((2, 2 * SPAN, 128), F32),
            pltpu.VMEM((PAIRS, MODEL, 128, 128), BF16),
            pltpu.VMEM((2, PAIRS, MODEL, 128, 128), BF16),
            pltpu.VMEM((MODEL, NSUB, HV, SUBC), BF16),
            pltpu.VMEM((2, NSUB, 128, SUBC), BF16),
            pltpu.VMEM((2, 256, SUBC), F32),
            dma((18,)),
            dma((3, 2)), dma((3, 2)),
            dma((2,)), dma((MODEL,)), dma((MODEL, NSUB)),
            dma((MODEL,)), dma((MODEL, NSUB)),
            dma((MODEL, 2)), dma((MODEL, 2, NSUB)),
            dma((PAIRS, 3)), dma((PAIRS, 3)),
            dma((PAIRS,)), dma((PAIRS,)),
            dma((NSUB,)), dma((NSUB,)), dma((NSUB,)),
        ],
        compiler_params=pltpu.CompilerParams(collective_id=0, has_side_effects=True, vmem_limit_bytes=60 * 1024 * 1024),
        name='mla_layer',
    )(x, pos, freq, gq, gkv, wdq, wuq, wqr, wdkv, wkr, wuk, wuv, wout)


def solution(mesh):
    inv_freq = (ROPE_BASE ** (-(np.arange(ROPE // 2, dtype=np.float64) * 2.0 / ROPE))).astype(np.float32)
    freq = np.tile(inv_freq, 128 // (ROPE // 2))[None, :]

    def local(x_tokens, positions, w_dq, gain_q, w_uq, w_qr, w_dkv, gain_kv, w_kr, w_uk, w_uv, w_out):
        return layer(x_tokens, positions[None, :], jnp.asarray(freq), w_dq, gain_q.reshape(Q_RANK // 128, 128), w_uq,
                     w_qr.T, w_dkv, gain_kv[None, :], w_kr.T, w_uk, w_uv, w_out)

    in_specs = (P(('dp', 'ctx'), None), P(('dp', 'ctx')), P(), P(), P(None, 'model'), P(None, 'model'), P(), P(), P(), P(None, 'model'), P(None, 'model'), P('model', None))
    out_specs = P(('dp', 'ctx', 'model'), None)
    return jax.shard_map(local, mesh=mesh, in_specs=in_specs, out_specs=out_specs, check_vma=False)
```

```python
import functools

import jax
import jax.numpy as jnp
import numpy as np
from jax import lax
from jax.experimental import pallas as pl
from jax.experimental.pallas import tpu as pltpu
from jax.sharding import PartitionSpec as P

MESH = pl.DeviceIdType.MESH


def scoped(fn):
    @functools.wraps(fn)
    def run(*args):
        tag = "_".join(str(a) for a in args if isinstance(a, int))
        with jax.named_scope(fn.__name__ + tag):
            return fn(*args)
    return run


F32 = jnp.float32
BF16 = jnp.bfloat16

HIDDEN = 2560
Q_RANK = 768
KV_RANK = 256
HEADS = 10
PAIRS = HEADS // 2
NOPE = 64
ROPE = 32
VDIM = 64
ROWS = 512
SPAN = 256
NSPAN = 8
CTX = 4
MODEL = 4
HV = HEADS * VDIM
NHALF = HIDDEN // 2
QROWS = HV // 4
NSUB = 5
SUBC = NHALF // NSUB
KRP = SPAN // 8
EPS = 1e-6
ROPE_BASE = 10000.0
SM_SCALE = float((NOPE + ROPE) ** -0.5 * np.log2(np.e))
NEG = -1e30


def dot(a, b):
    return jnp.dot(a, b, preferred_element_type=F32)


def dot_nt(a, b):
    return lax.dot_general(a, b, (((1,), (1,)), ((), ())), preferred_element_type=F32)


def rms(h, gain):
    ms = jnp.mean(h * h, axis=-1, keepdims=True)
    return (h * lax.rsqrt(ms + EPS) * gain).astype(BF16)


def kernel(x_h, pos_h, freq_h, gq_h, gkv_h, wdq_h, wuq_h, wqr_h, wdkv_h, wkr_h, wuk_h, wuv_h, wout_h, out_h,
           pos_r, freq_r, gq_r, gkv_r, x_v, wdq_v, wuq_v, wqr_v, wdkv_v, wkr_v, wkv_v,
           cos_v, sin_v, tile_v, lat_v, cq_v, qm_v, k_v, v_v, kr_v, s_v, mx_v, mb_v, l_v, acc_v,
           os_v, oall_v, wall_v, yst_v, yacc_v,
           lsem, kv_ssem, kv_rsem, wz_own, wz_ssem, wz_rsem, wy_ssem, wy_rsem, wd_ssem, wd_rsem,
           oz_ssem, oz_rsem, ox_ssem, ox_rsem, yb_ssem, yb_rsem, yl_sem):
    dp = lax.axis_index('dp')
    z = lax.axis_index('model')
    ctx = lax.axis_index('ctx')
    partner = ctx + 1 - 2 * lax.rem(ctx, 2)
    ynbr = lax.rem(ctx + 2, CTX)
    diag = lax.rem(partner + 2, CTX)
    xn = 1 - dp

    def dev(d=None, m=None, c=None):
        return (dp if d is None else d, z if m is None else m, ctx if c is None else c)

    def remote(src, dst, ss, rs, where):
        return pltpu.make_async_remote_copy(src_ref=src, dst_ref=dst, send_sem=ss, recv_sem=rs,
                                            device_id=where, device_id_type=MESH)

    def local(src, dst, idx):
        return pltpu.make_async_copy(src, dst, lsem.at[idx])

    small = [local(pos_h, pos_r, 14), local(freq_h, freq_r, 15), local(gq_h, gq_r, 16), local(gkv_h, gkv_r, 17)]
    loads = [
        local(wkr_h, wkr_v, 0),
        local(x_h.at[pl.ds(0, SPAN)], x_v.at[pl.ds(0, SPAN)], 1),
        local(wdkv_h, wdkv_v, 2),
        local(x_h.at[pl.ds(SPAN, SPAN)], x_v.at[pl.ds(SPAN, SPAN)], 3),
        local(wdq_h, wdq_v, 4),
        local(wuq_h, wuq_v, 5),
        local(wqr_h, wqr_v, 6),
        local(wuk_h, wkv_v.at[:, pl.ds(0, HV)], 7),
        local(wuv_h, wkv_v.at[:, pl.ds(HV, HV)], 8),
    ] + [
        local(wout_h.at[:, pl.ds(pl.multiple_of(dp * NHALF + SUBC * n, 128), SUBC)], wall_v.at[z, n], 9 + n)
        for n in range(NSUB)
    ]
    for c in small + loads:
        c.start()

    barrier = pltpu.get_barrier_semaphore()
    peers = [dev(m=lax.rem(z + d, MODEL)) for d in (1, 2, 3)] + [dev(d=xn), dev(c=partner), dev(c=ynbr)]
    for p in peers:
        pl.semaphore_signal(barrier, inc=1, device_id=p, device_id_type=MESH)
    with jax.named_scope('barrier'):
        pl.semaphore_wait(barrier, len(peers))

    def wpiece(s, c, n=None):
        rows = pl.ds(pl.multiple_of(c * QROWS, 16), QROWS)
        return wall_v.at[s, :, rows] if n is None else wall_v.at[s, n, rows]

    def wsrc(n):
        rows = pl.ds(pl.multiple_of(ctx * QROWS, 16), QROWS)
        return wout_h.at[rows, pl.ds(pl.multiple_of(dp * NHALF + SUBC * n, 128), SUBC)]

    def w_own(up, n=None):
        src = wpiece(z, ctx) if n is None else wsrc(n)
        return remote(src, wpiece(z, ctx, n), wz_own.at[up], wz_rsem.at[z, n or 0], dev(m=z + 2 * up - 1))

    def w_fwd_z(s, to, n=None):
        return remote(wpiece(s, ctx, n), wpiece(s, ctx, n), wz_ssem.at[s], wz_rsem.at[s, n or 0], dev(m=to))

    def w_fwd_y(s, n=None):
        return remote(wpiece(s, ctx, n), wpiece(s, ctx, n), wy_ssem.at[s], wy_rsem.at[s, n or 0], dev(c=ynbr))

    def w_fwd_d(s, which, n=None):
        c = ctx if which == 0 else ynbr
        return remote(wpiece(s, c, n), wpiece(s, c, n), wd_ssem.at[s, which], wd_rsem.at[s, which, n or 0], dev(c=partner))

    def wait_wz(s, n):
        remote(wpiece(s, ctx, n), wpiece(s, ctx, n), wz_ssem.at[s], wz_rsem.at[s, n], dev()).wait_recv()

    def wait_wy(s, n):
        remote(wpiece(s, ynbr, n), wpiece(s, ynbr, n), wy_ssem.at[s], wy_rsem.at[s, n], dev()).wait_recv()

    def wait_wd(s, which, n):
        c = partner if which == 0 else diag
        remote(wpiece(s, c, n), wpiece(s, c, n), wd_ssem.at[s, which], wd_rsem.at[s, which, n], dev()).wait_recv()

    @pl.when(z < MODEL - 1)
    def _():
        for n in range(NSUB):
            w_own(1, n).start()

    @pl.when(z > 0)
    def _():
        for n in range(NSUB):
            w_own(0, n).start()

    def each_share(j, fn):
        for sign in (-1, 1):
            s = z + sign * j

            @pl.when((s >= 0) & (s < MODEL))
            def _(s=s, sign=sign):
                fn(s, sign)

    @scoped
    def zfwd(q):
        j, n = q // NSUB + 1, q % NSUB

        def step(s, sign):
            to = z - sign

            @pl.when((to >= 0) & (to < MODEL))
            def _():
                w_fwd_z(s, to, n).start()
        each_share(j, step)

    def yfwd(q):
        j, n = q // NSUB + 1, q % NSUB
        each_share(j, lambda s, sign: w_fwd_y(s, n).start())

    @scoped
    def hop(q, zf=True, yf=True):
        j, n = q // NSUB + 1, q % NSUB

        def step(s, sign):
            wait_wz(s, n)
            to = z - sign
            if zf:
                @pl.when((to >= 0) & (to < MODEL))
                def _():
                    w_fwd_z(s, to, n).start()
            if yf:
                w_fwd_y(s, n).start()
            w_fwd_d(s, 0, n).start()
        each_share(j, step)

    @scoped
    def across(q):
        j, n = q // NSUB + 1, q % NSUB

        def step(s, sign):
            wait_wy(s, n)
            w_fwd_d(s, 1, n).start()
        each_share(j, step)

    lane = lax.broadcasted_iota(jnp.int32, (1, 128), 1)
    with jax.named_scope('small'):
        for c in small:
            c.wait()

    def tables():
        for g in range(ROWS // 128):
            row = pos_r[:, pl.ds(128 * g, 128)].astype(F32)
            col = jnp.transpose(jnp.broadcast_to(row, (128, 128)), (1, 0))
            ang = col * freq_r[...]
            cos_v[pl.ds(128 * g, 128), :] = jnp.cos(ang)
            sin_v[pl.ds(128 * g, 128), :] = jnp.sin(ang)
        rr = lax.broadcasted_iota(jnp.int32, (KV_RANK, 1024), 0)
        cc = lax.broadcasted_iota(jnp.int32, (KV_RANK, 1024), 1)
        tile_v[...] = jnp.where((rr // ROPE == cc // 128) & (rr % ROPE == cc % ROPE), 1.0, 0.0).astype(BF16)

    low = (lane % ROPE) < (ROPE // 2)

    def rope(v, r0):
        up = pltpu.roll(v, 128 - ROPE // 2, 1)
        dn = pltpu.roll(v, ROPE // 2, 1)
        rot = jnp.where(low, -up, dn)
        return v * cos_v[pl.ds(r0, SPAN), :] + rot * sin_v[pl.ds(r0, SPAN), :]

    def kv_copy(c, t, idx, to):
        return remote(lat_v.at[c, t], lat_v.at[c, t], kv_ssem.at[idx, t], kv_rsem.at[idx, t], dev(c=to))

    loads[0].wait()
    gkv = gkv_r[...]
    with jax.named_scope('ckv'):
        for t in range(2):
            r0 = t * SPAN
            if t == 0:
                loads[1].wait()
                loads[2].wait()
                tables()
                wkr4 = jnp.concatenate([wkr_v[...]] * 4, axis=0)
            else:
                loads[3].wait()
            xs = x_v[pl.ds(r0, SPAN), :]
            lat_v[ctx, t, pl.ds(0, SPAN), :] = rms(dot(xs, wdkv_v[...]), gkv)
            kr = rope(dot_nt(xs, wkr4), r0)
            for half in range(2):
                packed = kr[128 * half:128 * half + KRP]
                for g in range(1, 4):
                    a = 128 * half + KRP * g
                    packed = jnp.where(lane // ROPE == g, kr[a:a + KRP], packed)
                lat_v[ctx, t, pl.ds(SPAN, KRP), pl.ds(128 * half, 128)] = packed.astype(BF16)
            if t == 0:
                kv_copy(ctx, t, 0, ynbr).start()
            else:
                @pl.when(ctx >= 2)
                def _():
                    kv_copy(ctx, 1, 0, ynbr).start()
            kv_copy(ctx, t, 1, partner).start()

    with jax.named_scope('ld4'):
        loads[4].wait()
    gq = jnp.concatenate([gq_r[g:g + 1, :] for g in range(Q_RANK // 128)], axis=1)
    with jax.named_scope('cq'):
        for t in range(2):
            cq_v[pl.ds(t * SPAN, SPAN), :] = rms(dot(x_v[pl.ds(t * SPAN, SPAN), :], wdq_v[...]), gq)
    hop(0, True, False)
    loads[5].wait()
    loads[6].wait()
    with jax.named_scope('qup'):
        for t in range(2):
            cq = cq_v[pl.ds(t * SPAN, SPAN), :]
            qn = dot(cq, wuq_v[...]).astype(BF16)
            zero = jnp.zeros((SPAN, 128), BF16)
            for p in range(PAIRS):
                blk = qn[:, 128 * p:128 * p + 128]
                qm_v[p, t, pl.ds(0, SPAN), pl.ds(0, 128)] = jnp.where(lane < NOPE, blk, zero)
                qm_v[p, t, pl.ds(SPAN, SPAN), pl.ds(0, 128)] = jnp.where(lane < NOPE, zero, blk)
            for b in range(3):
                w = wqr_v[pl.ds(128 * b, 128), :] if b < 2 else jnp.concatenate([wqr_v[pl.ds(256, 64), :]] * 2, axis=0)
                qr = rope(dot_nt(cq, w), t * SPAN).astype(BF16)
                for h in range(4 * b, min(4 * b + 4, HEADS)):
                    qm_v[h // 2, t, pl.ds(SPAN * (h % 2), SPAN), pl.ds(128, 128)] = jnp.where(lane // ROPE == h % 4, qr, zero)

    hop(1, True, False)

    @scoped
    def up(c, t):
        sp = c if t == 0 else NSPAN - 1 - c
        lat = lat_v[c, t, pl.ds(0, SPAN), :]
        kv = dot(lat, wkv_v[...]).astype(BF16)
        k_v[sp] = kv[:, :HV]
        v_v[sp] = kv[:, HV:]
        big = dot(lat_v[c, t, pl.ds(SPAN, KRP), :], tile_v[...]).astype(BF16)
        for g in range(8):
            kr_v[sp, pl.ds(KRP * g, KRP), :] = big[:, 128 * g:128 * g + 128]

    def up_late(c):
        @pl.when(c >= ctx)
        def _():
            up(c, 1)

    loads[7].wait()
    loads[8].wait()
    up(ctx, 0)
    up(ctx, 1)
    with jax.named_scope('kvw_partner'):
        kv_copy(partner, 0, 1, ctx).wait_recv()
        kv_copy(partner, 1, 1, ctx).wait_recv()
    up(partner, 0)
    up_late(partner)
    hop(2, True, False)
    with jax.named_scope('kvw_ynbr'):
        kv_copy(ynbr, 0, 0, ctx).wait_recv()
    kv_copy(ynbr, 0, 2, partner).start()
    up(ynbr, 0)

    @pl.when(ctx < 2)
    def _():
        kv_copy(ynbr, 1, 0, ctx).wait_recv()
        kv_copy(ynbr, 1, 2, partner).start()
        up(ynbr, 1)
    for q in range(3):
        yfwd(q)
    hop(3)
    with jax.named_scope('kvw_diag'):
        kv_copy(diag, 0, 2, ctx).wait_recv()
    up(diag, 0)

    @pl.when(ctx < 2)
    def _():
        kv_copy(diag, 1, 2, ctx).wait_recv()
        up(diag, 1)
    hop(4)

    def block(b):
        if b < 5:
            return 1, NSPAN - 1 - ctx - b
        if b == 8:
            return 0, ctx
        hi = b < NSPAN - ctx
        return jnp.where(hi, 1, 0), jnp.where(hi, NSPAN - 1 - ctx - b, b - (NSPAN - ctx))

    ORDER = (0, 8, 1, 2, 3, 4, 5, 6, 7)
    q_i = lax.broadcasted_iota(jnp.int32, (SPAN, SPAN), 0)
    k_i = lax.broadcasted_iota(jnp.int32, (SPAN, SPAN), 1)
    causal = k_i <= q_i

    def scores(p, b):
        buf = p % 2
        qs, ks = block(b)
        kc = jnp.concatenate([k_v[ks, :, pl.ds(128 * p, 128)], kr_v[ks]], axis=1)
        for a in range(2):
            rows = pl.ds(SPAN * a, SPAN)
            s = dot_nt(qm_v[p, qs, rows, :], kc)
            if b in (0, 8):
                s = jnp.where(causal, s, NEG)
            s_v[buf, b, rows, :] = s
            m = jnp.maximum(s[:, :128], s[:, 128:])
            if b not in (0, 8):
                m = jnp.maximum(mx_v[buf, qs, rows, :], m)
            mx_v[buf, qs, rows, :] = m

    @scoped
    def maxima(p):
        buf = p % 2
        for qs in range(2):
            for a in range(2):
                rows = pl.ds(SPAN * a, SPAN)
                m = jnp.max(mx_v[buf, qs, rows, :], axis=1, keepdims=True)
                mb_v[qs, rows, :] = jnp.broadcast_to(m * SM_SCALE, (SPAN, 128))

    def values(p, b):
        buf = p % 2
        qs, ks = block(b)
        vb = v_v[ks, :, pl.ds(128 * p, 128)]
        for a in range(2):
            rows = pl.ds(SPAN * a, SPAN)
            m = mb_v[qs, rows, :]
            e0 = jnp.exp2(s_v[buf, b, rows, pl.ds(0, 128)] * SM_SCALE - m)
            e1 = jnp.exp2(s_v[buf, b, rows, pl.ds(128, 128)] * SM_SCALE - m)
            pv = dot(jnp.concatenate([e0.astype(BF16), e1.astype(BF16)], axis=1), vb)
            l = e0 + e1
            if b in (0, 8):
                l_v[qs, rows, :] = l
                acc_v[qs, rows, :] = pv
            else:
                l_v[qs, rows, :] += l
                acc_v[qs, rows, :] += pv

    @scoped
    def finish(p):
        for qs in range(2):
            o = []
            for a in range(2):
                rows = pl.ds(SPAN * a, SPAN)
                l = jnp.sum(l_v[qs, rows, :], axis=1, keepdims=True)
                o.append(acc_v[qs, rows, :] / l)
            both = jnp.where(lane < VDIM, o[0], o[1]).astype(BF16)
            os_v[p, 2 * qs] = both[:128]
            os_v[p, 2 * qs + 1] = both[128:]

    def oblk(blk, p, src):
        return oall_v.at[blk, p, src]

    def o_z(p, d):
        to = lax.rem(z + d, MODEL)
        return remote(os_v.at[p, to], oblk(dp, p, z),
                      oz_ssem.at[p, d - 1], oz_rsem.at[p, d - 1], dev(m=to))

    def o_z_wait(p, d):
        src = lax.rem(z + MODEL - d, MODEL)
        remote(os_v.at[p, z], oblk(dp, p, src),
               oz_ssem.at[p, d - 1], oz_rsem.at[p, d - 1], dev()).wait_recv()

    def o_x(p, src_dp, to):
        part = oall_v.at[src_dp, p]
        return remote(part, part, ox_ssem.at[p], ox_rsem.at[p], dev(d=to))

    @scoped
    def send_o(p):
        oblk(dp, p, z)[...] = os_v[p, z]
        for d in (1, 2, 3):
            o_z(p, d).start()

    @scoped
    def pass_o(p):
        for d in (1, 2, 3):
            o_z_wait(p, d)
        o_x(p, dp, xn).start()

    with jax.named_scope('scores0'):
        for b in ORDER:
            scores(0, b)
    maxima(0)
    hop(5, False)
    relay = {
        0: lambda: (hop(6, False),),
        1: lambda: (hop(7, False),),
        2: lambda: (hop(8, False), zfwd(5), pass_o(0)),
        3: lambda: (hop(9, False), zfwd(6), pass_o(1)),
        4: lambda: (zfwd(7), zfwd(8), zfwd(9), pass_o(2)),
    }
    for p in range(PAIRS):
        with jax.named_scope('attn%d' % p):
            for b in ORDER:
                if p + 1 < PAIRS:
                    scores(p + 1, b)
                values(p, b)
        finish(p)
        if p + 1 < PAIRS:
            maxima(p + 1)
        send_o(p)
        relay[p]()
    for q in range(5):
        across(q)
    pass_o(3)
    hop(10)
    pass_o(4)
    hop(11)
    for q in range(5, 8):
        across(q)
    hop(12)
    across(8)
    hop(13)
    across(9)
    hop(14)
    for n in range(NSUB):
        loads[9 + n].wait()

    with jax.named_scope('drain1'):
        for t in range(2):
            kv_copy(ctx, t, 1, partner).wait_send()
        kv_copy(ctx, 0, 0, ynbr).wait_send()
        kv_copy(ynbr, 0, 2, partner).wait_send()

        @pl.when(ctx >= 2)
        def _():
            kv_copy(ctx, 1, 0, ynbr).wait_send()

        @pl.when(ctx < 2)
        def _():
            kv_copy(ynbr, 1, 2, partner).wait_send()

        @pl.when(z < MODEL - 1)
        def _():
            w_own(1).wait_send()

        @pl.when(z > 0)
        def _():
            w_own(0).wait_send()

        for p in range(PAIRS):
            for d in (1, 2, 3):
                o_z(p, d).wait_send()
    def ycols(half, n):
        return out_h.at[:, pl.ds(pl.multiple_of(half * NHALF + SUBC * n, 128), SUBC)]

    def y_back(n):
        return remote(yst_v.at[xn, n], ycols(dp, n), yb_ssem.at[n], yb_rsem.at[n], dev(d=xn))

    def y_come(n):
        return remote(yst_v.at[xn, n], ycols(xn, n), yb_ssem.at[n], yb_rsem.at[n], dev())

    def y_local(n):
        return pltpu.make_async_copy(yst_v.at[dp, n], ycols(dp, n), yl_sem.at[n])

    def wcols(ps, n):
        return jnp.concatenate([wall_v[s, n, pl.ds(128 * p, 128), :] for p in ps for s in range(MODEL)], axis=0)

    def orows(ps):
        return jnp.concatenate([jnp.concatenate([oall_v[blk, p, s] for p in ps for s in range(MODEL)], axis=1) for blk in range(2)], axis=0)

    def have_w(n):
        with jax.named_scope('wdwait'):
            for j in (1, 2, 3):
                each_share(j, lambda s, sign: (wait_wd(s, 0, n), wait_wd(s, 1, n)))

    def finish_y(n, y):
        yst_v[0, n] = y[:128].astype(BF16)
        yst_v[1, n] = y[128:].astype(BF16)
        y_back(n).start()
        y_local(n).start()

    early, last = range(PAIRS - 1), (PAIRS - 1,)

    def final_a(n):
        have_w(n)
        with jax.named_scope('finala%d' % n):
            yacc_v[n] = dot(orows(early), wcols(early, n))

    def final_b(n):
        with jax.named_scope('finalb%d' % n):
            finish_y(n, yacc_v[n] + dot(orows(last), wcols(last, n)))

    def final(n):
        have_w(n)
        with jax.named_scope('final%d' % n):
            finish_y(n, dot(orows(range(PAIRS)), wcols(range(PAIRS), n)))

    across(10)
    across(11)
    with jax.named_scope('oxwait'):
        for p in early:
            o_x(p, xn, dp).wait_recv()
    final_a(0)
    across(12)
    final_a(1)
    with jax.named_scope('oxwait4'):
        o_x(PAIRS - 1, xn, dp).wait_recv()
    final_b(0)
    across(13)
    final_b(1)
    across(14)
    final(2)
    final(3)
    final(4)

    def sent(s, sign):
        to = z - sign

        @pl.when((to >= 0) & (to < MODEL))
        def _():
            w_fwd_z(s, to).wait_send()
        w_fwd_y(s).wait_send()
        w_fwd_d(s, 0).wait_send()
        w_fwd_d(s, 1).wait_send()

    with jax.named_scope('drain2'):
        for j in (1, 2, 3):
            each_share(j, sent)
        for p in range(PAIRS):
            o_x(p, dp, xn).wait_send()
        for n in range(NSUB):
            y_back(n).wait_send()
            y_local(n).wait()
            y_come(n).wait_recv()


def layer(x, pos, freq, wdq, gq, wuq, wqr, wdkv, gkv, wkr, wuk, wuv, wout):
    hb = pl.BlockSpec(memory_space=pl.ANY)
    dma = pltpu.SemaphoreType.DMA
    return pl.pallas_call(
        kernel,
        out_shape=jax.ShapeDtypeStruct((ROWS // MODEL, HIDDEN), BF16),
        in_specs=[hb] * 13,
        out_specs=hb,
        scratch_shapes=[
            pltpu.VMEM((1, ROWS), jnp.int32),
            pltpu.VMEM((1, 128), F32),
            pltpu.VMEM((Q_RANK // 128, 128), F32),
            pltpu.VMEM((1, KV_RANK), F32),
            pltpu.VMEM((ROWS, HIDDEN), BF16),
            pltpu.VMEM((HIDDEN, Q_RANK), BF16),
            pltpu.VMEM((Q_RANK, HEADS * NOPE), BF16),
            pltpu.VMEM((HEADS * ROPE, Q_RANK), BF16),
            pltpu.VMEM((HIDDEN, KV_RANK), BF16),
            pltpu.VMEM((ROPE, HIDDEN), BF16),
            pltpu.VMEM((KV_RANK, 2 * HV), BF16),
            pltpu.VMEM((ROWS, 128), F32),
            pltpu.VMEM((ROWS, 128), F32),
            pltpu.VMEM((KV_RANK, 1024), BF16),
            pltpu.VMEM((CTX, 2, SPAN + KRP, KV_RANK), BF16),
            pltpu.VMEM((ROWS, Q_RANK), BF16),
            pltpu.VMEM((PAIRS, 2, 2 * SPAN, 256), BF16),
            pltpu.VMEM((NSPAN, SPAN, HEADS * NOPE), BF16),
            pltpu.VMEM((NSPAN, SPAN, HEADS * VDIM), BF16),
            pltpu.VMEM((NSPAN, SPAN, 128), BF16),
            pltpu.VMEM((2, 9, 2 * SPAN, SPAN), F32),
            pltpu.VMEM((2, 2, 2 * SPAN, 128), F32),
            pltpu.VMEM((2, 2 * SPAN, 128), F32),
            pltpu.VMEM((2, 2 * SPAN, 128), F32),
            pltpu.VMEM((2, 2 * SPAN, 128), F32),
            pltpu.VMEM((PAIRS, MODEL, 128, 128), BF16),
            pltpu.VMEM((2, PAIRS, MODEL, 128, 128), BF16),
            pltpu.VMEM((MODEL, NSUB, HV, SUBC), BF16),
            pltpu.VMEM((2, NSUB, 128, SUBC), BF16),
            pltpu.VMEM((2, 256, SUBC), F32),
            dma((18,)),
            dma((3, 2)), dma((3, 2)),
            dma((2,)), dma((MODEL,)), dma((MODEL, NSUB)),
            dma((MODEL,)), dma((MODEL, NSUB)),
            dma((MODEL, 2)), dma((MODEL, 2, NSUB)),
            dma((PAIRS, 3)), dma((PAIRS, 3)),
            dma((PAIRS,)), dma((PAIRS,)),
            dma((NSUB,)), dma((NSUB,)), dma((NSUB,)),
        ],
        compiler_params=pltpu.CompilerParams(collective_id=0, has_side_effects=True, vmem_limit_bytes=60 * 1024 * 1024),
        name='mla_layer',
    )(x, pos, freq, gq, gkv, wdq, wuq, wqr, wdkv, wkr, wuk, wuv, wout)


def solution(mesh):
    inv_freq = (ROPE_BASE ** (-(np.arange(ROPE // 2, dtype=np.float64) * 2.0 / ROPE))).astype(np.float32)
    freq = np.tile(inv_freq, 128 // (ROPE // 2))[None, :]

    def local(x_tokens, positions, w_dq, gain_q, w_uq, w_qr, w_dkv, gain_kv, w_kr, w_uk, w_uv, w_out):
        return layer(x_tokens, positions[None, :], jnp.asarray(freq), w_dq, gain_q.reshape(Q_RANK // 128, 128), w_uq,
                     w_qr.T, w_dkv, gain_kv[None, :], w_kr.T, w_uk, w_uv, w_out)

    in_specs = (P(('dp', 'ctx'), None), P(('dp', 'ctx')), P(), P(), P(None, 'model'), P(None, 'model'), P(), P(), P(), P(None, 'model'), P(None, 'model'), P('model', None))
    out_specs = P(('dp', 'ctx', 'model'), None)
    return jax.shard_map(local, mesh=mesh, in_specs=in_specs, out_specs=out_specs, check_vma=False)
```

```python
import functools

import jax
import jax.numpy as jnp
import numpy as np
from jax import lax
from jax.experimental import pallas as pl
from jax.experimental.pallas import tpu as pltpu
from jax.sharding import PartitionSpec as P

MESH = pl.DeviceIdType.MESH


def scoped(fn):
    @functools.wraps(fn)
    def run(*args):
        tag = "_".join(str(a) for a in args if isinstance(a, int))
        with jax.named_scope(fn.__name__ + tag):
            return fn(*args)
    return run


F32 = jnp.float32
BF16 = jnp.bfloat16

HIDDEN = 2560
Q_RANK = 768
KV_RANK = 256
HEADS = 10
PAIRS = HEADS // 2
NOPE = 64
ROPE = 32
VDIM = 64
ROWS = 512
SPAN = 256
NSPAN = 8
CTX = 4
MODEL = 4
HV = HEADS * VDIM
NHALF = HIDDEN // 2
QROWS = HV // 4
WIDTHS = (256, 256, 256, 256, 128, 128)
OFFSETS = (0, 256, 512, 768, 1024, 1152)
NSUB = len(WIDTHS)
WIDE = 4
KRP = SPAN // 8
EPS = 1e-6
ROPE_BASE = 10000.0
SM_SCALE = float((NOPE + ROPE) ** -0.5 * np.log2(np.e))
NEG = -1e30


def dot(a, b):
    return jnp.dot(a, b, preferred_element_type=F32)


def dot_nt(a, b):
    return lax.dot_general(a, b, (((1,), (1,)), ((), ())), preferred_element_type=F32)


def rms(h, gain):
    ms = jnp.mean(h * h, axis=-1, keepdims=True)
    return (h * lax.rsqrt(ms + EPS) * gain).astype(BF16)


def kernel(x_h, pos_h, freq_h, gq_h, gkv_h, wdq_h, wuq_h, wqr_h, wdkv_h, wkr_h, wuk_h, wuv_h, wout_h, out_h,
           pos_r, freq_r, gq_r, gkv_r, x_v, wdq_v, wuq_v, wqr_v, wdkv_v, wkr_v, wkv_v,
           cos_v, sin_v, tile_v, lat_v, cq_v, qm_v, k_v, v_v, kr_v, s_v, mx_v, mb_v, l_v, acc_v,
           os_v, oall_v, wall_v, wallb_v, yown_v, ysend_v, yrecv_v,
           lsem, kv_ssem, kv_rsem, wz_own, wz_ssem, wz_rsem, wy_ssem, wy_rsem, wd_ssem, wd_rsem,
           oz_ssem, oz_rsem, ox_ssem, ox_rsem, yb_ssem, yb_rsem, yl_sem, yp_sem):
    dp = lax.axis_index('dp')
    z = lax.axis_index('model')
    ctx = lax.axis_index('ctx')
    partner = ctx + 1 - 2 * lax.rem(ctx, 2)
    ynbr = lax.rem(ctx + 2, CTX)
    diag = lax.rem(partner + 2, CTX)
    xn = 1 - dp

    def dev(d=None, m=None, c=None):
        return (dp if d is None else d, z if m is None else m, ctx if c is None else c)

    def remote(src, dst, ss, rs, where):
        return pltpu.make_async_remote_copy(src_ref=src, dst_ref=dst, send_sem=ss, recv_sem=rs,
                                            device_id=where, device_id_type=MESH)

    def local(src, dst, idx):
        return pltpu.make_async_copy(src, dst, lsem.at[idx])

    small = [local(pos_h, pos_r, 15), local(freq_h, freq_r, 16), local(gq_h, gq_r, 17), local(gkv_h, gkv_r, 18)]
    loads = [
        local(wkr_h, wkr_v, 0),
        local(x_h.at[pl.ds(0, SPAN)], x_v.at[pl.ds(0, SPAN)], 1),
        local(wdkv_h, wdkv_v, 2),
        local(x_h.at[pl.ds(SPAN, SPAN)], x_v.at[pl.ds(SPAN, SPAN)], 3),
        local(wdq_h, wdq_v, 4),
        local(wuq_h, wuq_v, 5),
        local(wqr_h, wqr_v, 6),
        local(wuk_h, wkv_v.at[:, pl.ds(0, HV)], 7),
        local(wuv_h, wkv_v.at[:, pl.ds(HV, HV)], 8),
    ]

    def wsub(s, n):
        return wall_v.at[s, n] if n < WIDE else wallb_v.at[s, n - WIDE]

    def whbm(rows, n):
        return wout_h.at[rows, pl.ds(pl.multiple_of(dp * NHALF + OFFSETS[n], 128), WIDTHS[n])]

    loads += [local(whbm(pl.ds(0, HV), n), wsub(z, n), 9 + n) for n in range(NSUB)]
    for c in small + loads:
        c.start()

    barrier = pltpu.get_barrier_semaphore()
    peers = [dev(m=lax.rem(z + d, MODEL)) for d in (1, 2, 3)] + [dev(d=xn), dev(c=partner), dev(c=ynbr)]
    for p in peers:
        pl.semaphore_signal(barrier, inc=1, device_id=p, device_id_type=MESH)
    with jax.named_scope('barrier'):
        pl.semaphore_wait(barrier, len(peers))

    def wrows(c):
        return pl.ds(pl.multiple_of(c * QROWS, 16), QROWS)

    def wpiece(s, c, n):
        return wsub(s, n).at[wrows(c)]

    def wgroup(s, c, g):
        return (wall_v if g == 0 else wallb_v).at[s, :, wrows(c)]

    def grp(n):
        return 0 if n < WIDE else 1

    def w_own(up, n):
        return remote(whbm(wrows(ctx), n), wpiece(z, ctx, n), wz_own.at[up, grp(n)], wz_rsem.at[z, n], dev(m=z + 2 * up - 1))

    def w_fwd_z(s, to, n):
        return remote(wpiece(s, ctx, n), wpiece(s, ctx, n), wz_ssem.at[s, grp(n)], wz_rsem.at[s, n], dev(m=to))

    def w_fwd_y(s, n):
        return remote(wpiece(s, ctx, n), wpiece(s, ctx, n), wy_ssem.at[s, grp(n)], wy_rsem.at[s, n], dev(c=ynbr))

    def w_fwd_d(s, which, n):
        c = ctx if which == 0 else ynbr
        return remote(wpiece(s, c, n), wpiece(s, c, n), wd_ssem.at[s, which, grp(n)], wd_rsem.at[s, which, n], dev(c=partner))

    def w_sent(sem, s, c):
        for g in range(2):
            remote(wgroup(s, c, g), wgroup(s, c, g), sem.at[g], wz_rsem.at[s, 0], dev()).wait_send()

    def wait_wz(s, n):
        remote(wpiece(s, ctx, n), wpiece(s, ctx, n), wz_ssem.at[s, 0], wz_rsem.at[s, n], dev()).wait_recv()

    def wait_wy(s, n):
        remote(wpiece(s, ynbr, n), wpiece(s, ynbr, n), wy_ssem.at[s, 0], wy_rsem.at[s, n], dev()).wait_recv()

    def wait_wd(s, which, n):
        c = partner if which == 0 else diag
        remote(wpiece(s, c, n), wpiece(s, c, n), wd_ssem.at[s, which, 0], wd_rsem.at[s, which, n], dev()).wait_recv()

    @pl.when(z < MODEL - 1)
    def _():
        for n in range(NSUB):
            w_own(1, n).start()

    @pl.when(z > 0)
    def _():
        for n in range(NSUB):
            w_own(0, n).start()

    def each_share(j, fn):
        for sign in (-1, 1):
            s = z + sign * j

            @pl.when((s >= 0) & (s < MODEL))
            def _(s=s, sign=sign):
                fn(s, sign)

    @scoped
    def zfwd(q):
        j, n = q // NSUB + 1, q % NSUB

        def step(s, sign):
            to = z - sign

            @pl.when((to >= 0) & (to < MODEL))
            def _():
                w_fwd_z(s, to, n).start()
        each_share(j, step)

    def yfwd(q):
        j, n = q // NSUB + 1, q % NSUB
        each_share(j, lambda s, sign: w_fwd_y(s, n).start())

    @scoped
    def hop(q, zf=True, yf=True):
        j, n = q // NSUB + 1, q % NSUB

        def step(s, sign):
            wait_wz(s, n)
            to = z - sign
            if zf:
                @pl.when((to >= 0) & (to < MODEL))
                def _():
                    w_fwd_z(s, to, n).start()
            if yf:
                w_fwd_y(s, n).start()
            w_fwd_d(s, 0, n).start()
        each_share(j, step)

    @scoped
    def across(q):
        j, n = q // NSUB + 1, q % NSUB

        def step(s, sign):
            wait_wy(s, n)
            w_fwd_d(s, 1, n).start()
        each_share(j, step)

    lane = lax.broadcasted_iota(jnp.int32, (1, 128), 1)
    with jax.named_scope('small'):
        for c in small:
            c.wait()

    def tables():
        for g in range(ROWS // 128):
            row = pos_r[:, pl.ds(128 * g, 128)].astype(F32)
            col = jnp.transpose(jnp.broadcast_to(row, (128, 128)), (1, 0))
            ang = col * freq_r[...]
            cos_v[pl.ds(128 * g, 128), :] = jnp.cos(ang)
            sin_v[pl.ds(128 * g, 128), :] = jnp.sin(ang)
        rr = lax.broadcasted_iota(jnp.int32, (KV_RANK, 1024), 0)
        cc = lax.broadcasted_iota(jnp.int32, (KV_RANK, 1024), 1)
        tile_v[...] = jnp.where((rr // ROPE == cc // 128) & (rr % ROPE == cc % ROPE), 1.0, 0.0).astype(BF16)

    low = (lane % ROPE) < (ROPE // 2)

    def rope(v, r0):
        up = pltpu.roll(v, 128 - ROPE // 2, 1)
        dn = pltpu.roll(v, ROPE // 2, 1)
        rot = jnp.where(low, -up, dn)
        return v * cos_v[pl.ds(r0, SPAN), :] + rot * sin_v[pl.ds(r0, SPAN), :]

    def kv_copy(c, t, idx, to):
        return remote(lat_v.at[c, t], lat_v.at[c, t], kv_ssem.at[idx, t], kv_rsem.at[idx, t], dev(c=to))

    loads[0].wait()
    gkv = gkv_r[...]
    with jax.named_scope('ckv'):
        for t in range(2):
            r0 = t * SPAN
            if t == 0:
                loads[1].wait()
                loads[2].wait()
                tables()
                wkr4 = jnp.concatenate([wkr_v[...]] * 4, axis=0)
            else:
                loads[3].wait()
            xs = x_v[pl.ds(r0, SPAN), :]
            lat_v[ctx, t, pl.ds(0, SPAN), :] = rms(dot(xs, wdkv_v[...]), gkv)
            kr = rope(dot_nt(xs, wkr4), r0)
            for half in range(2):
                packed = kr[128 * half:128 * half + KRP]
                for g in range(1, 4):
                    a = 128 * half + KRP * g
                    packed = jnp.where(lane // ROPE == g, kr[a:a + KRP], packed)
                lat_v[ctx, t, pl.ds(SPAN, KRP), pl.ds(128 * half, 128)] = packed.astype(BF16)
            if t == 0:
                kv_copy(ctx, t, 0, ynbr).start()
            else:
                @pl.when(ctx >= 2)
                def _():
                    kv_copy(ctx, 1, 0, ynbr).start()
            kv_copy(ctx, t, 1, partner).start()

    with jax.named_scope('ld4'):
        loads[4].wait()
    gq = jnp.concatenate([gq_r[g:g + 1, :] for g in range(Q_RANK // 128)], axis=1)
    with jax.named_scope('cq'):
        for t in range(2):
            cq_v[pl.ds(t * SPAN, SPAN), :] = rms(dot(x_v[pl.ds(t * SPAN, SPAN), :], wdq_v[...]), gq)
    hop(0, True, False)
    loads[5].wait()
    loads[6].wait()
    with jax.named_scope('qup'):
        for t in range(2):
            cq = cq_v[pl.ds(t * SPAN, SPAN), :]
            qn = dot(cq, wuq_v[...]).astype(BF16)
            zero = jnp.zeros((SPAN, 128), BF16)
            for p in range(PAIRS):
                blk = qn[:, 128 * p:128 * p + 128]
                qm_v[p, t, pl.ds(0, SPAN), pl.ds(0, 128)] = jnp.where(lane < NOPE, blk, zero)
                qm_v[p, t, pl.ds(SPAN, SPAN), pl.ds(0, 128)] = jnp.where(lane < NOPE, zero, blk)
            for b in range(3):
                w = wqr_v[pl.ds(128 * b, 128), :] if b < 2 else jnp.concatenate([wqr_v[pl.ds(256, 64), :]] * 2, axis=0)
                qr = rope(dot_nt(cq, w), t * SPAN).astype(BF16)
                for h in range(4 * b, min(4 * b + 4, HEADS)):
                    qm_v[h // 2, t, pl.ds(SPAN * (h % 2), SPAN), pl.ds(128, 128)] = jnp.where(lane // ROPE == h % 4, qr, zero)

    hop(1, True, False)

    @scoped
    def up(c, t):
        sp = c if t == 0 else NSPAN - 1 - c
        lat = lat_v[c, t, pl.ds(0, SPAN), :]
        kv = dot(lat, wkv_v[...]).astype(BF16)
        k_v[sp] = kv[:, :HV]
        v_v[sp] = kv[:, HV:]
        big = dot(lat_v[c, t, pl.ds(SPAN, KRP), :], tile_v[...]).astype(BF16)
        for g in range(8):
            kr_v[sp, pl.ds(KRP * g, KRP), :] = big[:, 128 * g:128 * g + 128]

    def up_late(c):
        @pl.when(c >= ctx)
        def _():
            up(c, 1)

    loads[7].wait()
    loads[8].wait()
    up(ctx, 0)
    up(ctx, 1)
    with jax.named_scope('kvw_partner'):
        kv_copy(partner, 0, 1, ctx).wait_recv()
        kv_copy(partner, 1, 1, ctx).wait_recv()
    up(partner, 0)
    up_late(partner)
    hop(2, True, False)
    with jax.named_scope('kvw_ynbr'):
        kv_copy(ynbr, 0, 0, ctx).wait_recv()
    kv_copy(ynbr, 0, 2, partner).start()
    up(ynbr, 0)

    @pl.when(ctx < 2)
    def _():
        kv_copy(ynbr, 1, 0, ctx).wait_recv()
        kv_copy(ynbr, 1, 2, partner).start()
        up(ynbr, 1)
    for q in range(3):
        yfwd(q)
    hop(3)
    with jax.named_scope('kvw_diag'):
        kv_copy(diag, 0, 2, ctx).wait_recv()
    up(diag, 0)

    @pl.when(ctx < 2)
    def _():
        kv_copy(diag, 1, 2, ctx).wait_recv()
        up(diag, 1)
    hop(4)
    hop(5)

    def block(b):
        if b < 5:
            return 1, NSPAN - 1 - ctx - b
        if b == 8:
            return 0, ctx
        hi = b < NSPAN - ctx
        return jnp.where(hi, 1, 0), jnp.where(hi, NSPAN - 1 - ctx - b, b - (NSPAN - ctx))

    ORDER = (0, 8, 1, 2, 3, 4, 5, 6, 7)
    q_i = lax.broadcasted_iota(jnp.int32, (SPAN, SPAN), 0)
    k_i = lax.broadcasted_iota(jnp.int32, (SPAN, SPAN), 1)
    causal = k_i <= q_i

    def scores(p, b):
        buf = p % 2
        qs, ks = block(b)
        kc = jnp.concatenate([k_v[ks, :, pl.ds(128 * p, 128)], kr_v[ks]], axis=1)
        for a in range(2):
            rows = pl.ds(SPAN * a, SPAN)
            s = dot_nt(qm_v[p, qs, rows, :], kc)
            if b in (0, 8):
                s = jnp.where(causal, s, NEG)
            s_v[buf, b, rows, :] = s
            m = jnp.maximum(s[:, :128], s[:, 128:])
            if b not in (0, 8):
                m = jnp.maximum(mx_v[buf, qs, rows, :], m)
            mx_v[buf, qs, rows, :] = m

    @scoped
    def maxima(p):
        buf = p % 2
        for qs in range(2):
            for a in range(2):
                rows = pl.ds(SPAN * a, SPAN)
                m = jnp.max(mx_v[buf, qs, rows, :], axis=1, keepdims=True)
                mb_v[qs, rows, :] = jnp.broadcast_to(m * SM_SCALE, (SPAN, 128))

    def values(p, b):
        buf = p % 2
        qs, ks = block(b)
        vb = v_v[ks, :, pl.ds(128 * p, 128)]
        for a in range(2):
            rows = pl.ds(SPAN * a, SPAN)
            m = mb_v[qs, rows, :]
            e0 = jnp.exp2(s_v[buf, b, rows, pl.ds(0, 128)] * SM_SCALE - m)
            e1 = jnp.exp2(s_v[buf, b, rows, pl.ds(128, 128)] * SM_SCALE - m)
            pv = dot(jnp.concatenate([e0.astype(BF16), e1.astype(BF16)], axis=1), vb)
            l = e0 + e1
            if b in (0, 8):
                l_v[qs, rows, :] = l
                acc_v[qs, rows, :] = pv
            else:
                l_v[qs, rows, :] += l
                acc_v[qs, rows, :] += pv

    @scoped
    def finish(p):
        for qs in range(2):
            o = []
            for a in range(2):
                rows = pl.ds(SPAN * a, SPAN)
                l = jnp.sum(l_v[qs, rows, :], axis=1, keepdims=True)
                o.append(acc_v[qs, rows, :] / l)
            both = jnp.where(lane < VDIM, o[0], o[1]).astype(BF16)
            os_v[p, 2 * qs] = both[:128]
            os_v[p, 2 * qs + 1] = both[128:]

    def oblk(blk, p, src):
        return oall_v.at[blk, p, src]

    def o_z(p, d):
        to = lax.rem(z + d, MODEL)
        return remote(os_v.at[p, to], oblk(dp, p, z),
                      oz_ssem.at[p, d - 1], oz_rsem.at[p, d - 1], dev(m=to))

    def o_z_wait(p, d):
        src = lax.rem(z + MODEL - d, MODEL)
        remote(os_v.at[p, z], oblk(dp, p, src),
               oz_ssem.at[p, d - 1], oz_rsem.at[p, d - 1], dev()).wait_recv()

    def o_x(p, src_dp, to):
        part = oall_v.at[src_dp, p]
        return remote(part, part, ox_ssem.at[p], ox_rsem.at[p], dev(d=to))

    @scoped
    def send_o(p):
        oblk(dp, p, z)[...] = os_v[p, z]
        for d in (1, 2, 3):
            o_z(p, d).start()

    @scoped
    def pass_o(p):
        for d in (1, 2, 3):
            o_z_wait(p, d)
        o_x(p, dp, xn).start()

    with jax.named_scope('scores0'):
        for b in ORDER:
            scores(0, b)
    maxima(0)
    hop(6, False)
    relay = {
        0: lambda: (hop(7, False),),
        1: lambda: (hop(8, False),),
        2: lambda: (hop(9, False), zfwd(6), pass_o(0)),
        3: lambda: (hop(10, False), hop(11, False), zfwd(7), pass_o(1)),
        4: lambda: (zfwd(8), zfwd(9), zfwd(10), zfwd(11), pass_o(2)),
    }
    for p in range(PAIRS):
        with jax.named_scope('attn%d' % p):
            for b in ORDER:
                if p + 1 < PAIRS:
                    scores(p + 1, b)
                values(p, b)
        finish(p)
        if p + 1 < PAIRS:
            maxima(p + 1)
        send_o(p)
        relay[p]()
    for q in range(NSUB):
        across(q)
    pass_o(3)
    hop(12)
    pass_o(4)
    hop(13)
    for q in range(6, 10):
        across(q)
    hop(14)
    across(10)
    across(11)
    across(12)
    hop(15)
    across(13)
    hop(16)
    hop(17)
    for n in range(NSUB):
        loads[9 + n].wait()

    with jax.named_scope('drain1'):
        for t in range(2):
            kv_copy(ctx, t, 1, partner).wait_send()
        kv_copy(ctx, 0, 0, ynbr).wait_send()
        kv_copy(ynbr, 0, 2, partner).wait_send()

        @pl.when(ctx >= 2)
        def _():
            kv_copy(ctx, 1, 0, ynbr).wait_send()

        @pl.when(ctx < 2)
        def _():
            kv_copy(ynbr, 1, 2, partner).wait_send()

        @pl.when(z < MODEL - 1)
        def _():
            w_sent(wz_own.at[1], z, ctx)

        @pl.when(z > 0)
        def _():
            w_sent(wz_own.at[0], z, ctx)

        for p in range(PAIRS):
            for d in (1, 2, 3):
                o_z(p, d).wait_send()
    def ycols(half, n):
        return out_h.at[:, pl.ds(pl.multiple_of(half * NHALF + OFFSETS[n], 128), WIDTHS[n])]

    def yblk(ref, n):
        return ref.at[pl.ds(OFFSETS[n] // 128, WIDTHS[n] // 128)]

    def y_back(n):
        return remote(yblk(ysend_v, n), yblk(yrecv_v, n), yb_ssem.at[n], yb_rsem.at[n], dev(d=xn))

    def y_local(n):
        return pltpu.make_async_copy(yown_v.at[dp, :, pl.ds(OFFSETS[n], WIDTHS[n])], ycols(dp, n), yl_sem.at[n])

    def y_place(i):
        cols = pl.ds(pl.multiple_of(xn * NHALF + 128 * i, 128), 128)
        return pltpu.make_async_copy(yrecv_v.at[i], out_h.at[:, cols], yp_sem.at[i])

    def final(n):
        with jax.named_scope('wdwait%d' % n):
            for j in (1, 2, 3):
                each_share(j, lambda s, sign: (wait_wd(s, 0, n), wait_wd(s, 1, n)))
        with jax.named_scope('final%d' % n):
            o = jnp.concatenate([jnp.concatenate([oall_v[blk, p, s] for s in range(MODEL) for p in range(PAIRS)], axis=1)
                                 for blk in range(2)], axis=0)
            w = jnp.concatenate([wsub(s, n)[...] for s in range(MODEL)], axis=0)
            y = dot(o, w).astype(BF16)
            for blk in range(2):
                yown_v[blk, :, pl.ds(OFFSETS[n], WIDTHS[n])] = y[128 * blk:128 * blk + 128]
            for i in range(WIDTHS[n] // 128):
                ysend_v[OFFSETS[n] // 128 + i] = yown_v[xn, :, pl.ds(OFFSETS[n] + 128 * i, 128)]
            y_back(n).start()
            y_local(n).start()

    with jax.named_scope('oxwait'):
        for p in range(PAIRS):
            o_x(p, xn, dp).wait_recv()
    final(0)
    across(14)
    final(1)
    across(15)
    final(2)
    across(16)
    across(17)
    final(3)
    final(4)
    final(5)

    def sent(s, sign):
        to = z - sign

        @pl.when((to >= 0) & (to < MODEL))
        def _():
            w_sent(wz_ssem.at[s], s, ctx)
        w_sent(wy_ssem.at[s], s, ctx)
        w_sent(wd_ssem.at[s, 0], s, ctx)
        w_sent(wd_ssem.at[s, 1], s, ynbr)

    with jax.named_scope('drain2'):
        for j in (1, 2, 3):
            each_share(j, sent)
        for p in range(PAIRS):
            o_x(p, dp, xn).wait_send()
        for n in range(NSUB):
            y_back(n).wait_recv()
            for i in range(WIDTHS[n] // 128):
                y_place(OFFSETS[n] // 128 + i).start()
        for n in range(NSUB):
            y_back(n).wait_send()
            y_local(n).wait()
        for i in range(NHALF // 128):
            y_place(i).wait()


def layer(x, pos, freq, wdq, gq, wuq, wqr, wdkv, gkv, wkr, wuk, wuv, wout):
    hb = pl.BlockSpec(memory_space=pl.ANY)
    dma = pltpu.SemaphoreType.DMA
    return pl.pallas_call(
        kernel,
        out_shape=jax.ShapeDtypeStruct((ROWS // MODEL, HIDDEN), BF16),
        in_specs=[hb] * 13,
        out_specs=hb,
        scratch_shapes=[
            pltpu.VMEM((1, ROWS), jnp.int32),
            pltpu.VMEM((1, 128), F32),
            pltpu.VMEM((Q_RANK // 128, 128), F32),
            pltpu.VMEM((1, KV_RANK), F32),
            pltpu.VMEM((ROWS, HIDDEN), BF16),
            pltpu.VMEM((HIDDEN, Q_RANK), BF16),
            pltpu.VMEM((Q_RANK, HEADS * NOPE), BF16),
            pltpu.VMEM((HEADS * ROPE, Q_RANK), BF16),
            pltpu.VMEM((HIDDEN, KV_RANK), BF16),
            pltpu.VMEM((ROPE, HIDDEN), BF16),
            pltpu.VMEM((KV_RANK, 2 * HV), BF16),
            pltpu.VMEM((ROWS, 128), F32),
            pltpu.VMEM((ROWS, 128), F32),
            pltpu.VMEM((KV_RANK, 1024), BF16),
            pltpu.VMEM((CTX, 2, SPAN + KRP, KV_RANK), BF16),
            pltpu.VMEM((ROWS, Q_RANK), BF16),
            pltpu.VMEM((PAIRS, 2, 2 * SPAN, 256), BF16),
            pltpu.VMEM((NSPAN, SPAN, HEADS * NOPE), BF16),
            pltpu.VMEM((NSPAN, SPAN, HEADS * VDIM), BF16),
            pltpu.VMEM((NSPAN, SPAN, 128), BF16),
            pltpu.VMEM((2, 9, 2 * SPAN, SPAN), F32),
            pltpu.VMEM((2, 2, 2 * SPAN, 128), F32),
            pltpu.VMEM((2, 2 * SPAN, 128), F32),
            pltpu.VMEM((2, 2 * SPAN, 128), F32),
            pltpu.VMEM((2, 2 * SPAN, 128), F32),
            pltpu.VMEM((PAIRS, MODEL, 128, 128), BF16),
            pltpu.VMEM((2, PAIRS, MODEL, 128, 128), BF16),
            pltpu.VMEM((MODEL, WIDE, HV, 256), BF16),
            pltpu.VMEM((MODEL, NSUB - WIDE, HV, 128), BF16),
            pltpu.VMEM((2, 128, NHALF), BF16),
            pltpu.VMEM((NHALF // 128, 128, 128), BF16),
            pltpu.VMEM((NHALF // 128, 128, 128), BF16),
            dma((19,)),
            dma((3, 2)), dma((3, 2)),
            dma((2, 2)), dma((MODEL, 2)), dma((MODEL, NSUB)),
            dma((MODEL, 2)), dma((MODEL, NSUB)),
            dma((MODEL, 2, 2)), dma((MODEL, 2, NSUB)),
            dma((PAIRS, 3)), dma((PAIRS, 3)),
            dma((PAIRS,)), dma((PAIRS,)),
            dma((NSUB,)), dma((NSUB,)), dma((NSUB,)), dma((NHALF // 128,)),
        ],
        compiler_params=pltpu.CompilerParams(collective_id=0, has_side_effects=True, vmem_limit_bytes=60 * 1024 * 1024),
        name='mla_layer',
    )(x, pos, freq, gq, gkv, wdq, wuq, wqr, wdkv, wkr, wuk, wuv, wout)


def solution(mesh):
    inv_freq = (ROPE_BASE ** (-(np.arange(ROPE // 2, dtype=np.float64) * 2.0 / ROPE))).astype(np.float32)
    freq = np.tile(inv_freq, 128 // (ROPE // 2))[None, :]

    def local(x_tokens, positions, w_dq, gain_q, w_uq, w_qr, w_dkv, gain_kv, w_kr, w_uk, w_uv, w_out):
        return layer(x_tokens, positions[None, :], jnp.asarray(freq), w_dq, gain_q.reshape(Q_RANK // 128, 128), w_uq,
                     w_qr.T, w_dkv, gain_kv[None, :], w_kr.T, w_uk, w_uv, w_out)

    in_specs = (P(('dp', 'ctx'), None), P(('dp', 'ctx')), P(), P(), P(None, 'model'), P(None, 'model'), P(), P(), P(), P(None, 'model'), P(None, 'model'), P('model', None))
    out_specs = P(('dp', 'ctx', 'model'), None)
    return jax.shard_map(local, mesh=mesh, in_specs=in_specs, out_specs=out_specs, check_vma=False)
```

```python
import functools

import jax
import jax.numpy as jnp
import numpy as np
from jax import lax
from jax.experimental import pallas as pl
from jax.experimental.pallas import tpu as pltpu
from jax.sharding import PartitionSpec as P

MESH = pl.DeviceIdType.MESH


def scoped(fn):
    @functools.wraps(fn)
    def run(*args):
        tag = "_".join(str(a) for a in args if isinstance(a, int))
        with jax.named_scope(fn.__name__ + tag):
            return fn(*args)
    return run


F32 = jnp.float32
BF16 = jnp.bfloat16

HIDDEN = 2560
Q_RANK = 768
KV_RANK = 256
HEADS = 10
PAIRS = HEADS // 2
NOPE = 64
ROPE = 32
VDIM = 64
ROWS = 512
SPAN = 256
NSPAN = 8
CTX = 4
MODEL = 4
HV = HEADS * VDIM
NHALF = HIDDEN // 2
QROWS = HV // 4
WIDTHS = (256, 256, 256, 256, 128, 128)
OFFSETS = (0, 256, 512, 768, 1024, 1152)
NSUB = len(WIDTHS)
WIDE = 4
KRP = SPAN // 8
EPS = 1e-6
ROPE_BASE = 10000.0
SM_SCALE = float((NOPE + ROPE) ** -0.5 * np.log2(np.e))
NEG = -1e30


def dot(a, b):
    return jnp.dot(a, b, preferred_element_type=F32)


def dot_nt(a, b):
    return lax.dot_general(a, b, (((1,), (1,)), ((), ())), preferred_element_type=F32)


def rms(h, gain):
    ms = jnp.mean(h * h, axis=-1, keepdims=True)
    return (h * lax.rsqrt(ms + EPS) * gain).astype(BF16)


def kernel(x_h, pos_h, freq_h, gq_h, gkv_h, wdq_h, wuq_h, wqr_h, wdkv_h, wkr_h, wuk_h, wuv_h, wout_h, out_h,
           pos_r, freq_r, gq_r, gkv_r, x_v, wdq_v, wuq_v, wqr_v, wdkv_v, wkr_v, wkv_v,
           cos_v, sin_v, tile_v, lat_v, cq_v, qm_v, k_v, v_v, kr_v, s_v, mx_v, mb_v, l_v, acc_v,
           os_v, oall_v, wall_v, wallb_v, yown_v, ysend_v, yrecv_v,
           lsem, kv_ssem, kv_rsem, wz_own, wz_ssem, wz_rsem, wy_ssem, wy_rsem, wd_ssem, wd_rsem,
           oz_ssem, oz_rsem, ox_ssem, ox_rsem, yb_ssem, yb_rsem, yl_sem, yp_sem):
    dp = lax.axis_index('dp')
    z = lax.axis_index('model')
    ctx = lax.axis_index('ctx')
    partner = ctx + 1 - 2 * lax.rem(ctx, 2)
    ynbr = lax.rem(ctx + 2, CTX)
    diag = lax.rem(partner + 2, CTX)
    xn = 1 - dp

    def dev(d=None, m=None, c=None):
        return (dp if d is None else d, z if m is None else m, ctx if c is None else c)

    def remote(src, dst, ss, rs, where):
        return pltpu.make_async_remote_copy(src_ref=src, dst_ref=dst, send_sem=ss, recv_sem=rs,
                                            device_id=where, device_id_type=MESH)

    def local(src, dst, idx):
        return pltpu.make_async_copy(src, dst, lsem.at[idx])

    small = [local(pos_h, pos_r, 15), local(freq_h, freq_r, 16), local(gq_h, gq_r, 17), local(gkv_h, gkv_r, 18)]
    loads = [
        local(wkr_h, wkr_v, 0),
        local(x_h.at[pl.ds(0, SPAN)], x_v.at[pl.ds(0, SPAN)], 1),
        local(wdkv_h, wdkv_v, 2),
        local(x_h.at[pl.ds(SPAN, SPAN)], x_v.at[pl.ds(SPAN, SPAN)], 3),
        local(wdq_h, wdq_v, 4),
        local(wuq_h, wuq_v, 5),
        local(wqr_h, wqr_v, 6),
        local(wuk_h, wkv_v.at[:, pl.ds(0, HV)], 7),
        local(wuv_h, wkv_v.at[:, pl.ds(HV, HV)], 8),
    ]

    def wsub(s, n):
        return wall_v.at[s, n] if n < WIDE else wallb_v.at[s, n - WIDE]

    def whbm(rows, n):
        return wout_h.at[rows, pl.ds(pl.multiple_of(dp * NHALF + OFFSETS[n], 128), WIDTHS[n])]

    loads += [local(whbm(pl.ds(0, HV), n), wsub(z, n), 9 + n) for n in range(NSUB)]
    for c in small + loads:
        c.start()

    barrier = pltpu.get_barrier_semaphore()
    peers = [dev(m=lax.rem(z + d, MODEL)) for d in (1, 2, 3)] + [dev(d=xn), dev(c=partner), dev(c=ynbr)]
    for p in peers:
        pl.semaphore_signal(barrier, inc=1, device_id=p, device_id_type=MESH)
    with jax.named_scope('barrier'):
        pl.semaphore_wait(barrier, len(peers))

    def wrows(c):
        return pl.ds(pl.multiple_of(c * QROWS, 16), QROWS)

    def wpiece(s, c, n):
        return wsub(s, n).at[wrows(c)]

    def wgroup(s, c, g):
        return (wall_v if g == 0 else wallb_v).at[s, :, wrows(c)]

    def grp(n):
        return 0 if n < WIDE else 1

    def w_own(up, n):
        return remote(whbm(wrows(ctx), n), wpiece(z, ctx, n), wz_own.at[up, grp(n)], wz_rsem.at[z, n], dev(m=z + 2 * up - 1))

    def w_fwd_z(s, to, n):
        return remote(wpiece(s, ctx, n), wpiece(s, ctx, n), wz_ssem.at[s, grp(n)], wz_rsem.at[s, n], dev(m=to))

    def w_fwd_y(s, n):
        return remote(wpiece(s, ctx, n), wpiece(s, ctx, n), wy_ssem.at[s, grp(n)], wy_rsem.at[s, n], dev(c=ynbr))

    def w_fwd_d(s, which, n):
        c = ctx if which == 0 else ynbr
        return remote(wpiece(s, c, n), wpiece(s, c, n), wd_ssem.at[s, which, grp(n)], wd_rsem.at[s, which, n], dev(c=partner))

    def w_sent(sem, s, c):
        for g in range(2):
            remote(wgroup(s, c, g), wgroup(s, c, g), sem.at[g], wz_rsem.at[s, 0], dev()).wait_send()

    def wait_wz(s, n):
        remote(wpiece(s, ctx, n), wpiece(s, ctx, n), wz_ssem.at[s, 0], wz_rsem.at[s, n], dev()).wait_recv()

    def wait_wy(s, n):
        remote(wpiece(s, ynbr, n), wpiece(s, ynbr, n), wy_ssem.at[s, 0], wy_rsem.at[s, n], dev()).wait_recv()

    def wait_wd(s, which, n):
        c = partner if which == 0 else diag
        remote(wpiece(s, c, n), wpiece(s, c, n), wd_ssem.at[s, which, 0], wd_rsem.at[s, which, n], dev()).wait_recv()

    @pl.when(z < MODEL - 1)
    def _():
        for n in range(NSUB):
            w_own(1, n).start()

    @pl.when(z > 0)
    def _():
        for n in range(NSUB):
            w_own(0, n).start()

    def each_share(j, fn):
        for sign in (-1, 1):
            s = z + sign * j

            @pl.when((s >= 0) & (s < MODEL))
            def _(s=s, sign=sign):
                fn(s, sign)

    @scoped
    def zfwd(q):
        j, n = q // NSUB + 1, q % NSUB

        def step(s, sign):
            to = z - sign

            @pl.when((to >= 0) & (to < MODEL))
            def _():
                w_fwd_z(s, to, n).start()
        each_share(j, step)

    def yfwd(q):
        j, n = q // NSUB + 1, q % NSUB
        each_share(j, lambda s, sign: w_fwd_y(s, n).start())

    @scoped
    def hop(q, zf=True, yf=True):
        j, n = q // NSUB + 1, q % NSUB

        def step(s, sign):
            wait_wz(s, n)
            to = z - sign
            if zf:
                @pl.when((to >= 0) & (to < MODEL))
                def _():
                    w_fwd_z(s, to, n).start()
            if yf:
                w_fwd_y(s, n).start()
            w_fwd_d(s, 0, n).start()
        each_share(j, step)

    @scoped
    def across(q):
        j, n = q // NSUB + 1, q % NSUB

        def step(s, sign):
            wait_wy(s, n)
            w_fwd_d(s, 1, n).start()
        each_share(j, step)

    lane = lax.broadcasted_iota(jnp.int32, (1, 128), 1)
    with jax.named_scope('small'):
        for c in small:
            c.wait()

    def tables():
        for g in range(ROWS // 128):
            row = pos_r[:, pl.ds(128 * g, 128)].astype(F32)
            col = jnp.transpose(jnp.broadcast_to(row, (128, 128)), (1, 0))
            ang = col * freq_r[...]
            cos_v[pl.ds(128 * g, 128), :] = jnp.cos(ang)
            sin_v[pl.ds(128 * g, 128), :] = jnp.sin(ang)
        rr = lax.broadcasted_iota(jnp.int32, (KV_RANK, 1024), 0)
        cc = lax.broadcasted_iota(jnp.int32, (KV_RANK, 1024), 1)
        tile_v[...] = jnp.where((rr // ROPE == cc // 128) & (rr % ROPE == cc % ROPE), 1.0, 0.0).astype(BF16)

    low = (lane % ROPE) < (ROPE // 2)

    def rope(v, r0):
        up = pltpu.roll(v, 128 - ROPE // 2, 1)
        dn = pltpu.roll(v, ROPE // 2, 1)
        rot = jnp.where(low, -up, dn)
        return v * cos_v[pl.ds(r0, SPAN), :] + rot * sin_v[pl.ds(r0, SPAN), :]

    def kv_copy(c, t, idx, to):
        return remote(lat_v.at[c, t], lat_v.at[c, t], kv_ssem.at[idx, t], kv_rsem.at[idx, t], dev(c=to))

    loads[0].wait()
    gkv = gkv_r[...]
    with jax.named_scope('ckv'):
        for t in range(2):
            r0 = t * SPAN
            if t == 0:
                loads[1].wait()
                loads[2].wait()
                tables()
                wkr4 = jnp.concatenate([wkr_v[...]] * 4, axis=0)
            else:
                loads[3].wait()
            xs = x_v[pl.ds(r0, SPAN), :]
            lat_v[ctx, t, pl.ds(0, SPAN), :] = rms(dot(xs, wdkv_v[...]), gkv)
            kr = rope(dot_nt(xs, wkr4), r0)
            for half in range(2):
                packed = kr[128 * half:128 * half + KRP]
                for g in range(1, 4):
                    a = 128 * half + KRP * g
                    packed = jnp.where(lane // ROPE == g, kr[a:a + KRP], packed)
                lat_v[ctx, t, pl.ds(SPAN, KRP), pl.ds(128 * half, 128)] = packed.astype(BF16)
            if t == 0:
                kv_copy(ctx, t, 0, ynbr).start()
            else:
                @pl.when(ctx >= 2)
                def _():
                    kv_copy(ctx, 1, 0, ynbr).start()
            kv_copy(ctx, t, 1, partner).start()

    with jax.named_scope('ld4'):
        loads[4].wait()
    gq = jnp.concatenate([gq_r[g:g + 1, :] for g in range(Q_RANK // 128)], axis=1)
    with jax.named_scope('cq'):
        for t in range(2):
            cq_v[pl.ds(t * SPAN, SPAN), :] = rms(dot(x_v[pl.ds(t * SPAN, SPAN), :], wdq_v[...]), gq)
    hop(0, True, False)
    loads[5].wait()
    loads[6].wait()
    with jax.named_scope('qup'):
        for t in range(2):
            cq = cq_v[pl.ds(t * SPAN, SPAN), :]
            qn = dot(cq, wuq_v[...]).astype(BF16)
            zero = jnp.zeros((SPAN, 128), BF16)
            for p in range(PAIRS):
                blk = qn[:, 128 * p:128 * p + 128]
                qm_v[p, t, pl.ds(0, SPAN), pl.ds(0, 128)] = jnp.where(lane < NOPE, blk, zero)
                qm_v[p, t, pl.ds(SPAN, SPAN), pl.ds(0, 128)] = jnp.where(lane < NOPE, zero, blk)
            for b in range(3):
                w = wqr_v[pl.ds(128 * b, 128), :] if b < 2 else jnp.concatenate([wqr_v[pl.ds(256, 64), :]] * 2, axis=0)
                qr = rope(dot_nt(cq, w), t * SPAN).astype(BF16)
                for h in range(4 * b, min(4 * b + 4, HEADS)):
                    qm_v[h // 2, t, pl.ds(SPAN * (h % 2), SPAN), pl.ds(128, 128)] = jnp.where(lane // ROPE == h % 4, qr, zero)

    hop(1, True, False)

    @scoped
    def up(c, t):
        sp = c if t == 0 else NSPAN - 1 - c
        lat = lat_v[c, t, pl.ds(0, SPAN), :]
        kv = dot(lat, wkv_v[...]).astype(BF16)
        k_v[sp] = kv[:, :HV]
        v_v[sp] = kv[:, HV:]
        big = dot(lat_v[c, t, pl.ds(SPAN, KRP), :], tile_v[...]).astype(BF16)
        for g in range(8):
            kr_v[sp, pl.ds(KRP * g, KRP), :] = big[:, 128 * g:128 * g + 128]

    def up_late(c):
        @pl.when(c >= ctx)
        def _():
            up(c, 1)

    loads[7].wait()
    loads[8].wait()
    up(ctx, 0)
    up(ctx, 1)
    with jax.named_scope('kvw_partner'):
        kv_copy(partner, 0, 1, ctx).wait_recv()
        kv_copy(partner, 1, 1, ctx).wait_recv()
    up(partner, 0)
    up_late(partner)
    hop(2, True, False)
    with jax.named_scope('kvw_ynbr'):
        kv_copy(ynbr, 0, 0, ctx).wait_recv()
    kv_copy(ynbr, 0, 2, partner).start()
    up(ynbr, 0)

    @pl.when(ctx < 2)
    def _():
        kv_copy(ynbr, 1, 0, ctx).wait_recv()
        kv_copy(ynbr, 1, 2, partner).start()
        up(ynbr, 1)
    for q in range(3):
        yfwd(q)
    hop(3)
    with jax.named_scope('kvw_diag'):
        kv_copy(diag, 0, 2, ctx).wait_recv()
    up(diag, 0)

    @pl.when(ctx < 2)
    def _():
        kv_copy(diag, 1, 2, ctx).wait_recv()
        up(diag, 1)
    hop(4, False)
    hop(5, False)

    def block(b):
        if b < 5:
            return 1, NSPAN - 1 - ctx - b
        if b == 8:
            return 0, ctx
        hi = b < NSPAN - ctx
        return jnp.where(hi, 1, 0), jnp.where(hi, NSPAN - 1 - ctx - b, b - (NSPAN - ctx))

    ORDER = (0, 8, 1, 2, 3, 4, 5, 6, 7)
    q_i = lax.broadcasted_iota(jnp.int32, (SPAN, SPAN), 0)
    k_i = lax.broadcasted_iota(jnp.int32, (SPAN, SPAN), 1)
    causal = k_i <= q_i

    def scores(p, b):
        buf = p % 2
        qs, ks = block(b)
        kc = jnp.concatenate([k_v[ks, :, pl.ds(128 * p, 128)], kr_v[ks]], axis=1)
        for a in range(2):
            rows = pl.ds(SPAN * a, SPAN)
            s = dot_nt(qm_v[p, qs, rows, :], kc)
            if b in (0, 8):
                s = jnp.where(causal, s, NEG)
            s_v[buf, b, rows, :] = s
            m = jnp.maximum(s[:, :128], s[:, 128:])
            if b not in (0, 8):
                m = jnp.maximum(mx_v[buf, qs, rows, :], m)
            mx_v[buf, qs, rows, :] = m

    @scoped
    def maxima(p):
        buf = p % 2
        for qs in range(2):
            for a in range(2):
                rows = pl.ds(SPAN * a, SPAN)
                m = jnp.max(mx_v[buf, qs, rows, :], axis=1, keepdims=True)
                mb_v[qs, rows, :] = jnp.broadcast_to(m * SM_SCALE, (SPAN, 128))

    def values(p, b):
        buf = p % 2
        qs, ks = block(b)
        vb = v_v[ks, :, pl.ds(128 * p, 128)]
        for a in range(2):
            rows = pl.ds(SPAN * a, SPAN)
            m = mb_v[qs, rows, :]
            e0 = jnp.exp2(s_v[buf, b, rows, pl.ds(0, 128)] * SM_SCALE - m)
            e1 = jnp.exp2(s_v[buf, b, rows, pl.ds(128, 128)] * SM_SCALE - m)
            pv = dot(jnp.concatenate([e0.astype(BF16), e1.astype(BF16)], axis=1), vb)
            l = e0 + e1
            if b in (0, 8):
                l_v[qs, rows, :] = l
                acc_v[qs, rows, :] = pv
            else:
                l_v[qs, rows, :] += l
                acc_v[qs, rows, :] += pv

    @scoped
    def finish(p):
        for qs in range(2):
            o = []
            for a in range(2):
                rows = pl.ds(SPAN * a, SPAN)
                l = jnp.sum(l_v[qs, rows, :], axis=1, keepdims=True)
                o.append(acc_v[qs, rows, :] / l)
            both = jnp.where(lane < VDIM, o[0], o[1]).astype(BF16)
            os_v[p, 2 * qs] = both[:128]
            os_v[p, 2 * qs + 1] = both[128:]

    def oblk(blk, p, src):
        return oall_v.at[blk, p, src]

    def o_z(p, d):
        to = lax.rem(z + d, MODEL)
        return remote(os_v.at[p, to], oblk(dp, p, z),
                      oz_ssem.at[p, d - 1], oz_rsem.at[p, d - 1], dev(m=to))

    def o_z_wait(p, d):
        src = lax.rem(z + MODEL - d, MODEL)
        remote(os_v.at[p, z], oblk(dp, p, src),
               oz_ssem.at[p, d - 1], oz_rsem.at[p, d - 1], dev()).wait_recv()

    def o_x(p, src_dp, to):
        part = oall_v.at[src_dp, p]
        return remote(part, part, ox_ssem.at[p], ox_rsem.at[p], dev(d=to))

    @scoped
    def send_o(p):
        oblk(dp, p, z)[...] = os_v[p, z]
        for d in (1, 2, 3):
            o_z(p, d).start()

    @scoped
    def pass_o(p):
        for d in (1, 2, 3):
            o_z_wait(p, d)
        o_x(p, dp, xn).start()

    with jax.named_scope('scores0'):
        for b in ORDER:
            scores(0, b)
    maxima(0)
    hop(6, False)
    relay = {
        0: lambda: (hop(7, False),),
        1: lambda: (hop(8, False),),
        2: lambda: (hop(9, False), pass_o(0)),
        3: lambda: (pass_o(1),),
        4: lambda: ([zfwd(q) for q in range(4, 10)], pass_o(2)),
    }
    for p in range(PAIRS):
        with jax.named_scope('attn%d' % p):
            for b in ORDER:
                if p + 1 < PAIRS:
                    scores(p + 1, b)
                values(p, b)
        finish(p)
        if p + 1 < PAIRS:
            maxima(p + 1)
        send_o(p)
        relay[p]()
    for q in range(NSUB):
        across(q)
    pass_o(3)
    pass_o(4)
    hop(10)
    hop(11)
    for q in range(6, 10):
        across(q)
    hop(12)
    hop(13)
    across(10)
    across(11)
    hop(14)
    across(12)
    hop(15)
    across(13)
    hop(16)
    hop(17)
    for n in range(NSUB):
        loads[9 + n].wait()

    with jax.named_scope('drain1'):
        for t in range(2):
            kv_copy(ctx, t, 1, partner).wait_send()
        kv_copy(ctx, 0, 0, ynbr).wait_send()
        kv_copy(ynbr, 0, 2, partner).wait_send()

        @pl.when(ctx >= 2)
        def _():
            kv_copy(ctx, 1, 0, ynbr).wait_send()

        @pl.when(ctx < 2)
        def _():
            kv_copy(ynbr, 1, 2, partner).wait_send()

        @pl.when(z < MODEL - 1)
        def _():
            w_sent(wz_own.at[1], z, ctx)

        @pl.when(z > 0)
        def _():
            w_sent(wz_own.at[0], z, ctx)

        for p in range(PAIRS):
            for d in (1, 2, 3):
                o_z(p, d).wait_send()
    def ycols(half, n):
        return out_h.at[:, pl.ds(pl.multiple_of(half * NHALF + OFFSETS[n], 128), WIDTHS[n])]

    def yblk(ref, n):
        return ref.at[pl.ds(OFFSETS[n] // 128, WIDTHS[n] // 128)]

    def y_back(n):
        return remote(yblk(ysend_v, n), yblk(yrecv_v, n), yb_ssem.at[n], yb_rsem.at[n], dev(d=xn))

    def y_local(n):
        return pltpu.make_async_copy(yown_v.at[dp, :, pl.ds(OFFSETS[n], WIDTHS[n])], ycols(dp, n), yl_sem.at[n])

    def y_place(i):
        cols = pl.ds(pl.multiple_of(xn * NHALF + 128 * i, 128), 128)
        return pltpu.make_async_copy(yrecv_v.at[i], out_h.at[:, cols], yp_sem.at[i])

    def final(n):
        with jax.named_scope('wdwait%d' % n):
            for j in (1, 2, 3):
                each_share(j, lambda s, sign: (wait_wd(s, 0, n), wait_wd(s, 1, n)))
        with jax.named_scope('final%d' % n):
            o = jnp.concatenate([jnp.concatenate([oall_v[blk, p, s] for s in range(MODEL) for p in range(PAIRS)], axis=1)
                                 for blk in range(2)], axis=0)
            w = jnp.concatenate([wsub(s, n)[...] for s in range(MODEL)], axis=0)
            y = dot(o, w).astype(BF16)
            for blk in range(2):
                yown_v[blk, :, pl.ds(OFFSETS[n], WIDTHS[n])] = y[128 * blk:128 * blk + 128]
            for i in range(WIDTHS[n] // 128):
                ysend_v[OFFSETS[n] // 128 + i] = yown_v[xn, :, pl.ds(OFFSETS[n] + 128 * i, 128)]
            y_back(n).start()
            y_local(n).start()

    with jax.named_scope('oxwait'):
        for p in range(PAIRS):
            o_x(p, xn, dp).wait_recv()
    final(0)
    across(14)
    final(1)
    across(15)
    final(2)
    across(16)
    across(17)
    final(3)
    final(4)
    final(5)

    def sent(s, sign):
        to = z - sign

        @pl.when((to >= 0) & (to < MODEL))
        def _():
            w_sent(wz_ssem.at[s], s, ctx)
        w_sent(wy_ssem.at[s], s, ctx)
        w_sent(wd_ssem.at[s, 0], s, ctx)
        w_sent(wd_ssem.at[s, 1], s, ynbr)

    with jax.named_scope('drain2'):
        for j in (1, 2, 3):
            each_share(j, sent)
        for p in range(PAIRS):
            o_x(p, dp, xn).wait_send()
        for n in range(NSUB):
            y_back(n).wait_recv()
            for i in range(WIDTHS[n] // 128):
                y_place(OFFSETS[n] // 128 + i).start()
        for n in range(NSUB):
            y_back(n).wait_send()
            y_local(n).wait()
        for i in range(NHALF // 128):
            y_place(i).wait()


def layer(x, pos, freq, wdq, gq, wuq, wqr, wdkv, gkv, wkr, wuk, wuv, wout):
    hb = pl.BlockSpec(memory_space=pl.ANY)
    dma = pltpu.SemaphoreType.DMA
    return pl.pallas_call(
        kernel,
        out_shape=jax.ShapeDtypeStruct((ROWS // MODEL, HIDDEN), BF16),
        in_specs=[hb] * 13,
        out_specs=hb,
        scratch_shapes=[
            pltpu.VMEM((1, ROWS), jnp.int32),
            pltpu.VMEM((1, 128), F32),
            pltpu.VMEM((Q_RANK // 128, 128), F32),
            pltpu.VMEM((1, KV_RANK), F32),
            pltpu.VMEM((ROWS, HIDDEN), BF16),
            pltpu.VMEM((HIDDEN, Q_RANK), BF16),
            pltpu.VMEM((Q_RANK, HEADS * NOPE), BF16),
            pltpu.VMEM((HEADS * ROPE, Q_RANK), BF16),
            pltpu.VMEM((HIDDEN, KV_RANK), BF16),
            pltpu.VMEM((ROPE, HIDDEN), BF16),
            pltpu.VMEM((KV_RANK, 2 * HV), BF16),
            pltpu.VMEM((ROWS, 128), F32),
            pltpu.VMEM((ROWS, 128), F32),
            pltpu.VMEM((KV_RANK, 1024), BF16),
            pltpu.VMEM((CTX, 2, SPAN + KRP, KV_RANK), BF16),
            pltpu.VMEM((ROWS, Q_RANK), BF16),
            pltpu.VMEM((PAIRS, 2, 2 * SPAN, 256), BF16),
            pltpu.VMEM((NSPAN, SPAN, HEADS * NOPE), BF16),
            pltpu.VMEM((NSPAN, SPAN, HEADS * VDIM), BF16),
            pltpu.VMEM((NSPAN, SPAN, 128), BF16),
            pltpu.VMEM((2, 9, 2 * SPAN, SPAN), F32),
            pltpu.VMEM((2, 2, 2 * SPAN, 128), F32),
            pltpu.VMEM((2, 2 * SPAN, 128), F32),
            pltpu.VMEM((2, 2 * SPAN, 128), F32),
            pltpu.VMEM((2, 2 * SPAN, 128), F32),
            pltpu.VMEM((PAIRS, MODEL, 128, 128), BF16),
            pltpu.VMEM((2, PAIRS, MODEL, 128, 128), BF16),
            pltpu.VMEM((MODEL, WIDE, HV, 256), BF16),
            pltpu.VMEM((MODEL, NSUB - WIDE, HV, 128), BF16),
            pltpu.VMEM((2, 128, NHALF), BF16),
            pltpu.VMEM((NHALF // 128, 128, 128), BF16),
            pltpu.VMEM((NHALF // 128, 128, 128), BF16),
            dma((19,)),
            dma((3, 2)), dma((3, 2)),
            dma((2, 2)), dma((MODEL, 2)), dma((MODEL, NSUB)),
            dma((MODEL, 2)), dma((MODEL, NSUB)),
            dma((MODEL, 2, 2)), dma((MODEL, 2, NSUB)),
            dma((PAIRS, 3)), dma((PAIRS, 3)),
            dma((PAIRS,)), dma((PAIRS,)),
            dma((NSUB,)), dma((NSUB,)), dma((NSUB,)), dma((NHALF // 128,)),
        ],
        compiler_params=pltpu.CompilerParams(collective_id=0, has_side_effects=True, vmem_limit_bytes=60 * 1024 * 1024),
        name='mla_layer',
    )(x, pos, freq, gq, gkv, wdq, wuq, wqr, wdkv, wkr, wuk, wuv, wout)


def solution(mesh):
    inv_freq = (ROPE_BASE ** (-(np.arange(ROPE // 2, dtype=np.float64) * 2.0 / ROPE))).astype(np.float32)
    freq = np.tile(inv_freq, 128 // (ROPE // 2))[None, :]

    def local(x_tokens, positions, w_dq, gain_q, w_uq, w_qr, w_dkv, gain_kv, w_kr, w_uk, w_uv, w_out):
        return layer(x_tokens, positions[None, :], jnp.asarray(freq), w_dq, gain_q.reshape(Q_RANK // 128, 128), w_uq,
                     w_qr.T, w_dkv, gain_kv[None, :], w_kr.T, w_uk, w_uv, w_out)

    in_specs = (P(('dp', 'ctx'), None), P(('dp', 'ctx')), P(), P(), P(None, 'model'), P(None, 'model'), P(), P(), P(), P(None, 'model'), P(None, 'model'), P('model', None))
    out_specs = P(('dp', 'ctx', 'model'), None)
    return jax.shard_map(local, mesh=mesh, in_specs=in_specs, out_specs=out_specs, check_vma=False)
```

```python
import functools

import jax
import jax.numpy as jnp
import numpy as np
from jax import lax
from jax.experimental import pallas as pl
from jax.experimental.pallas import tpu as pltpu
from jax.sharding import PartitionSpec as P

MESH = pl.DeviceIdType.MESH


def scoped(fn):
    @functools.wraps(fn)
    def run(*args):
        tag = "_".join(str(a) for a in args if isinstance(a, int))
        with jax.named_scope(fn.__name__ + tag):
            return fn(*args)
    return run


F32 = jnp.float32
BF16 = jnp.bfloat16

HIDDEN = 2560
Q_RANK = 768
KV_RANK = 256
HEADS = 10
PAIRS = HEADS // 2
NOPE = 64
ROPE = 32
VDIM = 64
ROWS = 512
SPAN = 256
NSPAN = 8
CTX = 4
MODEL = 4
HV = HEADS * VDIM
NHALF = HIDDEN // 2
QROWS = HV // 4
WIDTHS = (256, 256, 256, 256, 128, 128)
OFFSETS = (0, 256, 512, 768, 1024, 1152)
NSUB = len(WIDTHS)
WIDE = 4
KRP = SPAN // 8
EPS = 1e-6
ROPE_BASE = 10000.0
SM_SCALE = float((NOPE + ROPE) ** -0.5 * np.log2(np.e))
NEG = -1e30


def dot(a, b):
    return jnp.dot(a, b, preferred_element_type=F32)


def dot_nt(a, b):
    return lax.dot_general(a, b, (((1,), (1,)), ((), ())), preferred_element_type=F32)


def rms(h, gain):
    ms = jnp.mean(h * h, axis=-1, keepdims=True)
    return (h * lax.rsqrt(ms + EPS) * gain).astype(BF16)


def kernel(x_h, pos_h, freq_h, gq_h, gkv_h, wdq_h, wuq_h, wqr_h, wdkv_h, wkr_h, wuk_h, wuv_h, wout_h, out_h,
           pos_r, freq_r, gq_r, gkv_r, x_v, wdq_v, wuq_v, wqr_v, wdkv_v, wkr_v, wkv_v,
           cos_v, sin_v, lat_v, cq_v, qm_v, k_v, v_v, kr_v, s_v, mx_v, mb_v, l_v, acc_v,
           os_v, oall_v, wall_v, wallb_v, yown_v, ysend_v, yrecv_v,
           lsem, kv_ssem, kv_rsem, wz_own, wz_ssem, wz_rsem, wy_ssem, wy_rsem, wd_ssem, wd_rsem,
           oz_ssem, oz_rsem, ox_ssem, ox_rsem, yb_ssem, yb_rsem, yl_sem, yp_sem):
    dp = lax.axis_index('dp')
    z = lax.axis_index('model')
    ctx = lax.axis_index('ctx')
    partner = ctx + 1 - 2 * lax.rem(ctx, 2)
    ynbr = lax.rem(ctx + 2, CTX)
    diag = lax.rem(partner + 2, CTX)
    xn = 1 - dp

    def dev(d=None, m=None, c=None):
        return (dp if d is None else d, z if m is None else m, ctx if c is None else c)

    def remote(src, dst, ss, rs, where):
        return pltpu.make_async_remote_copy(src_ref=src, dst_ref=dst, send_sem=ss, recv_sem=rs,
                                            device_id=where, device_id_type=MESH)

    def local(src, dst, idx):
        return pltpu.make_async_copy(src, dst, lsem.at[idx])

    small = [local(pos_h, pos_r, 15), local(freq_h, freq_r, 16), local(gq_h, gq_r, 17), local(gkv_h, gkv_r, 18)]
    loads = [
        local(wkr_h, wkr_v, 0),
        local(x_h.at[pl.ds(0, SPAN)], x_v.at[pl.ds(0, SPAN)], 1),
        local(wdkv_h, wdkv_v, 2),
        local(x_h.at[pl.ds(SPAN, SPAN)], x_v.at[pl.ds(SPAN, SPAN)], 3),
        local(wdq_h, wdq_v, 4),
        local(wuq_h, wuq_v, 5),
        local(wqr_h, wqr_v, 6),
        local(wuk_h, wkv_v.at[:, pl.ds(0, HV)], 7),
        local(wuv_h, wkv_v.at[:, pl.ds(HV, HV)], 8),
    ]

    def wsub(s, n):
        return wall_v.at[s, n] if n < WIDE else wallb_v.at[s, n - WIDE]

    def whbm(rows, n):
        return wout_h.at[rows, pl.ds(pl.multiple_of(dp * NHALF + OFFSETS[n], 128), WIDTHS[n])]

    loads += [local(whbm(pl.ds(0, HV), n), wsub(z, n), 9 + n) for n in range(NSUB)]
    for c in small + loads:
        c.start()

    barrier = pltpu.get_barrier_semaphore()
    peers = [dev(m=lax.rem(z + d, MODEL)) for d in (1, 2, 3)] + [dev(d=xn), dev(c=partner), dev(c=ynbr)]
    for p in peers:
        pl.semaphore_signal(barrier, inc=1, device_id=p, device_id_type=MESH)
    with jax.named_scope('barrier'):
        pl.semaphore_wait(barrier, len(peers))

    def wrows(c):
        return pl.ds(pl.multiple_of(c * QROWS, 16), QROWS)

    def wpiece(s, c, n):
        return wsub(s, n).at[wrows(c)]

    def wgroup(s, c, g):
        return (wall_v if g == 0 else wallb_v).at[s, :, wrows(c)]

    def grp(n):
        return 0 if n < WIDE else 1

    def w_own(up, n):
        return remote(whbm(wrows(ctx), n), wpiece(z, ctx, n), wz_own.at[up, grp(n)], wz_rsem.at[z, n], dev(m=z + 2 * up - 1))

    def w_fwd_z(s, to, n):
        return remote(wpiece(s, ctx, n), wpiece(s, ctx, n), wz_ssem.at[s, grp(n)], wz_rsem.at[s, n], dev(m=to))

    def w_fwd_y(s, n):
        return remote(wpiece(s, ctx, n), wpiece(s, ctx, n), wy_ssem.at[s, grp(n)], wy_rsem.at[s, n], dev(c=ynbr))

    def w_fwd_d(s, which, n):
        c = ctx if which == 0 else ynbr
        return remote(wpiece(s, c, n), wpiece(s, c, n), wd_ssem.at[s, which, grp(n)], wd_rsem.at[s, which, n], dev(c=partner))

    def w_sent(sem, s, c):
        for g in range(2):
            remote(wgroup(s, c, g), wgroup(s, c, g), sem.at[g], wz_rsem.at[s, 0], dev()).wait_send()

    def wait_wz(s, n):
        remote(wpiece(s, ctx, n), wpiece(s, ctx, n), wz_ssem.at[s, 0], wz_rsem.at[s, n], dev()).wait_recv()

    def wait_wy(s, n):
        remote(wpiece(s, ynbr, n), wpiece(s, ynbr, n), wy_ssem.at[s, 0], wy_rsem.at[s, n], dev()).wait_recv()

    def wait_wd(s, which, n):
        c = partner if which == 0 else diag
        remote(wpiece(s, c, n), wpiece(s, c, n), wd_ssem.at[s, which, 0], wd_rsem.at[s, which, n], dev()).wait_recv()

    @pl.when(z < MODEL - 1)
    def _():
        for n in range(NSUB):
            w_own(1, n).start()

    @pl.when(z > 0)
    def _():
        for n in range(NSUB):
            w_own(0, n).start()

    def each_share(j, fn):
        for sign in (-1, 1):
            s = z + sign * j

            @pl.when((s >= 0) & (s < MODEL))
            def _(s=s, sign=sign):
                fn(s, sign)

    @scoped
    def zfwd(q):
        j, n = q // NSUB + 1, q % NSUB

        def step(s, sign):
            to = z - sign

            @pl.when((to >= 0) & (to < MODEL))
            def _():
                w_fwd_z(s, to, n).start()
        each_share(j, step)

    def yfwd(q):
        j, n = q // NSUB + 1, q % NSUB
        each_share(j, lambda s, sign: w_fwd_y(s, n).start())

    @scoped
    def hop(q, zf=True, yf=True):
        j, n = q // NSUB + 1, q % NSUB

        def step(s, sign):
            wait_wz(s, n)
            to = z - sign
            if zf:
                @pl.when((to >= 0) & (to < MODEL))
                def _():
                    w_fwd_z(s, to, n).start()
            if yf:
                w_fwd_y(s, n).start()
            w_fwd_d(s, 0, n).start()
        each_share(j, step)

    @scoped
    def across(q):
        j, n = q // NSUB + 1, q % NSUB

        def step(s, sign):
            wait_wy(s, n)
            w_fwd_d(s, 1, n).start()
        each_share(j, step)

    lane = lax.broadcasted_iota(jnp.int32, (1, 128), 1)
    with jax.named_scope('small'):
        for c in small:
            c.wait()

    def tables():
        half = ROPE // 2
        pos = jnp.zeros((64, 128), F32)
        for g in range(8):
            if g % 2 == 0:
                row = pos_r[:, pl.ds(64 * g, 128)].astype(F32)
                col = jnp.transpose(jnp.broadcast_to(row, (128, 128)), (1, 0))
            pos = jnp.where(lane // half == g, col[64 * (g % 2):64 * (g % 2) + 64], pos)
        ang = pos * freq_r[...]
        for ref, val in ((cos_v, jnp.cos(ang)), (sin_v, jnp.sin(ang))):
            for g in range(8):
                part = jnp.where(lane // half == g, val, 0.0)
                for shift in (16, 32, 64):
                    part = part + pltpu.roll(part, shift, 1)
                ref[pl.ds(64 * g, 64), :] = part

    low = (lane % ROPE) < (ROPE // 2)

    def rope(v, r0):
        up = pltpu.roll(v, 128 - ROPE // 2, 1)
        dn = pltpu.roll(v, ROPE // 2, 1)
        rot = jnp.where(low, -up, dn)
        return v * cos_v[pl.ds(r0, SPAN), :] + rot * sin_v[pl.ds(r0, SPAN), :]

    def kv_copy(c, t, idx, to):
        return remote(lat_v.at[c, t], lat_v.at[c, t], kv_ssem.at[idx, t], kv_rsem.at[idx, t], dev(c=to))

    loads[0].wait()
    gkv = gkv_r[...]
    with jax.named_scope('ckv'):
        for t in range(2):
            r0 = t * SPAN
            if t == 0:
                loads[1].wait()
                loads[2].wait()
                tables()
                wkr4 = jnp.concatenate([wkr_v[...]] * 4, axis=0)
            else:
                loads[3].wait()
            xs = x_v[pl.ds(r0, SPAN), :]
            lat_v[ctx, t, pl.ds(0, SPAN), :] = rms(dot(xs, wdkv_v[...]), gkv)
            kr = rope(dot_nt(xs, wkr4), r0)
            for half in range(2):
                packed = kr[128 * half:128 * half + KRP]
                for g in range(1, 4):
                    a = 128 * half + KRP * g
                    packed = jnp.where(lane // ROPE == g, kr[a:a + KRP], packed)
                lat_v[ctx, t, pl.ds(SPAN, KRP), pl.ds(128 * half, 128)] = packed.astype(BF16)
            if t == 0:
                kv_copy(ctx, t, 0, ynbr).start()
            else:
                @pl.when(ctx >= 2)
                def _():
                    kv_copy(ctx, 1, 0, ynbr).start()
            kv_copy(ctx, t, 1, partner).start()

    with jax.named_scope('ld4'):
        loads[4].wait()
    gq = jnp.concatenate([gq_r[g:g + 1, :] for g in range(Q_RANK // 128)], axis=1)
    with jax.named_scope('cq'):
        for t in range(2):
            cq_v[pl.ds(t * SPAN, SPAN), :] = rms(dot(x_v[pl.ds(t * SPAN, SPAN), :], wdq_v[...]), gq)
    hop(0, True, False)
    loads[5].wait()
    loads[6].wait()
    with jax.named_scope('qup'):
        for t in range(2):
            cq = cq_v[pl.ds(t * SPAN, SPAN), :]
            qn = dot(cq, wuq_v[...]).astype(BF16)
            zero = jnp.zeros((SPAN, 128), BF16)
            for p in range(PAIRS):
                blk = qn[:, 128 * p:128 * p + 128]
                qm_v[p, t, pl.ds(0, SPAN), pl.ds(0, 128)] = jnp.where(lane < NOPE, blk, zero)
                qm_v[p, t, pl.ds(SPAN, SPAN), pl.ds(0, 128)] = jnp.where(lane < NOPE, zero, blk)
            for b in range(3):
                w = wqr_v[pl.ds(128 * b, 128), :] if b < 2 else jnp.concatenate([wqr_v[pl.ds(256, 64), :]] * 2, axis=0)
                qr = rope(dot_nt(cq, w), t * SPAN).astype(BF16)
                for h in range(4 * b, min(4 * b + 4, HEADS)):
                    qm_v[h // 2, t, pl.ds(SPAN * (h % 2), SPAN), pl.ds(128, 128)] = jnp.where(lane // ROPE == h % 4, qr, zero)

    hop(1, True, False)

    @scoped
    def up(c, t):
        sp = c if t == 0 else NSPAN - 1 - c
        lat = lat_v[c, t, pl.ds(0, SPAN), :]
        kv = dot(lat, wkv_v[...]).astype(BF16)
        k_v[sp] = kv[:, :HV]
        v_v[sp] = kv[:, HV:]
        packed = lat_v[c, t, pl.ds(SPAN, KRP), :].astype(F32)
        for g in range(8):
            part = jnp.where(lane // ROPE == g % 4, packed[:, 128 * (g // 4):128 * (g // 4) + 128], 0.0)
            for shift in (32, 64):
                part = part + pltpu.roll(part, shift, 1)
            kr_v[sp, pl.ds(KRP * g, KRP), :] = part.astype(BF16)

    def up_late(c):
        @pl.when(c >= ctx)
        def _():
            up(c, 1)

    loads[7].wait()
    loads[8].wait()
    up(ctx, 0)
    up(ctx, 1)
    with jax.named_scope('kvw_partner'):
        kv_copy(partner, 0, 1, ctx).wait_recv()
        kv_copy(partner, 1, 1, ctx).wait_recv()
    up(partner, 0)
    up_late(partner)
    hop(2, True, False)
    with jax.named_scope('kvw_ynbr'):
        kv_copy(ynbr, 0, 0, ctx).wait_recv()
    kv_copy(ynbr, 0, 2, partner).start()
    up(ynbr, 0)

    @pl.when(ctx < 2)
    def _():
        kv_copy(ynbr, 1, 0, ctx).wait_recv()
        kv_copy(ynbr, 1, 2, partner).start()
        up(ynbr, 1)
    for q in range(3):
        yfwd(q)
    hop(3)
    with jax.named_scope('kvw_diag'):
        kv_copy(diag, 0, 2, ctx).wait_recv()
    up(diag, 0)

    @pl.when(ctx < 2)
    def _():
        kv_copy(diag, 1, 2, ctx).wait_recv()
        up(diag, 1)
    hop(4, False)
    hop(5, False)

    def block(b):
        if b < 5:
            return 1, NSPAN - 1 - ctx - b
        if b == 8:
            return 0, ctx
        hi = b < NSPAN - ctx
        return jnp.where(hi, 1, 0), jnp.where(hi, NSPAN - 1 - ctx - b, b - (NSPAN - ctx))

    ORDER = (0, 8, 1, 2, 3, 4, 5, 6, 7)
    q_i = lax.broadcasted_iota(jnp.int32, (SPAN, SPAN), 0)
    k_i = lax.broadcasted_iota(jnp.int32, (SPAN, SPAN), 1)
    causal = k_i <= q_i

    def scores(p, b):
        buf = p % 2
        qs, ks = block(b)
        kc = jnp.concatenate([k_v[ks, :, pl.ds(128 * p, 128)], kr_v[ks]], axis=1)
        for a in range(2):
            rows = pl.ds(SPAN * a, SPAN)
            s = dot_nt(qm_v[p, qs, rows, :], kc)
            if b in (0, 8):
                s = jnp.where(causal, s, NEG)
            s_v[buf, b, rows, :] = s
            m = jnp.maximum(s[:, :128], s[:, 128:])
            if b not in (0, 8):
                m = jnp.maximum(mx_v[buf, qs, rows, :], m)
            mx_v[buf, qs, rows, :] = m

    @scoped
    def maxima(p):
        buf = p % 2
        for qs in range(2):
            for a in range(2):
                rows = pl.ds(SPAN * a, SPAN)
                m = jnp.max(mx_v[buf, qs, rows, :], axis=1, keepdims=True)
                mb_v[qs, rows, :] = jnp.broadcast_to(m * SM_SCALE, (SPAN, 128))

    def values(p, b):
        buf = p % 2
        qs, ks = block(b)
        vb = v_v[ks, :, pl.ds(128 * p, 128)]
        for a in range(2):
            rows = pl.ds(SPAN * a, SPAN)
            m = mb_v[qs, rows, :]
            e0 = jnp.exp2(s_v[buf, b, rows, pl.ds(0, 128)] * SM_SCALE - m)
            e1 = jnp.exp2(s_v[buf, b, rows, pl.ds(128, 128)] * SM_SCALE - m)
            pv = dot(jnp.concatenate([e0.astype(BF16), e1.astype(BF16)], axis=1), vb)
            l = e0 + e1
            if b in (0, 8):
                l_v[qs, rows, :] = l
                acc_v[qs, rows, :] = pv
            else:
                l_v[qs, rows, :] += l
                acc_v[qs, rows, :] += pv

    @scoped
    def finish(p):
        for qs in range(2):
            o = []
            for a in range(2):
                rows = pl.ds(SPAN * a, SPAN)
                l = jnp.sum(l_v[qs, rows, :], axis=1, keepdims=True)
                o.append(acc_v[qs, rows, :] / l)
            both = jnp.where(lane < VDIM, o[0], o[1]).astype(BF16)
            os_v[p, 2 * qs] = both[:128]
            os_v[p, 2 * qs + 1] = both[128:]

    def oblk(blk, p, src):
        return oall_v.at[blk, p, src]

    def o_z(p, d):
        to = lax.rem(z + d, MODEL)
        return remote(os_v.at[p, to], oblk(dp, p, z),
                      oz_ssem.at[p, d - 1], oz_rsem.at[p, d - 1], dev(m=to))

    def o_z_wait(p, d):
        src = lax.rem(z + MODEL - d, MODEL)
        remote(os_v.at[p, z], oblk(dp, p, src),
               oz_ssem.at[p, d - 1], oz_rsem.at[p, d - 1], dev()).wait_recv()

    def o_x(p, src_dp, to):
        part = oall_v.at[src_dp, p]
        return remote(part, part, ox_ssem.at[p], ox_rsem.at[p], dev(d=to))

    @scoped
    def send_o(p):
        oblk(dp, p, z)[...] = os_v[p, z]
        for d in (1, 2, 3):
            o_z(p, d).start()

    @scoped
    def pass_o(p):
        for d in (1, 2, 3):
            o_z_wait(p, d)
        o_x(p, dp, xn).start()

    with jax.named_scope('scores0'):
        for b in ORDER:
            scores(0, b)
    maxima(0)
    hop(6, False)
    def pass_o_if(p, cond):
        @pl.when(cond)
        def _():
            pass_o(p)

    relay = {
        0: lambda: (hop(7, False),),
        1: lambda: (hop(8, False),),
        2: lambda: (hop(9, False), pass_o_if(0, ctx != 2)),
        3: lambda: (),
        4: lambda: ([zfwd(q) for q in range(4, 10)], pass_o_if(0, ctx == 2), pass_o(1)),
    }
    for p in range(PAIRS):
        with jax.named_scope('attn%d' % p):
            for b in ORDER:
                if p + 1 < PAIRS:
                    scores(p + 1, b)
                values(p, b)
        finish(p)
        if p + 1 < PAIRS:
            maxima(p + 1)
        send_o(p)
        relay[p]()
    pass_o(2)
    for q in range(4):
        across(q)
    hop(10)
    pass_o(3)
    hop(11)
    across(4)
    across(5)
    pass_o(4)
    hop(12)
    for q in range(6, 10):
        across(q)
    hop(13)
    across(10)
    across(11)
    hop(14)
    across(12)
    for n in range(NSUB):
        loads[9 + n].wait()

    with jax.named_scope('drain1'):
        for t in range(2):
            kv_copy(ctx, t, 1, partner).wait_send()
        kv_copy(ctx, 0, 0, ynbr).wait_send()
        kv_copy(ynbr, 0, 2, partner).wait_send()

        @pl.when(ctx >= 2)
        def _():
            kv_copy(ctx, 1, 0, ynbr).wait_send()

        @pl.when(ctx < 2)
        def _():
            kv_copy(ynbr, 1, 2, partner).wait_send()

        @pl.when(z < MODEL - 1)
        def _():
            w_sent(wz_own.at[1], z, ctx)

        @pl.when(z > 0)
        def _():
            w_sent(wz_own.at[0], z, ctx)

        for p in range(PAIRS):
            for d in (1, 2, 3):
                o_z(p, d).wait_send()
    def ycols(half, n):
        return out_h.at[:, pl.ds(pl.multiple_of(half * NHALF + OFFSETS[n], 128), WIDTHS[n])]

    def yblk(ref, n):
        return ref.at[pl.ds(OFFSETS[n] // 128, WIDTHS[n] // 128)]

    def y_back(n):
        return remote(yblk(ysend_v, n), yblk(yrecv_v, n), yb_ssem.at[n], yb_rsem.at[n], dev(d=xn))

    def y_local(n):
        return pltpu.make_async_copy(yown_v.at[dp, :, pl.ds(OFFSETS[n], WIDTHS[n])], ycols(dp, n), yl_sem.at[n])

    def y_place(i):
        cols = pl.ds(pl.multiple_of(xn * NHALF + 128 * i, 128), 128)
        return pltpu.make_async_copy(yrecv_v.at[i], out_h.at[:, cols], yp_sem.at[i])

    def final(n):
        with jax.named_scope('wdwait%d' % n):
            for j in (1, 2, 3):
                each_share(j, lambda s, sign: (wait_wd(s, 0, n), wait_wd(s, 1, n)))
        with jax.named_scope('final%d' % n):
            o = jnp.concatenate([jnp.concatenate([oall_v[blk, p, s] for s in range(MODEL) for p in range(PAIRS)], axis=1)
                                 for blk in range(2)], axis=0)
            w = jnp.concatenate([wsub(s, n)[...] for s in range(MODEL)], axis=0)
            y = dot(o, w).astype(BF16)
            for blk in range(2):
                yown_v[blk, :, pl.ds(OFFSETS[n], WIDTHS[n])] = y[128 * blk:128 * blk + 128]
            for i in range(WIDTHS[n] // 128):
                ysend_v[OFFSETS[n] // 128 + i] = yown_v[xn, :, pl.ds(OFFSETS[n] + 128 * i, 128)]
            y_back(n).start()
            y_local(n).start()

    with jax.named_scope('oxwait'):
        for p in range(PAIRS):
            o_x(p, xn, dp).wait_recv()
    hop(15)
    final(0)
    across(13)
    hop(16)
    hop(17)
    final(1)
    across(14)
    final(2)
    across(15)
    across(16)
    final(3)
    across(17)
    final(4)
    final(5)

    def sent(s, sign):
        to = z - sign

        @pl.when((to >= 0) & (to < MODEL))
        def _():
            w_sent(wz_ssem.at[s], s, ctx)
        w_sent(wy_ssem.at[s], s, ctx)
        w_sent(wd_ssem.at[s, 0], s, ctx)
        w_sent(wd_ssem.at[s, 1], s, ynbr)

    with jax.named_scope('drain2'):
        for j in (1, 2, 3):
            each_share(j, sent)
        for p in range(PAIRS):
            o_x(p, dp, xn).wait_send()
        for n in range(NSUB):
            y_back(n).wait_recv()
            for i in range(WIDTHS[n] // 128):
                y_place(OFFSETS[n] // 128 + i).start()
        for n in range(NSUB):
            y_back(n).wait_send()
            y_local(n).wait()
        for i in range(NHALF // 128):
            y_place(i).wait()


def layer(x, pos, freq, wdq, gq, wuq, wqr, wdkv, gkv, wkr, wuk, wuv, wout):
    hb = pl.BlockSpec(memory_space=pl.ANY)
    dma = pltpu.SemaphoreType.DMA
    return pl.pallas_call(
        kernel,
        out_shape=jax.ShapeDtypeStruct((ROWS // MODEL, HIDDEN), BF16),
        in_specs=[hb] * 13,
        out_specs=hb,
        scratch_shapes=[
            pltpu.VMEM((1, ROWS), jnp.int32),
            pltpu.VMEM((1, 128), F32),
            pltpu.VMEM((Q_RANK // 128, 128), F32),
            pltpu.VMEM((1, KV_RANK), F32),
            pltpu.VMEM((ROWS, HIDDEN), BF16),
            pltpu.VMEM((HIDDEN, Q_RANK), BF16),
            pltpu.VMEM((Q_RANK, HEADS * NOPE), BF16),
            pltpu.VMEM((HEADS * ROPE, Q_RANK), BF16),
            pltpu.VMEM((HIDDEN, KV_RANK), BF16),
            pltpu.VMEM((ROPE, HIDDEN), BF16),
            pltpu.VMEM((KV_RANK, 2 * HV), BF16),
            pltpu.VMEM((ROWS, 128), F32),
            pltpu.VMEM((ROWS, 128), F32),
            pltpu.VMEM((CTX, 2, SPAN + KRP, KV_RANK), BF16),
            pltpu.VMEM((ROWS, Q_RANK), BF16),
            pltpu.VMEM((PAIRS, 2, 2 * SPAN, 256), BF16),
            pltpu.VMEM((NSPAN, SPAN, HEADS * NOPE), BF16),
            pltpu.VMEM((NSPAN, SPAN, HEADS * VDIM), BF16),
            pltpu.VMEM((NSPAN, SPAN, 128), BF16),
            pltpu.VMEM((2, 9, 2 * SPAN, SPAN), F32),
            pltpu.VMEM((2, 2, 2 * SPAN, 128), F32),
            pltpu.VMEM((2, 2 * SPAN, 128), F32),
            pltpu.VMEM((2, 2 * SPAN, 128), F32),
            pltpu.VMEM((2, 2 * SPAN, 128), F32),
            pltpu.VMEM((PAIRS, MODEL, 128, 128), BF16),
            pltpu.VMEM((2, PAIRS, MODEL, 128, 128), BF16),
            pltpu.VMEM((MODEL, WIDE, HV, 256), BF16),
            pltpu.VMEM((MODEL, NSUB - WIDE, HV, 128), BF16),
            pltpu.VMEM((2, 128, NHALF), BF16),
            pltpu.VMEM((NHALF // 128, 128, 128), BF16),
            pltpu.VMEM((NHALF // 128, 128, 128), BF16),
            dma((19,)),
            dma((3, 2)), dma((3, 2)),
            dma((2, 2)), dma((MODEL, 2)), dma((MODEL, NSUB)),
            dma((MODEL, 2)), dma((MODEL, NSUB)),
            dma((MODEL, 2, 2)), dma((MODEL, 2, NSUB)),
            dma((PAIRS, 3)), dma((PAIRS, 3)),
            dma((PAIRS,)), dma((PAIRS,)),
            dma((NSUB,)), dma((NSUB,)), dma((NSUB,)), dma((NHALF // 128,)),
        ],
        compiler_params=pltpu.CompilerParams(collective_id=0, has_side_effects=True, vmem_limit_bytes=60 * 1024 * 1024),
        name='mla_layer',
    )(x, pos, freq, gq, gkv, wdq, wuq, wqr, wdkv, wkr, wuk, wuv, wout)


def solution(mesh):
    inv_freq = (ROPE_BASE ** (-(np.arange(ROPE // 2, dtype=np.float64) * 2.0 / ROPE))).astype(np.float32)
    freq = np.tile(inv_freq, 128 // (ROPE // 2))[None, :]

    def local(x_tokens, positions, w_dq, gain_q, w_uq, w_qr, w_dkv, gain_kv, w_kr, w_uk, w_uv, w_out):
        return layer(x_tokens, positions[None, :], jnp.asarray(freq), w_dq, gain_q.reshape(Q_RANK // 128, 128), w_uq,
                     w_qr.T, w_dkv, gain_kv[None, :], w_kr.T, w_uk, w_uv, w_out)

    in_specs = (P(('dp', 'ctx'), None), P(('dp', 'ctx')), P(), P(), P(None, 'model'), P(None, 'model'), P(), P(), P(), P(None, 'model'), P(None, 'model'), P('model', None))
    out_specs = P(('dp', 'ctx', 'model'), None)
    return jax.shard_map(local, mesh=mesh, in_specs=in_specs, out_specs=out_specs, check_vma=False)
```
